32 devices in a mesh: gx: 4 (over y, core), gy: 4 (over z), gz: 2 (over x).
Axes of the slice: x: 2, y: 2, z: 4, core: 2. Of those that a mesh axis runs over, the one named last changes fastest.
Arguments:
- face_blocks: float32 [4, 4, 2, 6, 16384], P('gx', 'gy', 'gz'), may hold values from -6 to 6
- owner_rank: int32 [4, 4, 2, 6, 1], P('gx', 'gy', 'gz'), may hold values from 0 to 3; in each aligned block of 6 rows (0 to 5, 6 to 11, ..., all dimensions but the last counted through in order) at most 2 rows name the same one
- owner_tile: int32 [4, 4, 2, 6], P('gx', 'gy', 'gz'), may hold values from 0 to 31
- live_count: int32 [4, 4, 2], P('gx', 'gy', 'gz'), may hold values from 1 to 6, as said below
- right_side: float32 [64, 256, 256], P('gx', 'gy', 'gz'), may hold values from -8 to 8
- diagonal: float32 [64, 256, 256], P('gx', 'gy', 'gz'), may hold values from 0.05 to 1
Outputs:
- solution_field: float32 [64, 256, 256], P('gx', 'gy', 'gz')
- residual: float32 [64, 256, 256], P('gx', 'gy', 'gz')
The draws below stay inside these ranges and needn't reach their ends.
Inputs may be any that keep to these rules, and one draw needn't show every extreme that they name: `owner_rank`: on one device no owner is named by more than 2 of the 6 slots, live or not; some owner is named exactly 2 times on some devices. `live_count`: some device has all 6 slots live in every draw.
All inputs are finite; a program needn't handle non-finite values.
Results may differ from the reference program's by a relative error of at most 0.00012.
Values sent between devices are 32-bit elements; how exact they have to be, the bound alone decides.
A program may use at most 64 MiB of HBM per device.

```python
import math
import jax
import jax.numpy as jnp
import numpy as np

BLK = 128
CAP = 2
ITERS = 2
CX = 16
NB = 6
NX = 64
NY = 256
NZ = 256
N_GX = 4
N_GY = 4
N_GZ = 2


def draw_live_count(key, part):
    counts = jax.random.randint(key, (N_GX, N_GY, N_GZ), 1, NB + 1)
    return counts.at[0, 0, 0].set(NB).astype(jnp.int32)


def set_ends(array, key, smallest, largest):
    place = [jax.random.randint(jax.random.fold_in(key, axis), (), 0, length) for axis, length in enumerate(array.shape)]
    main_axis = array.shape.index(max(array.shape))
    neighbour = place[:main_axis] + [(place[main_axis] + 1) % array.shape[main_axis]] + place[main_axis + 1:]
    return array.at[tuple(place)].set(smallest).at[tuple(neighbour)].set(largest)


def block_scale(rng, dims, split, low, top_value):
    gain = 1.0
    for axis_at, parts in split:
        heights = jax.random.uniform(jax.random.fold_in(jax.random.fold_in(rng, 6), axis_at), (parts,), jnp.float32, low / len(split), top_value / len(split))
        gain = gain * jnp.repeat(jnp.exp(heights), dims[axis_at] // parts).reshape((-1,) + (1,) * (len(dims) - 1 - axis_at))
    return gain


def deal_out(key, own, number, rows, count, top, bound, skew):
    sequence = jax.random.permutation(key, count)
    packed, ordinary = portions_of(count, rows * top, bound, skew, True), portions_of(count, rows * top, bound, skew, False)
    places = jnp.arange(count)

    def named(lengths, turn):
        used = int((lengths > 0).sum())
        fixed = max(1, used // 4)
        shifted = fixed + (places - fixed + turn * (used - fixed)) % max(1, count - fixed)
        return jnp.zeros((count,), jnp.int32).at[sequence[jnp.where(places < fixed, places, shifted)]].set(jnp.asarray(lengths, jnp.int32))

    lengths = jnp.where(number % 4 == 0, named(packed, number // 4), named(ordinary, number - number // 4 - 1))
    mixed = jax.random.permutation(jax.random.fold_in(own, 3), count)
    donor, sink = mixed[0:count // 2 * 2:2], mixed[1:count // 2 * 2:2]
    margin = jnp.minimum(lengths[donor] - 1, bound - lengths[sink]) // 2
    margin = jnp.where((donor == sequence[0]) | (sink == sequence[0]) | (lengths[sink] == 0), 0, jnp.maximum(margin, 0))
    shifted = jax.random.randint(jax.random.fold_in(own, 4), (count // 2,), 0, 1 << 20) % (margin + 1)
    lengths = lengths.at[donor].add(-shifted).at[sink].add(shifted)
    members = jnp.searchsorted(jnp.cumsum(lengths), jnp.arange(rows * top), side="right").astype(jnp.int32)
    listing = members.reshape(top, rows).T
    listing = listing[jax.random.permutation(jax.random.fold_in(own, 1), rows)]
    turn = jax.random.randint(jax.random.fold_in(own, 2), (rows, 1), 0, top)
    return jnp.take_along_axis(listing, (jnp.arange(top)[None, :] + turn) % top, axis=1)


def portions_of(number_of, total, limit, slope, full):
    portions = [(1 << 20) // math.isqrt(standing ** slope) + 1 for standing in range(1, number_of + 1)]
    largest = limit if full else min(limit, max(-(-total // number_of), total * portions[0] // sum(portions)))
    least = 1 if total - largest >= number_of - 1 else 0
    given, spare = [largest] + [least] * (number_of - 1), total - largest - least * (number_of - 1)
    while spare > 0:
        movable = [i for i in range(1, number_of) if given[i] < largest] or [i for i in range(1, number_of) if given[i] < limit]
        mass, left = sum([portions[i] for i in movable]), spare
        for i in movable:
            more = min(limit - given[i], max(1, left * portions[i] // mass), spare)
            given[i] = given[i] + more
            spare = spare - more
    return np.array(given)


def scatter_about(own_key, dims, deviation, reach, split=(), held_as=jnp.bfloat16):
    values = jax.random.normal(own_key, dims, jnp.float32) * deviation
    if len(split) > 0:
        values = block_scale(own_key, dims, split, -0.22, 0.18) * values
    return jnp.clip(values, min=-reach, max=reach).astype(held_as)


def setup_inputs(seed: int = 0) -> dict:
    keys = jax.random.split(jax.random.key(seed), 7)
    face_blocks = scatter_about(keys[0], (N_GX, N_GY, N_GZ, NB, BLK * BLK), 1.0, 6.0, ((0, 4), (1, 4), (2, 2)), jnp.float32)
    owner_rank_keys = jax.random.split(jax.random.fold_in(keys[1], 1), N_GX * N_GY * N_GZ * NB // NB)
    owner_rank_turns = jax.random.permutation(jax.random.fold_in(keys[1], 3), N_GX * N_GY * N_GZ * NB // NB)
    owner_rank = jax.vmap(lambda own, number: deal_out(jax.random.fold_in(keys[1], 2), own, number, NB, N_GX, 1, CAP, 2))(owner_rank_keys, owner_rank_turns).reshape((N_GX, N_GY, N_GZ, NB, 1))
    owner_tile = set_ends(jax.random.randint(keys[2], (N_GX, N_GY, N_GZ, NB), 0, 2 * CX), jax.random.fold_in(keys[2], 1), 0, (2 * CX) - 1).astype(jnp.int32)
    live_count = draw_live_count(jax.random.fold_in(keys[6], 71), 0)
    right_side = scatter_about(keys[4], (NX, NY, NZ), 1.0, 8.0, ((0, 4), (1, 4), (2, 2)), jnp.float32)
    diagonal = jnp.clip(jnp.exp(math.log(1.0) - 2.9957323 * jax.random.uniform(keys[5], (NX, NY, NZ), jnp.float32) ** block_scale(keys[5], (NX, NY, NZ), ((0, 4), (1, 4), (2, 2)), -0.2, 0.2)), 0.05, 1.0)
    return dict(face_blocks=face_blocks, owner_rank=owner_rank, owner_tile=owner_tile, live_count=live_count, right_side=right_side, diagonal=diagonal)


def restrict(values):
    half = BLK // 2
    shaped = values.reshape(values.shape[:-1] + (half, 2, half, 2))
    summed = 0.25 * jnp.sum(shaped, axis=(-3, -1))
    return summed.reshape(values.shape[:-1] + (half * half,))


def operate(field, diagonal):
    padded = jnp.pad(field, 1)
    beside = padded[2:, 1:-1, 1:-1] + padded[:-2, 1:-1, 1:-1]
    beside = beside + padded[1:-1, 2:, 1:-1] + padded[1:-1, :-2, 1:-1]
    beside = beside + padded[1:-1, 1:-1, 2:] + padded[1:-1, 1:-1, :-2]
    return (6.0 + diagonal) * field - beside


def reference(face_blocks, owner_rank, owner_tile, live_count, right_side, diagonal):
    half = BLK // 2
    restricted = restrict(face_blocks)
    slots = jnp.arange(NB, dtype=jnp.int32)
    living = (slots[None, None, None, :] < live_count[..., None]).astype(jnp.float32)
    restricted = restricted * living[..., None]
    row_y = jnp.broadcast_to(jnp.arange(N_GY, dtype=jnp.int32)[None, :, None, None], (N_GX, N_GY, N_GZ, NB))
    row_z = jnp.broadcast_to(jnp.arange(N_GZ, dtype=jnp.int32)[None, None, :, None], (N_GX, N_GY, N_GZ, NB))
    target = owner_rank[..., 0].astype(jnp.int32)
    gathered = jnp.zeros((N_GX, N_GY, N_GZ, 2 * CX, half * half), jnp.float32)
    gathered = gathered.at[target, row_y, row_z, owner_tile.astype(jnp.int32)].add(restricted)
    shaped = gathered.reshape(N_GX, N_GY, N_GZ, CX, 2, half, half)
    source = jnp.transpose(shaped, (0, 3, 1, 5, 2, 4, 6)).reshape(NX, NY, NZ)
    load = right_side + source
    solution_field = jnp.zeros_like(load)
    residual, direction = load, load
    norm_now = jnp.sum(residual * residual)
    for iteration in range(ITERS):
        image = operate(direction, diagonal)
        alpha = norm_now / jnp.sum(direction * image)
        solution_field = solution_field + alpha * direction
        residual = residual - alpha * image
        norm_next = jnp.sum(residual * residual)
        direction = residual + (norm_next / norm_now) * direction
        norm_now = norm_next
    return solution_field, residual
```

```python
import functools
import math

import jax
import jax.numpy as jnp
from jax import lax
from jax.experimental import pallas as pl
from jax.experimental.pallas import tpu as pltpu
from jax.sharding import PartitionSpec as P

CAP = 2
AXES = ("gx", "gy", "gz")
MESH = pl.DeviceIdType.MESH
F32 = jnp.float32


def offsets_of(sizes, axes):
    found = [()]
    for axis in axes:
        found = [done + (step,) for done in found for step in range(sizes[axis])]
    return [dict(zip(axes, steps)) for steps in found if any(steps)]


def stages_of(sizes):
    stages = []
    for axis in ("gx", "gz", "gy"):
        if stages and math.prod(sizes[a] for a in stages[-1] + [axis]) <= 8:
            stages[-1].append(axis)
        else:
            stages.append([axis])
    return stages


def kernel(
    sizes, stages,
    rank_hbm, tile_hbm, live_hbm, face_hbm, right_hbm, diag_hbm,
    load_v, p_v, q_v, coef_ref,
    rank_ref, tile_ref, live_ref, face_v, diag_v, sums_v, send_v, recv_v, turned_v,
    hx_v, ysend_v, hy_v, zsend_v, hz_v, part_v, gath_v,
    in_sem, a2a_send, a2a_recv, halo_send, halo_recv, red_send, red_recv,
):
    cx, cy, cz = load_v.shape
    blocks = face_v.shape[0]
    group = sizes["gx"]
    at = {axis: lax.axis_index(axis) for axis in AXES}

    def near(axis, side):
        return at[axis] > 0 if side == 0 else at[axis] < sizes[axis] - 1

    def beside(offset):
        return {a: lax.rem(at[a] + s, sizes[a]) for a, s in offset.items() if s}

    loads = [
        pltpu.make_async_copy(face_hbm, face_v, in_sem.at[0]),
        pltpu.make_async_copy(right_hbm, load_v, in_sem.at[1]),
        pltpu.make_async_copy(diag_hbm, diag_v, in_sem.at[2]),
        pltpu.make_async_copy(live_hbm, live_ref, in_sem.at[3]),
        pltpu.make_async_copy(rank_hbm, rank_ref, in_sem.at[4]),
        pltpu.make_async_copy(tile_hbm, tile_ref, in_sem.at[5]),
    ]
    for copy in loads:
        copy.start()

    for number, (axis, halo) in enumerate((("gx", hx_v), ("gy", hy_v), ("gz", hz_v))):
        for side in range(2):
            @pl.when(at[axis] == (0 if side == 0 else sizes[axis] - 1))
            def _():
                for turn in range(2):
                    halo[turn, side] = jnp.zeros(halo.shape[2:], F32)

    peers = {}
    for group_axes in [["gx"], ["gy"], ["gz"]] + stages:
        for offset in offsets_of(sizes, group_axes):
            peers[tuple(offset.get(a, 0) for a in AXES)] = offset
    barrier = pltpu.get_barrier_semaphore()
    for offset in peers.values():
        pl.semaphore_signal(barrier, inc=1, device_id=beside(offset), device_id_type=MESH)

    lane = lax.broadcasted_iota(jnp.int32, (cy, cz), 1)
    lane8 = lax.broadcasted_iota(jnp.int32, (8, cz), 1)
    row = lax.broadcasted_iota(jnp.int32, (cy, cz), 0)
    right_half = lane >= cz // 2

    loads[0].wait()
    for copy in loads[3:]:
        copy.wait()
    pair = (
        lax.broadcasted_iota(jnp.int32, (cz, cz), 0) // 2
        == lax.broadcasted_iota(jnp.int32, (cz, cz), 1) % (cz // 2)
    )
    pair = jnp.where(pair, 0.25, 0.0).astype(jnp.bfloat16)
    for b in range(blocks):
        sums_v[b * cy:(b + 1) * cy] = (
            face_v[b, pl.ds(0, cy, stride=2), :] + face_v[b, pl.ds(1, cy, stride=2), :]
        )
    whole = sums_v[...]
    high = whole.astype(jnp.bfloat16)
    rest = whole - high.astype(F32)
    middle = rest.astype(jnp.bfloat16)
    low = (rest - middle.astype(F32)).astype(jnp.bfloat16)
    sums_v[...] = (
        jnp.dot(low, pair, preferred_element_type=F32)
        + jnp.dot(middle, pair, preferred_element_type=F32)
    ) + jnp.dot(high, pair, preferred_element_type=F32)

    target = [rank_ref[b] for b in range(blocks)]
    alive = [live_ref[0, 0, 0] > b for b in range(blocks)]
    position = []
    for b in range(blocks):
        count = jnp.int32(0)
        for before in range(b):
            count = count + jnp.where((target[before] == target[b]) & alive[before], 1, 0)
        position.append(count)
    for k in range(group):
        dest = lax.rem(at["gx"] + k, group)
        total = jnp.zeros((cy, cz), F32)
        tags = jnp.full((8, cz), -1.0, F32)
        for b in range(blocks):
            code = jnp.where(alive[b] & (target[b] == dest), position[b], CAP)
            left, right = jnp.where(code == 0, 1.0, 0.0), jnp.where(code == 1, 1.0, 0.0)
            weight = jnp.where(lane8 < cz // 2, left, right)
            tag = tile_ref[b].astype(F32)
            tags = jnp.where(weight > 0.5, tag, tags)
            values = sums_v[b * cy:(b + 1) * cy]
            total = total + values * jnp.where(right_half, right, left)
        (recv_v if k == 0 else send_v)[k, :cy] = total
        (recv_v if k == 0 else send_v)[k, cy:] = tags

    pl.semaphore_wait(barrier, len(peers))
    exchanges = []
    for k in range(1, group):
        copy = pltpu.make_async_remote_copy(
            src_ref=send_v.at[k], dst_ref=recv_v.at[k],
            send_sem=a2a_send.at[k], recv_sem=a2a_recv.at[k],
            device_id=beside({"gx": k}), device_id_type=MESH,
        )
        copy.start()
        exchanges.append(copy)
    loads[1].wait()
    loads[2].wait()
    for copy in exchanges:
        copy.wait_recv()

    for k in range(group):
        turned_v[k] = pltpu.roll(recv_v[k], cz // 2, axis=1)
    want = [(2 * x + jnp.where(lane8 >= cz // 2, 1, 0)).astype(F32)[:1] for x in range(cx)]
    order = [0, cx - 1] + list(range(1, cx - 1))

    def halo_copy(turn, axis, side, src):
        number, halo = AXES.index(axis), (hx_v, hy_v, hz_v)[AXES.index(axis)]
        step = sizes[axis] - 1 if side == 0 else 1
        return pltpu.make_async_remote_copy(
            src_ref=src, dst_ref=halo.at[turn, 1 - side],
            send_sem=halo_send.at[turn, 2 * number + side],
            recv_sem=halo_recv.at[turn, 2 * number + 1 - side],
            device_id={axis: lax.rem(at[axis] + step, sizes[axis])}, device_id_type=MESH,
        )

    def faces(turn, field, axis):
        if axis == "gx":
            return field.at[0], field.at[cx - 1]
        if axis == "gy":
            return ysend_v.at[turn, 0], ysend_v.at[turn, 1]
        return zsend_v.at[turn], zsend_v.at[turn]

    def send(turn, field, axis):
        for side in range(2):
            @pl.when(near(axis, side))
            def _():
                halo_copy(turn, axis, side, faces(turn, field, axis)[side]).start()

    def receive(turn, field, axis):
        for side in range(2):
            @pl.when(near(axis, side))
            def _():
                halo_copy(turn, axis, 1 - side, faces(turn, field, axis)[1 - side]).wait_recv()

    def finish(turn, field, axis):
        for side in range(2):
            @pl.when(near(axis, side))
            def _():
                halo_copy(turn, axis, side, faces(turn, field, axis)[side]).wait_send()

    def pack(turn, x, plane, packed):
        ysend_v[turn, 0, x:x + 1] = plane[:1]
        ysend_v[turn, 1, x:x + 1] = plane[cy - 1:]
        turned = plane if x == 0 else pltpu.roll(plane, 2 * x, axis=1)
        return jnp.where(((lane + 1) % cz) // 2 == x, turned, packed)

    packed = jnp.zeros((cy, cz), F32)
    for x in order:
        plane = load_v[x]
        for k in range(group):
            values, tags = recv_v[k, :cy], recv_v[k, cy:cy + 1]
            plane = plane + jnp.where(tags == want[x], values, 0.0)
            plane = plane + jnp.where(
                turned_v[k, cy:cy + 1] == want[x], turned_v[k, :cy], 0.0
            )
        load_v[x] = plane
        packed = pack(0, x, plane, packed)
        if x == cx - 1:
            send(0, load_v, "gx")
    zsend_v[0] = packed
    send(0, load_v, "gz")
    send(0, load_v, "gy")

    def inside(src, dst):
        for x in range(cx):
            plane = src[x]
            around = jnp.where(lane == 0, 0.0, pltpu.roll(plane, 1, axis=1))
            around = around + jnp.where(lane == cz - 1, 0.0, pltpu.roll(plane, cz - 1, axis=1))
            around = around + jnp.where(row == 0, 0.0, pltpu.roll(plane, 1, axis=0))
            around = around + jnp.where(row == cy - 1, 0.0, pltpu.roll(plane, cy - 1, axis=0))
            if x > 0:
                around = around + src[x - 1]
            if x < cx - 1:
                around = around + src[x + 1]
            dst[x] = diag_v[x] * plane - around

    def fold(acc, values):
        for part in range(cy // 8):
            acc = acc + values[8 * part:8 * part + 8]
        return acc

    def border(turn, src, dst, sink):
        for axis in ("gx", "gz", "gy"):
            receive(turn, src, axis)
        ahead, behind = hz_v[turn, 1], pltpu.roll(hz_v[turn, 0], 2, axis=1)
        merged = jnp.where(lane % 2 == 0, ahead, behind)
        for x in order:
            edge = pltpu.roll(merged, cz - 2 * x - 1, axis=1)
            plane = dst[x] - jnp.where((lane == 0) | (lane == cz - 1), edge, 0.0)
            plane = plane - jnp.where(row == 0, hy_v[turn, 0, x:x + 1], 0.0)
            plane = plane - jnp.where(row == cy - 1, hy_v[turn, 1, x:x + 1], 0.0)
            if x == 0:
                plane = plane - hx_v[turn, 0]
            if x == cx - 1:
                plane = plane - hx_v[turn, 1]
            dst[x] = plane
            sink(x, plane)

    inside(load_v, p_v)
    state = {"packed": jnp.zeros((cy, cz), F32)}

    def first(x, plane):
        state["packed"] = pack(1, x, plane, state["packed"])
        if x == cx - 1:
            send(1, p_v, "gx")

    border(0, load_v, p_v, first)
    zsend_v[1] = state["packed"]
    send(1, p_v, "gz")
    send(1, p_v, "gy")
    inside(p_v, q_v)
    acc = [jnp.zeros((8, cz), F32) for _ in range(4)]
    for x in range(cx):
        load, p = load_v[x], p_v[x]
        acc[0], acc[1], acc[2] = fold(acc[0], load * load), fold(acc[1], load * p), fold(acc[2], p * p)

    def second(x, plane):
        acc[3] = fold(acc[3], plane * p_v[x])

    border(1, p_v, q_v, second)

    row8 = lax.broadcasted_iota(jnp.int32, (8, cz), 0)
    mine = jnp.zeros((8, cz), F32)
    for number in range(4):
        mine = jnp.where(row8 == number, jnp.sum(acc[number], axis=0, keepdims=True), mine)
    slot = 0
    waiting = []
    for number, axes in enumerate(stages):
        part_v[number] = mine
        copies = []
        for offset in offsets_of(sizes, axes):
            copy = pltpu.make_async_remote_copy(
                src_ref=part_v.at[number], dst_ref=gath_v.at[slot],
                send_sem=red_send.at[slot], recv_sem=red_recv.at[slot],
                device_id=beside(offset), device_id_type=MESH,
            )
            copy.start()
            copies.append((slot, copy))
            slot += 1
        for at_slot, copy in copies:
            copy.wait_recv()
            mine = mine + gath_v[at_slot]
        waiting += [copy for _, copy in copies]

    sums = jnp.sum(mine, axis=1, keepdims=True)
    s0, s1, s2, s3 = (sums[n:n + 1] for n in range(4))
    step = 6.0 * s0 + s1
    a = s0 / step
    c = s1 / step
    norm = c * c * s0 - 2.0 * a * c * s1 + a * a * s2
    e = c + norm / s0
    curve = 6.0 * (e * e * s0 - 2.0 * e * a * s1 + a * a * s2) + (
        e * e * s1 - 2.0 * e * a * s2 + a * a * s3
    )
    b = norm / curve
    x_load, x_p = a + b * e, b * a
    r_load, r_p, r_q = c - 6.0 * b * e, a + b * (e - 6.0 * a), b * a
    for number, value in enumerate((x_load, x_p, r_load, r_p, r_q)):
        coef_ref[number:number + 1] = jnp.broadcast_to(value, (1, cz))
    for copy in exchanges + waiting:
        copy.wait_send()
    for turn, field in ((0, load_v), (1, p_v)):
        for axis in AXES:
            finish(turn, field, axis)


def combine(load_ref, p_ref, q_ref, coef_ref, x_hbm, r_hbm, x_v, r_v, sem):
    cx = load_ref.shape[0]
    x_load, x_p, r_load, r_p, r_q = (coef_ref[n:n + 1] for n in range(5))
    pieces = sem.shape[1]
    copies = []
    for piece in range(pieces):
        first, last = cx * piece // pieces, cx * (piece + 1) // pieces
        for x in range(first, last):
            load, p = load_ref[x], p_ref[x]
            x_v[x] = x_load * load - x_p * p
            r_v[x] = r_load * load - r_p * p + r_q * q_ref[x]
        span = pl.ds(first, last - first)
        for number, (src, dst) in enumerate(((x_v, x_hbm), (r_v, r_hbm))):
            copy = pltpu.make_async_copy(src.at[span], dst.at[span], sem.at[number, piece])
            copy.start()
            copies.append(copy)
    for copy in copies:
        copy.wait()


def combined(load, p, q, coef):
    cx, cy, cz = load.shape
    box = jax.ShapeDtypeStruct((cx, cy, cz), F32)
    vmem, hbm = (pl.BlockSpec(memory_space=space) for space in (pltpu.VMEM, pltpu.HBM))
    return pl.pallas_call(
        combine,
        out_shape=(box, box),
        in_specs=[vmem] * 4,
        out_specs=(hbm, hbm),
        scratch_shapes=[pltpu.VMEM((cx, cy, cz), F32)] * 2 + [pltpu.SemaphoreType.DMA((2, 4))],
    )(*(pltpu.with_memory_space_constraint(a, pltpu.VMEM) for a in (load, p, q, coef)))


def per_device(sizes, face_blocks, owner_rank, owner_tile, live_count, right_side, diagonal):
    blocks = face_blocks.shape[3]
    cx, cy, cz = right_side.shape
    group = sizes["gx"]
    stages = stages_of(sizes)
    slots = sum(len(offsets_of(sizes, axes)) for axes in stages)
    vmem, hbm = (pl.BlockSpec(memory_space=space) for space in (pltpu.VMEM, pltpu.HBM))
    box = pltpu.VMEM((cx, cy, cz), F32)
    load, p, q, coef = pl.pallas_call(
        functools.partial(kernel, sizes, stages),
        out_shape=(box, box, box, pltpu.VMEM((8, cz), F32)),
        in_specs=[hbm] * 6,
        out_specs=(vmem, vmem, vmem, vmem),
        scratch_shapes=[
            pltpu.SMEM((blocks,), jnp.int32),
            pltpu.SMEM((blocks,), jnp.int32),
            pltpu.SMEM(live_count.shape, jnp.int32),
            pltpu.VMEM((blocks, 2 * cy, cz), F32),
            pltpu.VMEM((cx, cy, cz), F32),
            pltpu.VMEM((blocks * cy, cz), F32),
            pltpu.VMEM((group, cy + 8, cz), F32),
            pltpu.VMEM((group, cy + 8, cz), F32),
            pltpu.VMEM((group, cy + 8, cz), F32),
            pltpu.VMEM((2, 2, cy, cz), F32),
            pltpu.VMEM((2, 2, cx, cz), F32),
            pltpu.VMEM((2, 2, cx, cz), F32),
            pltpu.VMEM((2, cy, cz), F32),
            pltpu.VMEM((2, 2, cy, cz), F32),
            pltpu.VMEM((len(stages), 8, cz), F32),
            pltpu.VMEM((slots, 8, cz), F32),
            pltpu.SemaphoreType.DMA((6,)),
            pltpu.SemaphoreType.DMA((group,)),
            pltpu.SemaphoreType.DMA((group,)),
            pltpu.SemaphoreType.DMA((2, 6)),
            pltpu.SemaphoreType.DMA((2, 6)),
            pltpu.SemaphoreType.DMA((slots,)),
            pltpu.SemaphoreType.DMA((slots,)),
        ],
        compiler_params=pltpu.CompilerParams(collective_id=0, has_side_effects=True),
    )(
        owner_rank.reshape(blocks), owner_tile.reshape(blocks),
        live_count,
        face_blocks.reshape(blocks, 2 * cy, cz), right_side, diagonal,
    )
    return combined(load, p, q, coef)


def solution(mesh):
    sizes = dict(mesh.shape)
    return jax.shard_map(
        functools.partial(per_device, sizes),
        mesh=mesh,
        in_specs=(
            P("gx", "gy", "gz", None, None),
            P("gx", "gy", "gz", None, None),
            P("gx", "gy", "gz", None),
            P("gx", "gy", "gz"),
            P("gx", "gy", "gz"),
            P("gx", "gy", "gz"),
        ),
        out_specs=(P("gx", "gy", "gz"), P("gx", "gy", "gz")),
        check_vma=False,
    )
```

```python
import functools
import math

import jax
import jax.numpy as jnp
from jax import lax
from jax.experimental import pallas as pl
from jax.experimental.pallas import tpu as pltpu
from jax.sharding import PartitionSpec as P

CAP = 2
AXES = ("gx", "gy", "gz")
MESH = pl.DeviceIdType.MESH
F32 = jnp.float32


def offsets_of(sizes, axes):
    found = [()]
    for axis in axes:
        found = [done + (step,) for done in found for step in range(sizes[axis])]
    return [dict(zip(axes, steps)) for steps in found if any(steps)]


def stages_of(sizes):
    stages = []
    for axis in ("gx", "gz", "gy"):
        if stages and math.prod(sizes[a] for a in stages[-1] + [axis]) <= 32:
            stages[-1].append(axis)
        else:
            stages.append([axis])
    return stages


def relays_of(sizes, stages):
    reach = max(
        sum(1 if axis == "gx" else sizes[axis] - 1 for axis in axes if sizes[axis] > 1)
        for axes in stages
    )
    return max(1, reach - 2)


def kernel(
    sizes, stages, relays,
    rank_hbm, tile_hbm, live_hbm, face_hbm, right_hbm, diag_hbm,
    load_v, p_v, q_v, coef_ref,
    rank_ref, tile_ref, live_ref, face_v, diag_v, sums_v, send_v, stag_v, recv_v, rtag_v, turned_v,
    hx_v, ysend_v, hy_v, zsend_v, hz_v, part_v, gath_v,
    in_sem, a2a_send, a2a_recv, relay_sem, halo_send, halo_recv, red_send, red_recv,
):
    cx, cy, cz = load_v.shape
    blocks = face_v.shape[0]
    group = sizes["gx"]
    at = {axis: lax.axis_index(axis) for axis in AXES}

    def near(axis, side):
        return at[axis] > 0 if side == 0 else at[axis] < sizes[axis] - 1

    def beside(offset):
        return {a: lax.rem(at[a] + s, sizes[a]) for a, s in offset.items() if s}

    loads = [
        pltpu.make_async_copy(face_hbm, face_v, in_sem.at[0]),
        pltpu.make_async_copy(right_hbm, load_v, in_sem.at[1]),
        pltpu.make_async_copy(diag_hbm, diag_v, in_sem.at[2]),
        pltpu.make_async_copy(live_hbm, live_ref, in_sem.at[3]),
        pltpu.make_async_copy(rank_hbm, rank_ref, in_sem.at[4]),
        pltpu.make_async_copy(tile_hbm, tile_ref, in_sem.at[5]),
    ]
    for copy in loads:
        copy.start()

    for number, (axis, halo) in enumerate((("gx", hx_v), ("gy", hy_v), ("gz", hz_v))):
        for side in range(2):
            @pl.when(at[axis] == (0 if side == 0 else sizes[axis] - 1))
            def _():
                for turn in range(2):
                    halo[turn, side] = jnp.zeros(halo.shape[2:], F32)

    def greet(semaphore):
        for k in range(1, group):
            pl.semaphore_signal(
                semaphore, inc=1, device_id=beside({"gx": k}), device_id_type=MESH
            )
        for axis in ("gy", "gz"):
            for side in range(2):
                @pl.when(near(axis, side))
                def _():
                    pl.semaphore_signal(
                        semaphore, inc=1, device_id={axis: at[axis] + 2 * side - 1},
                        device_id_type=MESH,
                    )

    greeted = jnp.int32(group - 1)
    for axis in ("gy", "gz"):
        for side in range(2):
            greeted = greeted + jnp.where(near(axis, side), 1, 0)
    barrier = pltpu.get_barrier_semaphore()
    greet(barrier)

    lane = lax.broadcasted_iota(jnp.int32, (cy, cz), 1)
    lane1 = lax.broadcasted_iota(jnp.int32, (1, cz), 1)
    lane8 = lax.broadcasted_iota(jnp.int32, (8, cz), 1)
    row = lax.broadcasted_iota(jnp.int32, (cy, cz), 0)
    right_half = lane >= cz // 2

    loads[0].wait()
    for copy in loads[3:]:
        copy.wait()
    pair = (
        lax.broadcasted_iota(jnp.int32, (cz, cz), 0) // 2
        == lax.broadcasted_iota(jnp.int32, (cz, cz), 1) % (cz // 2)
    )
    pair = jnp.where(pair, 0.25, 0.0).astype(jnp.bfloat16)
    for b in range(blocks):
        sums_v[b * cy:(b + 1) * cy] = (
            face_v[b, pl.ds(0, cy, stride=2), :] + face_v[b, pl.ds(1, cy, stride=2), :]
        )
    whole = sums_v[...]
    high = whole.astype(jnp.bfloat16)
    rest = whole - high.astype(F32)
    middle = rest.astype(jnp.bfloat16)
    low = (rest - middle.astype(F32)).astype(jnp.bfloat16)
    sums_v[...] = (
        jnp.dot(low, pair, preferred_element_type=F32)
        + jnp.dot(middle, pair, preferred_element_type=F32)
    ) + jnp.dot(high, pair, preferred_element_type=F32)

    target = [rank_ref[b] for b in range(blocks)]
    alive = [live_ref[0, 0, 0] > b for b in range(blocks)]
    position = []
    for b in range(blocks):
        count = jnp.int32(0)
        for before in range(b):
            count = count + jnp.where((target[before] == target[b]) & alive[before], 1, 0)
        position.append(count)
    for k in range(group):
        dest = lax.rem(at["gx"] + k, group)
        total = jnp.zeros((cy, cz), F32)
        tags = jnp.full((1, cz), -1.0, F32)
        for b in range(blocks):
            code = jnp.where(alive[b] & (target[b] == dest), position[b], CAP)
            left, right = jnp.where(code == 0, 1.0, 0.0), jnp.where(code == 1, 1.0, 0.0)
            weight = jnp.where(lane1 < cz // 2, left, right)
            tag = tile_ref[b].astype(F32)
            tags = jnp.where(weight > 0.5, tag, tags)
            values = sums_v[b * cy:(b + 1) * cy]
            total = total + values * jnp.where(right_half, right, left)
        (recv_v if k == 0 else send_v)[k] = total
        (rtag_v if k == 0 else stag_v)[k] = tags

    pl.semaphore_wait(barrier, greeted)
    exchanges = []
    for k in range(1, group):
        for number, (src, dst) in enumerate(((send_v, recv_v), (stag_v, rtag_v))):
            copy = pltpu.make_async_remote_copy(
                src_ref=src.at[k], dst_ref=dst.at[k],
                send_sem=a2a_send.at[number, k], recv_sem=a2a_recv.at[number, k],
                device_id=beside({"gx": k}), device_id_type=MESH,
            )
            copy.start()
            exchanges.append(copy)
    for relay in range(relays - 1):
        greet(relay_sem.at[relay])
        pl.semaphore_wait(relay_sem.at[relay], greeted)
    greet(relay_sem.at[relays - 1])
    loads[1].wait()
    loads[2].wait()
    for copy in exchanges:
        copy.wait_recv()

    for k in range(group):
        turned_v[k] = pltpu.roll(recv_v[k], cz // 2, axis=1)
    tags_of = [rtag_v[k] for k in range(group)]
    turned_tags = [
        pltpu.roll(jnp.broadcast_to(tags, (8, cz)), cz // 2, axis=1)[:1] for tags in tags_of
    ]
    want = [(2 * x + jnp.where(lane1 >= cz // 2, 1, 0)).astype(F32) for x in range(cx)]
    order = [0, cx - 1] + list(range(1, cx - 1))

    def halo_copy(turn, axis, side, src):
        number, halo = AXES.index(axis), (hx_v, hy_v, hz_v)[AXES.index(axis)]
        step = sizes[axis] - 1 if side == 0 else 1
        return pltpu.make_async_remote_copy(
            src_ref=src, dst_ref=halo.at[turn, 1 - side],
            send_sem=halo_send.at[turn, 2 * number + side],
            recv_sem=halo_recv.at[turn, 2 * number + 1 - side],
            device_id={axis: lax.rem(at[axis] + step, sizes[axis])}, device_id_type=MESH,
        )

    def faces(turn, field, axis):
        if axis == "gx":
            return field.at[0], field.at[cx - 1]
        if axis == "gy":
            return ysend_v.at[turn, 0], ysend_v.at[turn, 1]
        return zsend_v.at[turn], zsend_v.at[turn]

    def send(turn, field, axis):
        for side in range(2):
            @pl.when(near(axis, side))
            def _():
                halo_copy(turn, axis, side, faces(turn, field, axis)[side]).start()

    def receive(turn, field, axis):
        for side in range(2):
            @pl.when(near(axis, side))
            def _():
                halo_copy(turn, axis, 1 - side, faces(turn, field, axis)[1 - side]).wait_recv()

    def finish(turn, field, axis):
        for side in range(2):
            @pl.when(near(axis, side))
            def _():
                halo_copy(turn, axis, side, faces(turn, field, axis)[side]).wait_send()

    def pack(turn, x, plane, packed):
        ysend_v[turn, 0, x:x + 1] = plane[:1]
        ysend_v[turn, 1, x:x + 1] = plane[cy - 1:]
        turned = plane if x == 0 else pltpu.roll(plane, 2 * x, axis=1)
        return jnp.where(((lane + 1) % cz) // 2 == x, turned, packed)

    packed = jnp.zeros((cy, cz), F32)
    for x in order:
        plane = load_v[x]
        for k in range(group):
            plane = plane + jnp.where(tags_of[k] == want[x], recv_v[k], 0.0)
            plane = plane + jnp.where(turned_tags[k] == want[x], turned_v[k], 0.0)
        load_v[x] = plane
        packed = pack(0, x, plane, packed)
        if x == cx - 1:
            send(0, load_v, "gx")
    zsend_v[0] = packed
    send(0, load_v, "gz")
    send(0, load_v, "gy")

    def inside(src, dst):
        for x in range(cx):
            plane = src[x]
            around = jnp.where(lane == 0, 0.0, pltpu.roll(plane, 1, axis=1))
            around = around + jnp.where(lane == cz - 1, 0.0, pltpu.roll(plane, cz - 1, axis=1))
            around = around + jnp.where(row == 0, 0.0, pltpu.roll(plane, 1, axis=0))
            around = around + jnp.where(row == cy - 1, 0.0, pltpu.roll(plane, cy - 1, axis=0))
            if x > 0:
                around = around + src[x - 1]
            if x < cx - 1:
                around = around + src[x + 1]
            dst[x] = diag_v[x] * plane - around

    def fold(acc, values):
        for part in range(cy // 8):
            acc = acc + values[8 * part:8 * part + 8]
        return acc

    def border(turn, src, dst, sink):
        for axis in ("gx", "gz", "gy"):
            receive(turn, src, axis)
        ahead, behind = hz_v[turn, 1], pltpu.roll(hz_v[turn, 0], 2, axis=1)
        merged = jnp.where(lane % 2 == 0, ahead, behind)
        for x in order:
            edge = pltpu.roll(merged, cz - 2 * x - 1, axis=1)
            plane = dst[x] - jnp.where((lane == 0) | (lane == cz - 1), edge, 0.0)
            plane = plane - jnp.where(row == 0, hy_v[turn, 0, x:x + 1], 0.0)
            plane = plane - jnp.where(row == cy - 1, hy_v[turn, 1, x:x + 1], 0.0)
            if x == 0:
                plane = plane - hx_v[turn, 0]
            if x == cx - 1:
                plane = plane - hx_v[turn, 1]
            dst[x] = plane
            sink(x, plane)

    pl.semaphore_wait(relay_sem.at[relays - 1], greeted)
    inside(load_v, p_v)
    state = {"packed": jnp.zeros((cy, cz), F32)}

    def first(x, plane):
        state["packed"] = pack(1, x, plane, state["packed"])
        if x == cx - 1:
            send(1, p_v, "gx")

    border(0, load_v, p_v, first)
    zsend_v[1] = state["packed"]
    send(1, p_v, "gz")
    send(1, p_v, "gy")
    inside(p_v, q_v)
    acc = [jnp.zeros((8, cz), F32) for _ in range(4)]
    for x in range(cx):
        load, p = load_v[x], p_v[x]
        acc[0], acc[1], acc[2] = fold(acc[0], load * load), fold(acc[1], load * p), fold(acc[2], p * p)

    def second(x, plane):
        acc[3] = fold(acc[3], plane * p_v[x])

    border(1, p_v, q_v, second)

    row8 = lax.broadcasted_iota(jnp.int32, (8, cz), 0)
    mine = jnp.zeros((8, cz), F32)
    for number in range(4):
        mine = jnp.where(row8 == number, jnp.sum(acc[number], axis=0, keepdims=True), mine)
    mine = mine + pltpu.roll(mine, cz // 2, axis=1)
    mine = mine + pltpu.roll(mine, cz // 4, axis=1)
    own = row8 == lane8 // (cz // 4)
    mine = jnp.sum(jnp.where(own, mine, 0.0), axis=0, keepdims=True)
    slot = 0
    waiting = []
    for number, axes in enumerate(stages):
        part_v[number] = mine
        copies = []
        for offset in offsets_of(sizes, axes):
            copy = pltpu.make_async_remote_copy(
                src_ref=part_v.at[number], dst_ref=gath_v.at[slot],
                send_sem=red_send.at[slot], recv_sem=red_recv.at[slot],
                device_id=beside(offset), device_id_type=MESH,
            )
            copy.start()
            copies.append((slot, copy))
            slot += 1
        for at_slot, copy in copies:
            copy.wait_recv()
            mine = mine + gath_v[at_slot]
        waiting += [copy for _, copy in copies]

    sums = jnp.sum(jnp.where(own, mine, 0.0), axis=1, keepdims=True)
    s0, s1, s2, s3 = (sums[n:n + 1] for n in range(4))
    step = 6.0 * s0 + s1
    a = s0 / step
    c = s1 / step
    norm = c * c * s0 - 2.0 * a * c * s1 + a * a * s2
    e = c + norm / s0
    curve = 6.0 * (e * e * s0 - 2.0 * e * a * s1 + a * a * s2) + (
        e * e * s1 - 2.0 * e * a * s2 + a * a * s3
    )
    b = norm / curve
    x_load, x_p = a + b * e, b * a
    r_load, r_p, r_q = c - 6.0 * b * e, a + b * (e - 6.0 * a), b * a
    for number, value in enumerate((x_load, x_p, r_load, r_p, r_q)):
        coef_ref[number:number + 1] = jnp.broadcast_to(value, (1, cz))
    for copy in exchanges + waiting:
        copy.wait_send()
    for turn, field in ((0, load_v), (1, p_v)):
        for axis in AXES:
            finish(turn, field, axis)


def combine(load_ref, p_ref, q_ref, coef_ref, x_hbm, r_hbm, x_v, r_v, sem):
    cx = load_ref.shape[0]
    x_load, x_p, r_load, r_p, r_q = (coef_ref[n:n + 1] for n in range(5))
    pieces = sem.shape[1]
    copies = []
    for piece in range(pieces):
        first, last = cx * piece // pieces, cx * (piece + 1) // pieces
        for x in range(first, last):
            load, p = load_ref[x], p_ref[x]
            x_v[x] = x_load * load - x_p * p
            r_v[x] = r_load * load - r_p * p + r_q * q_ref[x]
        span = pl.ds(first, last - first)
        for number, (src, dst) in enumerate(((x_v, x_hbm), (r_v, r_hbm))):
            copy = pltpu.make_async_copy(src.at[span], dst.at[span], sem.at[number, piece])
            copy.start()
            copies.append(copy)
    for copy in copies:
        copy.wait()


def combined(load, p, q, coef):
    cx, cy, cz = load.shape
    box = jax.ShapeDtypeStruct((cx, cy, cz), F32)
    vmem, hbm = (pl.BlockSpec(memory_space=space) for space in (pltpu.VMEM, pltpu.HBM))
    return pl.pallas_call(
        combine,
        out_shape=(box, box),
        in_specs=[vmem] * 4,
        out_specs=(hbm, hbm),
        scratch_shapes=[pltpu.VMEM((cx, cy, cz), F32)] * 2 + [pltpu.SemaphoreType.DMA((2, 4))],
    )(*(pltpu.with_memory_space_constraint(a, pltpu.VMEM) for a in (load, p, q, coef)))


def per_device(sizes, face_blocks, owner_rank, owner_tile, live_count, right_side, diagonal):
    blocks = face_blocks.shape[3]
    cx, cy, cz = right_side.shape
    group = sizes["gx"]
    stages = stages_of(sizes)
    relays = relays_of(sizes, stages)
    slots = sum(len(offsets_of(sizes, axes)) for axes in stages)
    vmem, hbm = (pl.BlockSpec(memory_space=space) for space in (pltpu.VMEM, pltpu.HBM))
    box = pltpu.VMEM((cx, cy, cz), F32)
    load, p, q, coef = pl.pallas_call(
        functools.partial(kernel, sizes, stages, relays),
        out_shape=(box, box, box, pltpu.VMEM((8, cz), F32)),
        in_specs=[hbm] * 6,
        out_specs=(vmem, vmem, vmem, vmem),
        scratch_shapes=[
            pltpu.SMEM((blocks,), jnp.int32),
            pltpu.SMEM((blocks,), jnp.int32),
            pltpu.SMEM(live_count.shape, jnp.int32),
            pltpu.VMEM((blocks, 2 * cy, cz), F32),
            pltpu.VMEM((cx, cy, cz), F32),
            pltpu.VMEM((blocks * cy, cz), F32),
            pltpu.VMEM((group, cy, cz), F32),
            pltpu.VMEM((group, 1, cz), F32),
            pltpu.VMEM((group, cy, cz), F32),
            pltpu.VMEM((group, 1, cz), F32),
            pltpu.VMEM((group, cy, cz), F32),
            pltpu.VMEM((2, 2, cy, cz), F32),
            pltpu.VMEM((2, 2, cx, cz), F32),
            pltpu.VMEM((2, 2, cx, cz), F32),
            pltpu.VMEM((2, cy, cz), F32),
            pltpu.VMEM((2, 2, cy, cz), F32),
            pltpu.VMEM((len(stages), 1, cz), F32),
            pltpu.VMEM((slots, 1, cz), F32),
            pltpu.SemaphoreType.DMA((6,)),
            pltpu.SemaphoreType.DMA((2, group)),
            pltpu.SemaphoreType.DMA((2, group)),
            pltpu.SemaphoreType.REGULAR((relays,)),
            pltpu.SemaphoreType.DMA((2, 6)),
            pltpu.SemaphoreType.DMA((2, 6)),
            pltpu.SemaphoreType.DMA((slots,)),
            pltpu.SemaphoreType.DMA((slots,)),
        ],
        compiler_params=pltpu.CompilerParams(collective_id=0, has_side_effects=True),
    )(
        owner_rank.reshape(blocks), owner_tile.reshape(blocks),
        live_count,
        face_blocks.reshape(blocks, 2 * cy, cz), right_side, diagonal,
    )
    return combined(load, p, q, coef)


def solution(mesh):
    sizes = dict(mesh.shape)
    return jax.shard_map(
        functools.partial(per_device, sizes),
        mesh=mesh,
        in_specs=(
            P("gx", "gy", "gz", None, None),
            P("gx", "gy", "gz", None, None),
            P("gx", "gy", "gz", None),
            P("gx", "gy", "gz"),
            P("gx", "gy", "gz"),
            P("gx", "gy", "gz"),
        ),
        out_specs=(P("gx", "gy", "gz"), P("gx", "gy", "gz")),
        check_vma=False,
    )
```

```python
import functools
import math

import jax
import jax.numpy as jnp
from jax import lax
from jax.experimental import pallas as pl
from jax.experimental.pallas import tpu as pltpu
from jax.sharding import PartitionSpec as P

CAP = 2
AXES = ("gx", "gy", "gz")
MESH = pl.DeviceIdType.MESH
F32 = jnp.float32


def offsets_of(sizes, axes):
    found = [()]
    for axis in axes:
        found = [done + (step,) for done in found for step in range(sizes[axis])]
    return [dict(zip(axes, steps)) for steps in found if any(steps)]


def stages_of(sizes):
    stages = []
    for axis in ("gx", "gz", "gy"):
        if stages and math.prod(sizes[a] for a in stages[-1] + [axis]) <= 32:
            stages[-1].append(axis)
        else:
            stages.append([axis])
    return stages


def relays_of(sizes, stages):
    reach = max(
        sum(1 if axis == "gx" else sizes[axis] - 1 for axis in axes if sizes[axis] > 1)
        for axes in stages
    )
    return max(1, reach - 2)


def kernel(
    sizes, stages, relays,
    rank_hbm, tile_hbm, live_hbm, face_hbm, right_hbm, diag_hbm,
    load_v, p_v, q_v, coef_ref,
    rank_ref, tile_ref, live_ref, face_v, diag_v, sums_v,
    send_v, stag_v, recv_v, rtag_v, turned_v, rows_v, drows_v, cols_v,
    hx_v, ysend_v, hy_v, zsend_v, hz_v, xy_v, hxy_v, yz_v, hyz_v, xz_v, hxz_v, part_v, gath_v,
    in_sem, a2a_send, a2a_recv, relay_sem, halo_send, halo_recv, red_send, red_recv,
):
    cx, cy, cz = load_v.shape
    blocks = face_v.shape[0]
    group = sizes["gx"]
    folds = cy // zsend_v.shape[0]
    at = {axis: lax.axis_index(axis) for axis in AXES}

    def near(axis, side):
        return at[axis] > 0 if side == 0 else at[axis] < sizes[axis] - 1

    def beside(offset):
        return {a: lax.rem(at[a] + s, sizes[a]) for a, s in offset.items() if s}

    def near_all(sides):
        found = near(*sides[0])
        for axis, side in sides[1:]:
            found = found & near(axis, side)
        return found

    loads = [
        pltpu.make_async_copy(face_hbm, face_v, in_sem.at[0]),
        pltpu.make_async_copy(right_hbm, load_v, in_sem.at[1]),
        pltpu.make_async_copy(diag_hbm, diag_v, in_sem.at[2]),
        pltpu.make_async_copy(live_hbm, live_ref, in_sem.at[3]),
        pltpu.make_async_copy(rank_hbm, rank_ref, in_sem.at[4]),
        pltpu.make_async_copy(tile_hbm, tile_ref, in_sem.at[5]),
    ]
    for copy in loads:
        copy.start()

    def greet(semaphore):
        for k in range(1, group):
            pl.semaphore_signal(
                semaphore, inc=1, device_id=beside({"gx": k}), device_id_type=MESH
            )
        for axis in ("gy", "gz"):
            for side in range(2):
                @pl.when(near(axis, side))
                def _():
                    pl.semaphore_signal(
                        semaphore, inc=1, device_id={axis: at[axis] + 2 * side - 1},
                        device_id_type=MESH,
                    )

    greeted = jnp.int32(group - 1)
    for axis in ("gy", "gz"):
        for side in range(2):
            greeted = greeted + jnp.where(near(axis, side), 1, 0)
    barrier = pltpu.get_barrier_semaphore()
    greet(barrier)

    messages = {"x": [], "z": [], "y": [], "corner": []}
    for s in range(2):
        end = (cx - 1) * s
        messages["x"].append(((("gx", s),), load_v.at[end], lambda s: hx_v.at[s, 0]))
        messages["x"].append(((("gx", s),), p_v.at[end], lambda s: hx_v.at[s, 1]))
        messages["y"].append(((("gy", s),), ysend_v.at[s], lambda s: hy_v.at[s]))
        messages["z"].append(((("gz", s),), zsend_v, lambda s: hz_v.at[s]))
    for s in range(2):
        for t in range(2):
            messages["corner"] += [
                ((("gx", s), ("gy", t)), xy_v.at[2 * s + t], lambda s, t: hxy_v.at[2 * s + t]),
                ((("gx", s), ("gz", t)), xz_v, lambda s, t: hxz_v.at[2 * s + t]),
                ((("gy", s), ("gz", t)), yz_v.at[s], lambda s, t: hyz_v.at[2 * s + t]),
            ]
    number = {}
    for name, group_of in messages.items():
        for order, (sides, _, _) in enumerate(group_of):
            number[name, order] = len(number)

    def opposite(name, order):
        sides = messages[name][order][0]
        width = {"x": 2, "y": 1, "z": 1, "corner": 3}[name]
        flipped = 0
        for _, side in sides:
            flipped = 2 * flipped + 1 - side
        return width * flipped + order % width

    def message(name, order):
        sides, src, place = messages[name][order]
        back = number[name, opposite(name, order)]
        return pltpu.make_async_remote_copy(
            src_ref=src, dst_ref=place(*[1 - side for _, side in sides]),
            send_sem=halo_send.at[number[name, order]], recv_sem=halo_recv.at[back],
            device_id={
                axis: lax.rem(at[axis] + (1 if side else sizes[axis] - 1), sizes[axis])
                for axis, side in sides
            },
            device_id_type=MESH,
        )

    def each(name, act):
        for order, (sides, _, _) in enumerate(messages[name]):
            @pl.when(near_all(sides))
            def _():
                act(name, order)

    def send(name):
        each(name, lambda name, order: message(name, order).start())

    def receive(name):
        each(name, lambda name, order: message(name, opposite(name, order)).wait_recv())

    def finish(name):
        each(name, lambda name, order: message(name, order).wait_send())

    for name in messages:
        for sides, _, place in messages[name]:
            slot = place(*[side for _, side in sides])

            @pl.when(jnp.logical_not(near_all(sides)))
            def _():
                slot[...] = jnp.zeros(slot.shape, F32)

    lane = lax.broadcasted_iota(jnp.int32, (cy, cz), 1)
    lane1 = lax.broadcasted_iota(jnp.int32, (1, cz), 1)
    lane8 = lax.broadcasted_iota(jnp.int32, (8, cz), 1)
    row = lax.broadcasted_iota(jnp.int32, (cy, cz), 0)
    row8 = lax.broadcasted_iota(jnp.int32, (8, cz), 0)
    layer = lax.broadcasted_iota(jnp.int32, (cx, cz), 0)
    lane_x = lax.broadcasted_iota(jnp.int32, (cx, cz), 1)
    right_half = lane >= cz // 2
    odd = lane % 2 == 1
    ends = (lane == 0) | (lane == cz - 1)

    def turn(values, by, axis=1):
        by = by % values.shape[axis]
        return values if by == 0 else pltpu.roll(values, by, axis=axis)

    loads[0].wait()
    for copy in loads[3:]:
        copy.wait()
    pair = (
        lax.broadcasted_iota(jnp.int32, (cz, cz), 0) // 2
        == lax.broadcasted_iota(jnp.int32, (cz, cz), 1) % (cz // 2)
    )
    pair = jnp.where(pair, 0.25, 0.0).astype(jnp.bfloat16)
    for b in range(blocks):
        sums_v[b * cy:(b + 1) * cy] = (
            face_v[b, pl.ds(0, cy, stride=2), :] + face_v[b, pl.ds(1, cy, stride=2), :]
        )
    whole = sums_v[...]
    high = whole.astype(jnp.bfloat16)
    rest = whole - high.astype(F32)
    middle = rest.astype(jnp.bfloat16)
    low = (rest - middle.astype(F32)).astype(jnp.bfloat16)
    sums_v[...] = (
        jnp.dot(low, pair, preferred_element_type=F32)
        + jnp.dot(middle, pair, preferred_element_type=F32)
    ) + jnp.dot(high, pair, preferred_element_type=F32)

    target = [rank_ref[b] for b in range(blocks)]
    alive = [live_ref[0, 0, 0] > b for b in range(blocks)]
    position = []
    for b in range(blocks):
        count = jnp.int32(0)
        for before in range(b):
            count = count + jnp.where((target[before] == target[b]) & alive[before], 1, 0)
        position.append(count)
    for k in range(group):
        dest = lax.rem(at["gx"] + k, group)
        total = jnp.zeros((cy, cz), F32)
        tags = jnp.full((1, cz), -1.0, F32)
        for b in range(blocks):
            code = jnp.where(alive[b] & (target[b] == dest), position[b], CAP)
            left, right = jnp.where(code == 0, 1.0, 0.0), jnp.where(code == 1, 1.0, 0.0)
            weight = jnp.where(lane1 < cz // 2, left, right)
            tag = tile_ref[b].astype(F32)
            tags = jnp.where(weight > 0.5, tag, tags)
            values = sums_v[b * cy:(b + 1) * cy]
            total = total + values * jnp.where(right_half, right, left)
        (recv_v if k == 0 else send_v)[k] = total
        (rtag_v if k == 0 else stag_v)[k] = tags

    pl.semaphore_wait(barrier, greeted)
    exchanges = []
    for k in range(1, group):
        for order, (src, dst) in enumerate(((send_v, recv_v), (stag_v, rtag_v))):
            copy = pltpu.make_async_remote_copy(
                src_ref=src.at[k], dst_ref=dst.at[k],
                send_sem=a2a_send.at[order, k], recv_sem=a2a_recv.at[order, k],
                device_id=beside({"gx": k}), device_id_type=MESH,
            )
            copy.start()
            exchanges.append(copy)
    greet(relay_sem.at[0])
    loads[1].wait()
    loads[2].wait()

    for x in range(cx):
        for place, y in enumerate((0, 1, cy - 2, cy - 1)):
            rows_v[place, x:x + 1] = load_v[x, y:y + 1]
        for place, y in enumerate((0, cy - 1)):
            drows_v[place, x:x + 1] = diag_v[x, y:y + 1]
    outer, inner, outer_diag = (jnp.zeros((cy, cz), F32) for _ in range(3))
    for x in range(cx):
        plane = load_v[x]
        mine = lane // 2 == x
        outer = jnp.where(mine, turn(plane, 2 * x + 1), outer)
        outer_diag = jnp.where(mine, turn(diag_v[x], 2 * x + 1), outer_diag)
        second = jnp.where(odd, turn(plane, 2 * x), turn(plane, 2 * x + 2))
        inner = jnp.where(mine, second, inner)
    cols_v[0], cols_v[1], cols_v[2] = outer, inner, outer_diag

    for relay in range(relays):
        pl.semaphore_wait(relay_sem.at[relay], greeted)
        if relay < relays - 1:
            greet(relay_sem.at[relay + 1])
    for copy in exchanges:
        copy.wait_recv()

    for k in range(group):
        turned_v[k] = pltpu.roll(recv_v[k], cz // 2, axis=1)
    sources = []
    for k in range(group):
        tags = rtag_v[k]
        swapped = pltpu.roll(jnp.broadcast_to(tags, (8, cz)), cz // 2, axis=1)[:1]
        sources += [(recv_v.at[k], tags), (turned_v.at[k], swapped)]
    half1 = jnp.where(lane1 >= cz // 2, 1, 0)

    def scatter(x):
        want = (2 * x + half1).astype(F32)
        plane = load_v[x]
        for values, tags in sources:
            plane = plane + jnp.where(tags == want, values[...], 0.0)
        load_v[x] = plane

    def inside(src, x):
        plane = src[x]
        around = jnp.where(lane == 0, 0.0, pltpu.roll(plane, 1, axis=1))
        around = around + jnp.where(lane == cz - 1, 0.0, pltpu.roll(plane, cz - 1, axis=1))
        around = around + jnp.where(row == 0, 0.0, pltpu.roll(plane, 1, axis=0))
        around = around + jnp.where(row == cy - 1, 0.0, pltpu.roll(plane, cy - 1, axis=0))
        if x > 0:
            around = around + src[x - 1]
        if x < cx - 1:
            around = around + src[x + 1]
        return diag_v[x] * plane - around

    for x in (0, 1, cx - 2, cx - 1):
        scatter(x)
    for x in (0, cx - 1):
        p_v[x] = inside(load_v, x)
    send("x")

    want = (2 * layer + jnp.where(lane_x >= cz // 2, 1, 0)).astype(F32)
    faces = [rows_v[place] for place in range(4)]
    for values, tags in sources:
        hit = jnp.broadcast_to(tags, (cx, cz)) == want
        for place, y in enumerate((0, 1, cy - 2, cy - 1)):
            spread = jnp.broadcast_to(values[y:y + 1], (cx, cz))
            faces[place] = faces[place] + jnp.where(hit, spread, 0.0)
    for side in range(2):
        face, second = faces[3 * side], faces[1 + side]
        around = jnp.where(lane_x == 0, 0.0, pltpu.roll(face, 1, axis=1)) + second
        around = around + jnp.where(lane_x == cz - 1, 0.0, pltpu.roll(face, cz - 1, axis=1))
        around = around + jnp.where(layer == 0, 0.0, pltpu.roll(face, 1, axis=0))
        around = around + jnp.where(layer == cx - 1, 0.0, pltpu.roll(face, cx - 1, axis=0))
        ysend_v[side, 0] = face
        ysend_v[side, 1] = drows_v[side] * face - around
        for s in range(2):
            xy_v[2 * s + side] = face[(cx - 1) * s:(cx - 1) * s + 1]
    send("y")

    outer, inner = cols_v[0], cols_v[1]
    own_tile = (lane + 1 - 2 * (lane % 2)).astype(F32)
    for values, tags in sources:
        first = jnp.broadcast_to(tags[:, :1], (1, cz))
        last = jnp.broadcast_to(tags[:, cz - 1:], (1, cz))
        tag = jnp.where(lane1 % 2 == 1, first, last)
        hit = jnp.broadcast_to(tag, (cy, cz)) == own_tile
        field = values[...]
        for depth in range(2):
            low_z = jnp.broadcast_to(field[:, depth:depth + 1], (cy, cz))
            high_z = jnp.broadcast_to(field[:, cz - 1 - depth:cz - depth], (cy, cz))
            added = jnp.where(hit, jnp.where(odd, low_z, high_z), 0.0)
            if depth == 0:
                outer = outer + added
            else:
                inner = inner + added
    cols_v[0] = outer
    around = jnp.where(row == 0, 0.0, pltpu.roll(outer, 1, axis=0)) + inner
    around = around + jnp.where(row == cy - 1, 0.0, pltpu.roll(outer, cy - 1, axis=0))
    around = around + jnp.where(lane < 2, 0.0, turn(outer, 2))
    around = around + jnp.where(lane >= 2 * cx - 2, 0.0, turn(outer, -2))
    image = cols_v[2] * outer - around
    both = jnp.where(lane < 2 * cx, outer, turn(image, 2 * cx))
    both = jnp.where(lane < 4 * cx, both, 0.0)
    rows = cy // folds
    folded = both[:rows]
    for part in range(1, folds):
        folded = folded + turn(both[part * rows:(part + 1) * rows], 4 * cx * part)
    zsend_v[...] = folded
    send("z")
    edge = jnp.zeros((8, cz), F32)
    for part in range(cy // 8):
        piece = outer[8 * part:8 * part + 8]
        piece = jnp.where(lane8 < 2, piece, turn(piece, 4 - 2 * cx))
        edge = jnp.where(lane8 // 4 == part, turn(piece, 4 * part), edge)
    xz_v[...] = edge
    yz_v[0], yz_v[1] = outer[:1], outer[cy - 1:]
    send("corner")

    def fold(acc, values):
        for part in range(cy // 8):
            acc = acc + values[8 * part:8 * part + 8]
        return acc

    for x in range(2, cx - 2):
        scatter(x)
    for x in range(1, cx - 1):
        p_v[x] = inside(load_v, x)
    acc = [jnp.zeros((8, cz), F32) for _ in range(4)]
    for x in range(cx):
        acc[0] = fold(acc[0], load_v[x] * load_v[x])

    def rim(plane, first, last):
        top = plane[:8] - jnp.where(row8 == 0, first, 0.0)
        bottom = plane[cy - 8:] - jnp.where(row8 == 7, last, 0.0)
        return jnp.concatenate([top, plane[8:cy - 8], bottom], axis=0)

    for name in ("x", "y", "z"):
        receive(name)
    finish("x")
    lane_f = lax.broadcasted_iota(jnp.int32, (rows, cz), 1)
    merged = jnp.where(lane_f % 2 == 0, hz_v[0], turn(hz_v[1], -2))
    for x in range(cx):
        sides = jnp.concatenate([turn(merged, -4 * cx * f - 2 * x) for f in range(folds)], axis=0)
        plane = p_v[x] - jnp.where(ends, sides, 0.0)
        plane = rim(plane, hy_v[0, 0, x:x + 1], hy_v[1, 0, x:x + 1])
        if x == 0:
            plane = plane - hx_v[0, 0]
        if x == cx - 1:
            plane = plane - hx_v[1, 0]
        p_v[x] = plane
        acc[1] = fold(acc[1], plane * load_v[x])
        acc[2] = fold(acc[2], plane * plane)
    for x in range(cx):
        q_v[x] = inside(p_v, x)

    receive("corner")
    there = {
        (axis, side): jnp.where(near(axis, side), 1.0, 0.0) for axis in AXES for side in range(2)
    }
    y_halo = []
    for side in range(2):
        halo = hy_v[side, 1] - there["gy", side] * ysend_v[side, 0]
        halo = halo - jnp.where(layer == 0, 2.0 * hxy_v[side], 0.0)
        y_halo.append(halo - jnp.where(layer == cx - 1, 2.0 * hxy_v[2 + side], 0.0))
    z_halo = jnp.concatenate([turn(merged, -4 * cx * f - 2 * cx) for f in range(folds)], axis=0)
    own = jnp.where(odd, there["gz", 1], there["gz", 0])
    z_halo = z_halo - own * turn(cols_v[0], -1)
    even1 = lane1 % 2 == 0
    z_halo = rim(z_halo, *(
        2.0 * jnp.where(
            even1, hyz_v[2 * side],
            turn(jnp.broadcast_to(hyz_v[2 * side + 1], (8, cz)), -2)[:1],
        )
        for side in range(2)
    ))
    code = lane8 % 4
    behind = jnp.where(code == 2, hxz_v[0], hxz_v[2])
    ahead = turn(jnp.where(code == 3, hxz_v[1], hxz_v[3]), -2)
    edge = jnp.where(lane8 % 2 == 0, behind, ahead)
    pieces = []
    for part in range(cy // 8):
        first = turn(edge, -4 * part - 2)
        last = turn(edge, 2 * cx - 2 - 4 * part)
        added = jnp.where((lane8 == 0) | (lane8 == cz - 1), first, 0.0)
        added = jnp.where((lane8 == 2 * cx - 2) | (lane8 == 2 * cx - 3), last, added)
        pieces.append(z_halo[8 * part:8 * part + 8] - 2.0 * added)
    z_halo = jnp.concatenate(pieces, axis=0)
    for x in range(cx):
        plane = q_v[x] - jnp.where(ends, turn(z_halo, -2 * x), 0.0)
        plane = rim(plane, y_halo[0][x:x + 1], y_halo[1][x:x + 1])
        for side in range(2):
            if x == (cx - 1) * side:
                plane = plane - hx_v[side, 1] + there["gx", side] * load_v[x]
        q_v[x] = plane
        acc[3] = fold(acc[3], plane * p_v[x])

    mine = jnp.zeros((8, cz), F32)
    for order in range(4):
        mine = jnp.where(row8 == order, jnp.sum(acc[order], axis=0, keepdims=True), mine)
    mine = mine + pltpu.roll(mine, cz // 2, axis=1)
    mine = mine + pltpu.roll(mine, cz // 4, axis=1)
    own = row8 == lane8 // (cz // 4)
    mine = jnp.sum(jnp.where(own, mine, 0.0), axis=0, keepdims=True)
    slot = 0
    waiting = []
    for order, axes in enumerate(stages):
        part_v[order] = mine
        copies = []
        for offset in offsets_of(sizes, axes):
            copy = pltpu.make_async_remote_copy(
                src_ref=part_v.at[order], dst_ref=gath_v.at[slot],
                send_sem=red_send.at[slot], recv_sem=red_recv.at[slot],
                device_id=beside(offset), device_id_type=MESH,
            )
            copy.start()
            copies.append((slot, copy))
            slot += 1
        for at_slot, copy in copies:
            copy.wait_recv()
            mine = mine + gath_v[at_slot]
        waiting += [copy for _, copy in copies]

    sums = jnp.sum(jnp.where(own, mine, 0.0), axis=1, keepdims=True)
    s0, s1, s2, s3 = (sums[n:n + 1] for n in range(4))
    step = 6.0 * s0 + s1
    a = s0 / step
    c = s1 / step
    norm = c * c * s0 - 2.0 * a * c * s1 + a * a * s2
    e = c + norm / s0
    curve = 6.0 * (e * e * s0 - 2.0 * e * a * s1 + a * a * s2) + (
        e * e * s1 - 2.0 * e * a * s2 + a * a * s3
    )
    b = norm / curve
    x_load, x_p = a + b * e, b * a
    r_load, r_p, r_q = c - 6.0 * b * e, a + b * (e - 6.0 * a), b * a
    for order, value in enumerate((x_load, x_p, r_load, r_p, r_q)):
        coef_ref[order:order + 1] = jnp.broadcast_to(value, (1, cz))
    for copy in exchanges + waiting:
        copy.wait_send()
    for name in ("y", "z", "corner"):
        finish(name)


def combine(load_ref, p_ref, q_ref, coef_ref, x_hbm, r_hbm, x_v, r_v, sem):
    cx = load_ref.shape[0]
    x_load, x_p, r_load, r_p, r_q = (coef_ref[n:n + 1] for n in range(5))
    pieces = sem.shape[1]
    copies = []
    for piece in range(pieces):
        first, last = cx * piece // pieces, cx * (piece + 1) // pieces
        for x in range(first, last):
            load, p = load_ref[x], p_ref[x]
            x_v[x] = x_load * load - x_p * p
            r_v[x] = r_load * load - r_p * p + r_q * q_ref[x]
        span = pl.ds(first, last - first)
        for number, (src, dst) in enumerate(((x_v, x_hbm), (r_v, r_hbm))):
            copy = pltpu.make_async_copy(src.at[span], dst.at[span], sem.at[number, piece])
            copy.start()
            copies.append(copy)
    for copy in copies:
        copy.wait()


def combined(load, p, q, coef):
    cx, cy, cz = load.shape
    box = jax.ShapeDtypeStruct((cx, cy, cz), F32)
    vmem, hbm = (pl.BlockSpec(memory_space=space) for space in (pltpu.VMEM, pltpu.HBM))
    return pl.pallas_call(
        combine,
        out_shape=(box, box),
        in_specs=[vmem] * 4,
        out_specs=(hbm, hbm),
        scratch_shapes=[pltpu.VMEM((cx, cy, cz), F32)] * 2 + [pltpu.SemaphoreType.DMA((2, 4))],
    )(*(pltpu.with_memory_space_constraint(a, pltpu.VMEM) for a in (load, p, q, coef)))


def per_device(sizes, face_blocks, owner_rank, owner_tile, live_count, right_side, diagonal):
    blocks = face_blocks.shape[3]
    cx, cy, cz = right_side.shape
    group = sizes["gx"]
    folds = cz // (4 * cx)
    stages = stages_of(sizes)
    relays = relays_of(sizes, stages)
    slots = sum(len(offsets_of(sizes, axes)) for axes in stages)
    vmem, hbm = (pl.BlockSpec(memory_space=space) for space in (pltpu.VMEM, pltpu.HBM))
    box = pltpu.VMEM((cx, cy, cz), F32)
    load, p, q, coef = pl.pallas_call(
        functools.partial(kernel, sizes, stages, relays),
        out_shape=(box, box, box, pltpu.VMEM((8, cz), F32)),
        in_specs=[hbm] * 6,
        out_specs=(vmem, vmem, vmem, vmem),
        scratch_shapes=[
            pltpu.SMEM((blocks,), jnp.int32),
            pltpu.SMEM((blocks,), jnp.int32),
            pltpu.SMEM(live_count.shape, jnp.int32),
            pltpu.VMEM((blocks, 2 * cy, cz), F32),
            pltpu.VMEM((cx, cy, cz), F32),
            pltpu.VMEM((blocks * cy, cz), F32),
            pltpu.VMEM((group, cy, cz), F32),
            pltpu.VMEM((group, 1, cz), F32),
            pltpu.VMEM((group, cy, cz), F32),
            pltpu.VMEM((group, 1, cz), F32),
            pltpu.VMEM((group, cy, cz), F32),
            pltpu.VMEM((4, cx, cz), F32),
            pltpu.VMEM((2, cx, cz), F32),
            pltpu.VMEM((3, cy, cz), F32),
            pltpu.VMEM((2, 2, cy, cz), F32),
            pltpu.VMEM((2, 2, cx, cz), F32),
            pltpu.VMEM((2, 2, cx, cz), F32),
            pltpu.VMEM((cy // folds, cz), F32),
            pltpu.VMEM((2, cy // folds, cz), F32),
            pltpu.VMEM((4, 1, cz), F32),
            pltpu.VMEM((4, 1, cz), F32),
            pltpu.VMEM((2, 1, cz), F32),
            pltpu.VMEM((4, 1, cz), F32),
            pltpu.VMEM((8, cz), F32),
            pltpu.VMEM((4, 8, cz), F32),
            pltpu.VMEM((len(stages), 1, cz), F32),
            pltpu.VMEM((slots, 1, cz), F32),
            pltpu.SemaphoreType.DMA((6,)),
            pltpu.SemaphoreType.DMA((2, group)),
            pltpu.SemaphoreType.DMA((2, group)),
            pltpu.SemaphoreType.REGULAR((relays,)),
            pltpu.SemaphoreType.DMA((20,)),
            pltpu.SemaphoreType.DMA((20,)),
            pltpu.SemaphoreType.DMA((slots,)),
            pltpu.SemaphoreType.DMA((slots,)),
        ],
        compiler_params=pltpu.CompilerParams(collective_id=0, has_side_effects=True),
    )(
        owner_rank.reshape(blocks), owner_tile.reshape(blocks),
        live_count,
        face_blocks.reshape(blocks, 2 * cy, cz), right_side, diagonal,
    )
    return combined(load, p, q, coef)


def solution(mesh):
    sizes = dict(mesh.shape)
    return jax.shard_map(
        functools.partial(per_device, sizes),
        mesh=mesh,
        in_specs=(
            P("gx", "gy", "gz", None, None),
            P("gx", "gy", "gz", None, None),
            P("gx", "gy", "gz", None),
            P("gx", "gy", "gz"),
            P("gx", "gy", "gz"),
            P("gx", "gy", "gz"),
        ),
        out_specs=(P("gx", "gy", "gz"), P("gx", "gy", "gz")),
        check_vma=False,
    )
```

```python
import functools
import math

import jax
import jax.numpy as jnp
from jax import lax
from jax.experimental import pallas as pl
from jax.experimental.pallas import tpu as pltpu
from jax.sharding import PartitionSpec as P

CAP = 2
AXES = ("gx", "gy", "gz")
MESH = pl.DeviceIdType.MESH
F32 = jnp.float32


def offsets_of(sizes, axes):
    found = [()]
    for axis in axes:
        found = [done + (step,) for done in found for step in range(sizes[axis])]
    return [dict(zip(axes, steps)) for steps in found if any(steps)]


def stages_of(sizes):
    stages = []
    for axis in ("gx", "gz", "gy"):
        if stages and math.prod(sizes[a] for a in stages[-1] + [axis]) <= 32:
            stages[-1].append(axis)
        else:
            stages.append([axis])
    return stages


def relays_of(sizes, stages):
    reach = max(
        sum(1 if axis == "gx" else sizes[axis] - 1 for axis in axes if sizes[axis] > 1)
        for axes in stages
    )
    return max(1, reach - 2)


def kernel(
    sizes, stages, relays,
    rank_hbm, tile_hbm, live_hbm, face_hbm, right_hbm, diag_hbm,
    load_v, p_v, q_v, coef_ref,
    rank_ref, tile_ref, live_ref, face_v, diag_v, sums_v,
    send_v, stag_v, recv_v, rtag_v, turned_v, rows_v, drows_v, cols_v,
    hx_v, ysend_v, hy_v, zsend_v, hz_v, xy_v, hxy_v, yz_v, hyz_v, xz_v, hxz_v, part_v, gath_v,
    in_sem, a2a_send, a2a_recv, relay_sem, halo_send, halo_recv, red_send, red_recv,
):
    cx, cy, cz = load_v.shape
    blocks = face_v.shape[0]
    group = sizes["gx"]
    folds = cy // zsend_v.shape[0]
    at = {axis: lax.axis_index(axis) for axis in AXES}

    def near(axis, side):
        return at[axis] > 0 if side == 0 else at[axis] < sizes[axis] - 1

    def beside(offset):
        return {a: lax.rem(at[a] + s, sizes[a]) for a, s in offset.items() if s}

    def near_all(sides):
        found = near(*sides[0])
        for axis, side in sides[1:]:
            found = found & near(axis, side)
        return found

    loads = [
        pltpu.make_async_copy(face_hbm, face_v, in_sem.at[0]),
        pltpu.make_async_copy(right_hbm, load_v, in_sem.at[1]),
        pltpu.make_async_copy(diag_hbm, diag_v, in_sem.at[2]),
        pltpu.make_async_copy(live_hbm, live_ref, in_sem.at[3]),
        pltpu.make_async_copy(rank_hbm, rank_ref, in_sem.at[4]),
        pltpu.make_async_copy(tile_hbm, tile_ref, in_sem.at[5]),
    ]
    for copy in loads:
        copy.start()

    def greet(semaphore):
        for k in range(1, group):
            pl.semaphore_signal(
                semaphore, inc=1, device_id=beside({"gx": k}), device_id_type=MESH
            )
        for axis in ("gy", "gz"):
            for side in range(2):
                @pl.when(near(axis, side))
                def _():
                    pl.semaphore_signal(
                        semaphore, inc=1, device_id={axis: at[axis] + 2 * side - 1},
                        device_id_type=MESH,
                    )

    greeted = jnp.int32(group - 1)
    for axis in ("gy", "gz"):
        for side in range(2):
            greeted = greeted + jnp.where(near(axis, side), 1, 0)
    barrier = pltpu.get_barrier_semaphore()
    greet(barrier)

    messages = {"x": [], "z": [], "y": [], "xy": [], "xz": [], "yz": []}
    places = {"x": hx_v, "y": hy_v, "z": hz_v, "xy": hxy_v, "xz": hxz_v, "yz": hyz_v}
    kinds = list(messages)
    for s in range(2):
        end = (cx - 1) * s
        messages["x"].append(((("gx", s),), load_v.at[end], lambda s: hx_v.at[s, 0]))
        messages["x"].append(((("gx", s),), p_v.at[end], lambda s: hx_v.at[s, 1]))
        messages["y"].append(((("gy", s),), ysend_v.at[s], lambda s: hy_v.at[s]))
        messages["z"].append(((("gz", s),), zsend_v, lambda s: hz_v.at[s]))
        for t in range(2):
            messages["xy"].append(
                ((("gx", s), ("gy", t)), xy_v.at[2 * s + t], lambda s, t: hxy_v.at[2 * s + t])
            )
            messages["xz"].append(
                ((("gx", s), ("gz", t)), xz_v, lambda s, t: hxz_v.at[2 * s + t])
            )
            messages["yz"].append(
                ((("gy", s), ("gz", t)), yz_v.at[s], lambda s, t: hyz_v.at[2 * s + t])
            )

    def send(name):
        for sides, src, place in messages[name]:
            @pl.when(near_all(sides))
            def _():
                pltpu.make_async_remote_copy(
                    src_ref=src, dst_ref=place(*[1 - side for _, side in sides]),
                    send_sem=halo_send.at[kinds.index(name)],
                    recv_sem=halo_recv.at[kinds.index(name)],
                    device_id={
                        axis: lax.rem(at[axis] + (1 if side else sizes[axis] - 1), sizes[axis])
                        for axis, side in sides
                    },
                    device_id_type=MESH,
                ).start()

    def settle(name, act):
        count = jnp.int32(1)
        for axis, _ in messages[name][0][0]:
            count = count * sum(jnp.where(near(axis, side), 1, 0) for side in range(2))
        for found in (1, 2, 4)[:places[name].shape[0] // 2 + 1]:
            @pl.when(count == found)
            def _():
                slots = places[name].at[pl.ds(0, found)]
                act(pltpu.make_async_remote_copy(
                    src_ref=slots, dst_ref=slots,
                    send_sem=halo_send.at[kinds.index(name)],
                    recv_sem=halo_recv.at[kinds.index(name)],
                    device_id=beside({"gx": 1}), device_id_type=MESH,
                ))

    def receive(name):
        settle(name, lambda copy: copy.wait_recv())

    def finish(name):
        settle(name, lambda copy: copy.wait_send())

    for name in messages:
        for sides, _, place in messages[name]:
            slot = place(*[side for _, side in sides])

            @pl.when(jnp.logical_not(near_all(sides)))
            def _():
                slot[...] = jnp.zeros(slot.shape, F32)

    lane = lax.broadcasted_iota(jnp.int32, (cy, cz), 1)
    lane1 = lax.broadcasted_iota(jnp.int32, (1, cz), 1)
    lane8 = lax.broadcasted_iota(jnp.int32, (8, cz), 1)
    row = lax.broadcasted_iota(jnp.int32, (cy, cz), 0)
    row8 = lax.broadcasted_iota(jnp.int32, (8, cz), 0)
    layer = lax.broadcasted_iota(jnp.int32, (cx, cz), 0)
    lane_x = lax.broadcasted_iota(jnp.int32, (cx, cz), 1)
    right_half = lane >= cz // 2
    odd = lane % 2 == 1
    ends = (lane == 0) | (lane == cz - 1)

    def turn(values, by, axis=1):
        by = by % values.shape[axis]
        return values if by == 0 else pltpu.roll(values, by, axis=axis)

    loads[0].wait()
    for copy in loads[3:]:
        copy.wait()
    pair = (
        lax.broadcasted_iota(jnp.int32, (cz, cz), 0) // 2
        == lax.broadcasted_iota(jnp.int32, (cz, cz), 1) % (cz // 2)
    )
    pair = jnp.where(pair, 0.25, 0.0).astype(jnp.bfloat16)
    for b in range(blocks):
        sums_v[b * cy:(b + 1) * cy] = (
            face_v[b, pl.ds(0, cy, stride=2), :] + face_v[b, pl.ds(1, cy, stride=2), :]
        )
    whole = sums_v[...]
    high = whole.astype(jnp.bfloat16)
    rest = whole - high.astype(F32)
    middle = rest.astype(jnp.bfloat16)
    low = (rest - middle.astype(F32)).astype(jnp.bfloat16)
    sums_v[...] = (
        jnp.dot(low, pair, preferred_element_type=F32)
        + jnp.dot(middle, pair, preferred_element_type=F32)
    ) + jnp.dot(high, pair, preferred_element_type=F32)

    target = [rank_ref[b] for b in range(blocks)]
    alive = [live_ref[0, 0, 0] > b for b in range(blocks)]
    position = []
    for b in range(blocks):
        count = jnp.int32(0)
        for before in range(b):
            count = count + jnp.where((target[before] == target[b]) & alive[before], 1, 0)
        position.append(count)
    for k in range(group):
        dest = lax.rem(at["gx"] + k, group)
        total = jnp.zeros((cy, cz), F32)
        tags = jnp.full((1, cz), -1.0, F32)
        for b in range(blocks):
            code = jnp.where(alive[b] & (target[b] == dest), position[b], CAP)
            left, right = jnp.where(code == 0, 1.0, 0.0), jnp.where(code == 1, 1.0, 0.0)
            weight = jnp.where(lane1 < cz // 2, left, right)
            tag = tile_ref[b].astype(F32)
            tags = jnp.where(weight > 0.5, tag, tags)
            values = sums_v[b * cy:(b + 1) * cy]
            total = total + values * jnp.where(right_half, right, left)
        (recv_v if k == 0 else send_v)[k] = total
        (rtag_v if k == 0 else stag_v)[k] = tags

    pl.semaphore_wait(barrier, greeted)
    boxes = ((send_v, recv_v), (stag_v, rtag_v))

    def exchange(order, slots, k):
        src, dst = boxes[order]
        return pltpu.make_async_remote_copy(
            src_ref=src.at[slots], dst_ref=dst.at[slots],
            send_sem=a2a_send.at[order], recv_sem=a2a_recv.at[order],
            device_id=beside({"gx": k}), device_id_type=MESH,
        )

    for k in range(1, group):
        for order in range(2):
            exchange(order, pl.ds(k, 1), k).start()
    arrivals = [exchange(order, pl.ds(1, group - 1), 1) for order in range(2)] if group > 1 else []
    greet(relay_sem.at[0])
    loads[1].wait()
    loads[2].wait()

    for x in range(cx):
        for place, y in enumerate((0, 1, cy - 2, cy - 1)):
            rows_v[place, x:x + 1] = load_v[x, y:y + 1]
        for place, y in enumerate((0, cy - 1)):
            drows_v[place, x:x + 1] = diag_v[x, y:y + 1]
    outer, inner, outer_diag = (jnp.zeros((cy, cz), F32) for _ in range(3))
    for x in range(cx):
        plane = load_v[x]
        mine = lane // 2 == x
        outer = jnp.where(mine, turn(plane, 2 * x + 1), outer)
        outer_diag = jnp.where(mine, turn(diag_v[x], 2 * x + 1), outer_diag)
        second = jnp.where(odd, turn(plane, 2 * x), turn(plane, 2 * x + 2))
        inner = jnp.where(mine, second, inner)
    cols_v[0], cols_v[1], cols_v[2] = outer, inner, outer_diag

    for relay in range(relays):
        pl.semaphore_wait(relay_sem.at[relay], greeted)
        if relay < relays - 1:
            greet(relay_sem.at[relay + 1])
    for copy in arrivals:
        copy.wait_recv()

    for k in range(group):
        turned_v[k] = pltpu.roll(recv_v[k], cz // 2, axis=1)
    sources = []
    for k in range(group):
        tags = rtag_v[k]
        swapped = pltpu.roll(jnp.broadcast_to(tags, (8, cz)), cz // 2, axis=1)[:1]
        sources += [(recv_v.at[k], tags), (turned_v.at[k], swapped)]
    half1 = jnp.where(lane1 >= cz // 2, 1, 0)

    def scatter(x):
        want = (2 * x + half1).astype(F32)
        plane = load_v[x]
        for values, tags in sources:
            plane = plane + jnp.where(tags == want, values[...], 0.0)
        load_v[x] = plane

    def inside(src, x):
        plane = src[x]
        around = jnp.where(lane == 0, 0.0, pltpu.roll(plane, 1, axis=1))
        around = around + jnp.where(lane == cz - 1, 0.0, pltpu.roll(plane, cz - 1, axis=1))
        around = around + jnp.where(row == 0, 0.0, pltpu.roll(plane, 1, axis=0))
        around = around + jnp.where(row == cy - 1, 0.0, pltpu.roll(plane, cy - 1, axis=0))
        if x > 0:
            around = around + src[x - 1]
        if x < cx - 1:
            around = around + src[x + 1]
        return diag_v[x] * plane - around

    for x in (0, 1, cx - 2, cx - 1):
        scatter(x)
    for x in (0, cx - 1):
        p_v[x] = inside(load_v, x)
    send("x")

    want = (2 * layer + jnp.where(lane_x >= cz // 2, 1, 0)).astype(F32)
    faces = [rows_v[place] for place in range(4)]
    for values, tags in sources:
        hit = jnp.broadcast_to(tags, (cx, cz)) == want
        for place, y in enumerate((0, 1, cy - 2, cy - 1)):
            spread = jnp.broadcast_to(values[y:y + 1], (cx, cz))
            faces[place] = faces[place] + jnp.where(hit, spread, 0.0)
    for side in range(2):
        face, second = faces[3 * side], faces[1 + side]
        around = jnp.where(lane_x == 0, 0.0, pltpu.roll(face, 1, axis=1)) + second
        around = around + jnp.where(lane_x == cz - 1, 0.0, pltpu.roll(face, cz - 1, axis=1))
        around = around + jnp.where(layer == 0, 0.0, pltpu.roll(face, 1, axis=0))
        around = around + jnp.where(layer == cx - 1, 0.0, pltpu.roll(face, cx - 1, axis=0))
        ysend_v[side, 0] = face
        ysend_v[side, 1] = drows_v[side] * face - around
        for s in range(2):
            xy_v[2 * s + side] = face[(cx - 1) * s:(cx - 1) * s + 1]
    send("y")

    outer, inner = cols_v[0], cols_v[1]
    own_tile = (lane + 1 - 2 * (lane % 2)).astype(F32)
    for values, tags in sources:
        first = jnp.broadcast_to(tags[:, :1], (1, cz))
        last = jnp.broadcast_to(tags[:, cz - 1:], (1, cz))
        tag = jnp.where(lane1 % 2 == 1, first, last)
        hit = jnp.broadcast_to(tag, (cy, cz)) == own_tile
        field = values[...]
        for depth in range(2):
            low_z = jnp.broadcast_to(field[:, depth:depth + 1], (cy, cz))
            high_z = jnp.broadcast_to(field[:, cz - 1 - depth:cz - depth], (cy, cz))
            added = jnp.where(hit, jnp.where(odd, low_z, high_z), 0.0)
            if depth == 0:
                outer = outer + added
            else:
                inner = inner + added
    cols_v[0] = outer
    around = jnp.where(row == 0, 0.0, pltpu.roll(outer, 1, axis=0)) + inner
    around = around + jnp.where(row == cy - 1, 0.0, pltpu.roll(outer, cy - 1, axis=0))
    around = around + jnp.where(lane < 2, 0.0, turn(outer, 2))
    around = around + jnp.where(lane >= 2 * cx - 2, 0.0, turn(outer, -2))
    image = cols_v[2] * outer - around
    both = jnp.where(lane < 2 * cx, outer, turn(image, 2 * cx))
    both = jnp.where(lane < 4 * cx, both, 0.0)
    rows = cy // folds
    folded = both[:rows]
    for part in range(1, folds):
        folded = folded + turn(both[part * rows:(part + 1) * rows], 4 * cx * part)
    zsend_v[...] = folded
    send("z")
    edge = jnp.zeros((8, cz), F32)
    for part in range(cy // 8):
        piece = outer[8 * part:8 * part + 8]
        piece = jnp.where(lane8 < 2, piece, turn(piece, 4 - 2 * cx))
        edge = jnp.where(lane8 // 4 == part, turn(piece, 4 * part), edge)
    xz_v[...] = edge
    yz_v[0], yz_v[1] = outer[:1], outer[cy - 1:]
    for name in ("xy", "xz", "yz"):
        send(name)

    def fold(acc, values):
        for part in range(cy // 8):
            acc = acc + values[8 * part:8 * part + 8]
        return acc

    for x in range(2, cx - 2):
        scatter(x)
    for x in range(1, cx - 1):
        p_v[x] = inside(load_v, x)
    acc = [jnp.zeros((8, cz), F32) for _ in range(4)]
    for x in range(cx):
        acc[0] = fold(acc[0], load_v[x] * load_v[x])

    def rim(plane, first, last):
        top = plane[:8] - jnp.where(row8 == 0, first, 0.0)
        bottom = plane[cy - 8:] - jnp.where(row8 == 7, last, 0.0)
        return jnp.concatenate([top, plane[8:cy - 8], bottom], axis=0)

    for name in ("x", "y", "z"):
        receive(name)
    finish("x")
    lane_f = lax.broadcasted_iota(jnp.int32, (rows, cz), 1)
    merged = jnp.where(lane_f % 2 == 0, hz_v[0], turn(hz_v[1], -2))
    for x in range(cx):
        sides = jnp.concatenate([turn(merged, -4 * cx * f - 2 * x) for f in range(folds)], axis=0)
        plane = p_v[x] - jnp.where(ends, sides, 0.0)
        plane = rim(plane, hy_v[0, 0, x:x + 1], hy_v[1, 0, x:x + 1])
        if x == 0:
            plane = plane - hx_v[0, 0]
        if x == cx - 1:
            plane = plane - hx_v[1, 0]
        p_v[x] = plane
        acc[1] = fold(acc[1], plane * load_v[x])
        acc[2] = fold(acc[2], plane * plane)
    for x in range(cx):
        q_v[x] = inside(p_v, x)

    for name in ("xy", "xz", "yz"):
        receive(name)
    there = {
        (axis, side): jnp.where(near(axis, side), 1.0, 0.0) for axis in AXES for side in range(2)
    }
    y_halo = []
    for side in range(2):
        halo = hy_v[side, 1] - there["gy", side] * ysend_v[side, 0]
        halo = halo - jnp.where(layer == 0, 2.0 * hxy_v[side], 0.0)
        y_halo.append(halo - jnp.where(layer == cx - 1, 2.0 * hxy_v[2 + side], 0.0))
    z_halo = jnp.concatenate([turn(merged, -4 * cx * f - 2 * cx) for f in range(folds)], axis=0)
    own = jnp.where(odd, there["gz", 1], there["gz", 0])
    z_halo = z_halo - own * turn(cols_v[0], -1)
    even1 = lane1 % 2 == 0
    z_halo = rim(z_halo, *(
        2.0 * jnp.where(
            even1, hyz_v[2 * side],
            turn(jnp.broadcast_to(hyz_v[2 * side + 1], (8, cz)), -2)[:1],
        )
        for side in range(2)
    ))
    code = lane8 % 4
    behind = jnp.where(code == 2, hxz_v[0], hxz_v[2])
    ahead = turn(jnp.where(code == 3, hxz_v[1], hxz_v[3]), -2)
    edge = jnp.where(lane8 % 2 == 0, behind, ahead)
    pieces = []
    for part in range(cy // 8):
        first = turn(edge, -4 * part - 2)
        last = turn(edge, 2 * cx - 2 - 4 * part)
        added = jnp.where((lane8 == 0) | (lane8 == cz - 1), first, 0.0)
        added = jnp.where((lane8 == 2 * cx - 2) | (lane8 == 2 * cx - 3), last, added)
        pieces.append(z_halo[8 * part:8 * part + 8] - 2.0 * added)
    z_halo = jnp.concatenate(pieces, axis=0)
    for x in range(cx):
        plane = q_v[x] - jnp.where(ends, turn(z_halo, -2 * x), 0.0)
        plane = rim(plane, y_halo[0][x:x + 1], y_halo[1][x:x + 1])
        for side in range(2):
            if x == (cx - 1) * side:
                plane = plane - hx_v[side, 1] + there["gx", side] * load_v[x]
        q_v[x] = plane
        acc[3] = fold(acc[3], plane * p_v[x])

    mine = jnp.zeros((8, cz), F32)
    for order in range(4):
        mine = jnp.where(row8 == order, jnp.sum(acc[order], axis=0, keepdims=True), mine)
    mine = mine + pltpu.roll(mine, cz // 2, axis=1)
    mine = mine + pltpu.roll(mine, cz // 4, axis=1)
    own = row8 == lane8 // (cz // 4)
    mine = jnp.sum(jnp.where(own, mine, 0.0), axis=0, keepdims=True)
    slot = 0
    waiting = []
    for order, axes in enumerate(stages):
        part_v[order] = mine
        offsets = offsets_of(sizes, axes)

        def part(offset, src, dst):
            return pltpu.make_async_remote_copy(
                src_ref=src, dst_ref=dst,
                send_sem=red_send.at[order], recv_sem=red_recv.at[order],
                device_id=beside(offset), device_id_type=MESH,
            )

        for place, offset in enumerate(offsets):
            part(offset, part_v.at[order], gath_v.at[slot + place]).start()
        if offsets:
            span = gath_v.at[pl.ds(slot, len(offsets))]
            waiting.append(part(offsets[0], span, span))
            waiting[-1].wait_recv()
        for place in range(len(offsets)):
            mine = mine + gath_v[slot + place]
        slot += len(offsets)

    sums = jnp.sum(jnp.where(own, mine, 0.0), axis=1, keepdims=True)
    s0, s1, s2, s3 = (sums[n:n + 1] for n in range(4))
    step = 6.0 * s0 + s1
    a = s0 / step
    c = s1 / step
    norm = c * c * s0 - 2.0 * a * c * s1 + a * a * s2
    e = c + norm / s0
    curve = 6.0 * (e * e * s0 - 2.0 * e * a * s1 + a * a * s2) + (
        e * e * s1 - 2.0 * e * a * s2 + a * a * s3
    )
    b = norm / curve
    x_load, x_p = a + b * e, b * a
    r_load, r_p, r_q = c - 6.0 * b * e, a + b * (e - 6.0 * a), b * a
    for order, value in enumerate((x_load, x_p, r_load, r_p, r_q)):
        coef_ref[order:order + 1] = jnp.broadcast_to(value, (1, cz))
    for copy in arrivals + waiting:
        copy.wait_send()
    for name in ("y", "z", "xy", "xz", "yz"):
        finish(name)


def combine(load_ref, p_ref, q_ref, coef_ref, x_hbm, r_hbm, x_v, r_v, sem):
    cx = load_ref.shape[0]
    x_load, x_p, r_load, r_p, r_q = (coef_ref[n:n + 1] for n in range(5))
    pieces = 4
    for piece in range(pieces):
        first, last = cx * piece // pieces, cx * (piece + 1) // pieces
        for x in range(first, last):
            load, p = load_ref[x], p_ref[x]
            x_v[x] = x_load * load - x_p * p
            r_v[x] = r_load * load - r_p * p + r_q * q_ref[x]
        span = pl.ds(first, last - first)
        for number, (src, dst) in enumerate(((x_v, x_hbm), (r_v, r_hbm))):
            pltpu.make_async_copy(src.at[span], dst.at[span], sem.at[number]).start()
    for number, (src, dst) in enumerate(((x_v, x_hbm), (r_v, r_hbm))):
        pltpu.make_async_copy(src, dst, sem.at[number]).wait()


def combined(load, p, q, coef):
    cx, cy, cz = load.shape
    box = jax.ShapeDtypeStruct((cx, cy, cz), F32)
    vmem, hbm = (pl.BlockSpec(memory_space=space) for space in (pltpu.VMEM, pltpu.HBM))
    return pl.pallas_call(
        combine,
        out_shape=(box, box),
        in_specs=[vmem] * 4,
        out_specs=(hbm, hbm),
        scratch_shapes=[pltpu.VMEM((cx, cy, cz), F32)] * 2 + [pltpu.SemaphoreType.DMA((2,))],
    )(*(pltpu.with_memory_space_constraint(a, pltpu.VMEM) for a in (load, p, q, coef)))


def per_device(sizes, face_blocks, owner_rank, owner_tile, live_count, right_side, diagonal):
    blocks = face_blocks.shape[3]
    cx, cy, cz = right_side.shape
    group = sizes["gx"]
    folds = cz // (4 * cx)
    stages = stages_of(sizes)
    relays = relays_of(sizes, stages)
    slots = sum(len(offsets_of(sizes, axes)) for axes in stages)
    vmem, hbm = (pl.BlockSpec(memory_space=space) for space in (pltpu.VMEM, pltpu.HBM))
    box = pltpu.VMEM((cx, cy, cz), F32)
    load, p, q, coef = pl.pallas_call(
        functools.partial(kernel, sizes, stages, relays),
        out_shape=(box, box, box, pltpu.VMEM((8, cz), F32)),
        in_specs=[hbm] * 6,
        out_specs=(vmem, vmem, vmem, vmem),
        scratch_shapes=[
            pltpu.SMEM((blocks,), jnp.int32),
            pltpu.SMEM((blocks,), jnp.int32),
            pltpu.SMEM(live_count.shape, jnp.int32),
            pltpu.VMEM((blocks, 2 * cy, cz), F32),
            pltpu.VMEM((cx, cy, cz), F32),
            pltpu.VMEM((blocks * cy, cz), F32),
            pltpu.VMEM((group, cy, cz), F32),
            pltpu.VMEM((group, 1, cz), F32),
            pltpu.VMEM((group, cy, cz), F32),
            pltpu.VMEM((group, 1, cz), F32),
            pltpu.VMEM((group, cy, cz), F32),
            pltpu.VMEM((4, cx, cz), F32),
            pltpu.VMEM((2, cx, cz), F32),
            pltpu.VMEM((3, cy, cz), F32),
            pltpu.VMEM((2, 2, cy, cz), F32),
            pltpu.VMEM((2, 2, cx, cz), F32),
            pltpu.VMEM((2, 2, cx, cz), F32),
            pltpu.VMEM((cy // folds, cz), F32),
            pltpu.VMEM((2, cy // folds, cz), F32),
            pltpu.VMEM((4, 1, cz), F32),
            pltpu.VMEM((4, 1, cz), F32),
            pltpu.VMEM((2, 1, cz), F32),
            pltpu.VMEM((4, 1, cz), F32),
            pltpu.VMEM((8, cz), F32),
            pltpu.VMEM((4, 8, cz), F32),
            pltpu.VMEM((len(stages), 1, cz), F32),
            pltpu.VMEM((slots, 1, cz), F32),
            pltpu.SemaphoreType.DMA((6,)),
            pltpu.SemaphoreType.DMA((2,)),
            pltpu.SemaphoreType.DMA((2,)),
            pltpu.SemaphoreType.REGULAR((relays,)),
            pltpu.SemaphoreType.DMA((6,)),
            pltpu.SemaphoreType.DMA((6,)),
            pltpu.SemaphoreType.DMA((len(stages),)),
            pltpu.SemaphoreType.DMA((len(stages),)),
        ],
        compiler_params=pltpu.CompilerParams(collective_id=0, has_side_effects=True),
    )(
        owner_rank.reshape(blocks), owner_tile.reshape(blocks),
        live_count,
        face_blocks.reshape(blocks, 2 * cy, cz), right_side, diagonal,
    )
    return combined(load, p, q, coef)


def solution(mesh):
    sizes = dict(mesh.shape)
    return jax.shard_map(
        functools.partial(per_device, sizes),
        mesh=mesh,
        in_specs=(
            P("gx", "gy", "gz", None, None),
            P("gx", "gy", "gz", None, None),
            P("gx", "gy", "gz", None),
            P("gx", "gy", "gz"),
            P("gx", "gy", "gz"),
            P("gx", "gy", "gz"),
        ),
        out_specs=(P("gx", "gy", "gz"), P("gx", "gy", "gz")),
        check_vma=False,
    )
```

```python
import functools
import math

import jax
import jax.numpy as jnp
from jax import lax
from jax.experimental import pallas as pl
from jax.experimental.pallas import tpu as pltpu
from jax.sharding import PartitionSpec as P

CAP = 2
AXES = ("gx", "gy", "gz")
MESH = pl.DeviceIdType.MESH
F32 = jnp.float32


def offsets_of(sizes, axes):
    found = [()]
    for axis in axes:
        found = [done + (step,) for done in found for step in range(sizes[axis])]
    offsets = [dict(zip(axes, steps)) for steps in found if any(steps)]
    return sorted(
        offsets, key=lambda o: -sum(s if a != "gx" else s / sizes[a] for a, s in o.items())
    )


def stages_of(sizes):
    stages = []
    for axis in ("gx", "gz", "gy"):
        if stages and math.prod(sizes[a] for a in stages[-1] + [axis]) <= 32:
            stages[-1].append(axis)
        else:
            stages.append([axis])
    return stages


def relays_of(sizes, stages):
    rounds = 1
    for axes in stages:
        steps = [sizes[axis] - 1 for axis in axes if axis != "gx"]
        single = sum(n % 2 for n in steps) + (1 if "gx" in axes and sizes["gx"] > 1 else 0)
        rounds = max(rounds, 1 + sum(n // 2 for n in steps) + max(0, single - 3))
    return rounds


def kernel(
    sizes, stages, relays,
    rank_hbm, tile_hbm, live_hbm, face_hbm, right_hbm, diag_hbm,
    load_v, p_v, q_v, coef_ref,
    rank_ref, tile_ref, live_ref, face_v, diag_v, sums_v,
    send_v, stag_v, recv_v, rtag_v, turned_v, rows_v, drows_v, cols_v,
    hx_v, ysend_v, hy_v, zsend_v, hz_v, xy_v, hxy_v, yz_v, hyz_v, xz_v, hxz_v, mix_v, part_v, gath_v,
    in_sem, a2a_send, a2a_recv, relay_sem, halo_send, halo_recv, red_send, red_recv,
):
    cx, cy, cz = load_v.shape
    blocks = face_v.shape[0]
    group = sizes["gx"]
    at = {axis: lax.axis_index(axis) for axis in AXES}

    def near(axis, side):
        return at[axis] > 0 if side == 0 else at[axis] < sizes[axis] - 1

    def beside(offset):
        return {a: lax.rem(at[a] + s, sizes[a]) for a, s in offset.items() if s}

    def across(offset):
        where = {}
        for axis, step in offset.items():
            if sizes[axis] & (sizes[axis] - 1):
                where[axis] = lax.rem(at[axis] + step, sizes[axis])
            else:
                where[axis] = at[axis]
                for bit in (1 << n for n in range(sizes[axis].bit_length())):
                    if step & bit:
                        where[axis] = where[axis] + bit - 2 * bit * lax.rem(at[axis] // bit, 2)
        return {axis: index for axis, index in where.items() if offset[axis]}

    def near_all(sides):
        found = near(*sides[0])
        for axis, side in sides[1:]:
            found = found & near(axis, side)
        return found

    loads = [
        pltpu.make_async_copy(face_hbm, face_v, in_sem.at[0]),
        pltpu.make_async_copy(right_hbm, load_v, in_sem.at[1]),
        pltpu.make_async_copy(diag_hbm, diag_v, in_sem.at[2]),
        pltpu.make_async_copy(live_hbm, live_ref, in_sem.at[3]),
        pltpu.make_async_copy(rank_hbm, rank_ref, in_sem.at[4]),
        pltpu.make_async_copy(tile_hbm, tile_ref, in_sem.at[5]),
    ]
    for copy in loads:
        copy.start()

    def within(axis, step):
        return at[axis] + step >= 0 if step < 0 else at[axis] + step < sizes[axis]

    def greet(semaphore, reach=1):
        for k in range(1, group):
            pl.semaphore_signal(
                semaphore, inc=1, device_id=beside({"gx": k}), device_id_type=MESH
            )
        for axis in ("gy", "gz"):
            for step in range(-reach, reach + 1):
                if 0 < abs(step) < sizes[axis]:
                    @pl.when(within(axis, step))
                    def _():
                        pl.semaphore_signal(
                            semaphore, inc=1, device_id={axis: at[axis] + step},
                            device_id_type=MESH,
                        )

    def greeted(reach=1):
        count = jnp.int32(group - 1)
        for axis in ("gy", "gz"):
            for step in range(-reach, reach + 1):
                if 0 < abs(step) < sizes[axis]:
                    count = count + jnp.where(within(axis, step), 1, 0)
        return count

    barrier = pltpu.get_barrier_semaphore()
    greet(barrier)

    messages = {"x": [], "z": [], "y": [], "xy": [], "xz": [], "yz": []}
    places = {"x": hx_v, "y": hy_v, "z": hz_v, "xy": hxy_v, "xz": hxz_v, "yz": hyz_v}
    kinds = list(messages)
    for s in range(2):
        end = (cx - 1) * s
        messages["x"].append(((("gx", s),), load_v.at[end], lambda s: hx_v.at[s, 0]))
        messages["x"].append(((("gx", s),), p_v.at[end], lambda s: hx_v.at[s, 1]))
        messages["y"].append(((("gy", s),), ysend_v.at[s], lambda s: hy_v.at[s]))
        messages["z"].append(((("gz", s),), zsend_v.at[s], lambda s: hz_v.at[s]))
        for t in range(2):
            messages["xy"].append(
                ((("gx", s), ("gy", t)), xy_v.at[2 * s + t], lambda s, t: hxy_v.at[2 * s + t])
            )
            messages["xz"].append(
                ((("gx", s), ("gz", t)), xz_v.at[2 * s + t], lambda s, t: hxz_v.at[2 * s + t])
            )
            messages["yz"].append(
                ((("gy", s), ("gz", t)), yz_v, lambda s, t: hyz_v.at[2 * s + t])
            )

    def send(name):
        for sides, src, place in messages[name]:
            @pl.when(near_all(sides))
            def _():
                pltpu.make_async_remote_copy(
                    src_ref=src, dst_ref=place(*[1 - side for _, side in sides]),
                    send_sem=halo_send.at[kinds.index(name)],
                    recv_sem=halo_recv.at[kinds.index(name)],
                    device_id={
                        axis: lax.rem(at[axis] + (1 if side else sizes[axis] - 1), sizes[axis])
                        for axis, side in sides
                    },
                    device_id_type=MESH,
                ).start()

    def settle(name, act):
        count = jnp.int32(1)
        for axis, _ in messages[name][0][0]:
            count = count * sum(jnp.where(near(axis, side), 1, 0) for side in range(2))
        for found in (1, 2, 4)[:places[name].shape[0] // 2 + 1]:
            @pl.when(count == found)
            def _():
                slots = places[name].at[pl.ds(0, found)]
                act(pltpu.make_async_remote_copy(
                    src_ref=slots, dst_ref=slots,
                    send_sem=halo_send.at[kinds.index(name)],
                    recv_sem=halo_recv.at[kinds.index(name)],
                    device_id=beside({"gx": 1}), device_id_type=MESH,
                ))

    def receive(name):
        settle(name, lambda copy: copy.wait_recv())

    def finish(name):
        settle(name, lambda copy: copy.wait_send())

    for name in messages:
        for sides, _, place in messages[name]:
            slot = place(*[side for _, side in sides])

            @pl.when(jnp.logical_not(near_all(sides)))
            def _():
                slot[...] = jnp.zeros(slot.shape, F32)

    lane = lax.broadcasted_iota(jnp.int32, (cy, cz), 1)
    lane1 = lax.broadcasted_iota(jnp.int32, (1, cz), 1)
    lane8 = lax.broadcasted_iota(jnp.int32, (8, cz), 1)
    row = lax.broadcasted_iota(jnp.int32, (cy, cz), 0)
    row8 = lax.broadcasted_iota(jnp.int32, (8, cz), 0)
    layer = lax.broadcasted_iota(jnp.int32, (cx, cz), 0)
    lane_x = lax.broadcasted_iota(jnp.int32, (cx, cz), 1)
    right_half = lane >= cz // 2
    ends = (lane == 0) | (lane == cz - 1)

    def turn(values, by, axis=1):
        by = by % values.shape[axis]
        return values if by == 0 else pltpu.roll(values, by, axis=axis)

    loads[0].wait()
    for copy in loads[3:]:
        copy.wait()
    pair = (
        lax.broadcasted_iota(jnp.int32, (cz, cz), 0) // 2
        == lax.broadcasted_iota(jnp.int32, (cz, cz), 1) % (cz // 2)
    )
    pair = jnp.where(pair, 0.25, 0.0).astype(jnp.bfloat16)
    for b in range(blocks):
        sums_v[b * cy:(b + 1) * cy] = (
            face_v[b, pl.ds(0, cy, stride=2), :] + face_v[b, pl.ds(1, cy, stride=2), :]
        )
    whole = sums_v[...]
    high = whole.astype(jnp.bfloat16)
    rest = whole - high.astype(F32)
    middle = rest.astype(jnp.bfloat16)
    low = (rest - middle.astype(F32)).astype(jnp.bfloat16)
    column = lax.broadcasted_iota(jnp.int32, (8, cz), 0)
    column = jnp.where(column < 2, column, cz // 2 - 4 + column)
    choice = (lax.broadcasted_iota(jnp.int32, (8, cz), 1) // 2 == column) & (column < cz // 2)
    choice = jnp.where(choice, 0.25, 0.0).astype(jnp.bfloat16)

    def columns_of(values):
        return lax.dot_general(
            choice, values, (((1,), (1,)), ((), ())), preferred_element_type=F32
        )

    columns = columns_of(low) + columns_of(middle) + columns_of(high)
    sums_v[...] = (
        jnp.dot(low, pair, preferred_element_type=F32)
        + jnp.dot(middle, pair, preferred_element_type=F32)
    ) + jnp.dot(high, pair, preferred_element_type=F32)

    target = [rank_ref[b] for b in range(blocks)]
    alive = [live_ref[0, 0, 0] > b for b in range(blocks)]
    position = []
    for b in range(blocks):
        count = jnp.int32(0)
        for before in range(b):
            count = count + jnp.where((target[before] == target[b]) & alive[before], 1, 0)
        position.append(count)
    edges = []
    for b in range(blocks):
        here = columns[:, b // 2 * cz:b // 2 * cz + cz]
        there = pltpu.roll(here, cz // 2, axis=1)
        first, last = (here, there) if b % 2 == 0 else (there, here)
        even = jnp.where(lane1 < cz // 2, first[0:1], last[1:2])
        other = jnp.where(lane1 < cz // 2, first[3:4], last[2:3])
        edges.append(jnp.where(lax.rem(tile_ref[b], 2) == 0, even, other))
    for k in range(group):
        dest = lax.rem(at["gx"] + k, group)
        outer = [jnp.zeros((1, cz), F32) for _ in range(CAP)]
        total = jnp.zeros((cy, cz), F32)
        tags = jnp.full((1, cz), -1.0, F32)
        for b in range(blocks):
            code = jnp.where(alive[b] & (target[b] == dest), position[b], CAP)
            left, right = jnp.where(code == 0, 1.0, 0.0), jnp.where(code == 1, 1.0, 0.0)
            weight = jnp.where(lane1 < cz // 2, left, right)
            tag = tile_ref[b].astype(F32)
            tags = jnp.where(weight > 0.5, tag, tags)
            values = sums_v[b * cy:(b + 1) * cy]
            total = total + values * jnp.where(right_half, right, left)
            outer = [outer[0] + left * edges[b], outer[1] + right * edges[b]]
        (recv_v if k == 0 else send_v)[k] = total
        for place, values in enumerate([tags] + outer):
            (rtag_v if k == 0 else stag_v)[3 * k + place] = values

    pl.semaphore_wait(barrier, greeted())
    boxes = ((send_v, recv_v), (stag_v, rtag_v))

    def exchange(order, slots, k):
        src, dst = boxes[order]
        return pltpu.make_async_remote_copy(
            src_ref=src.at[slots], dst_ref=dst.at[slots],
            send_sem=a2a_send.at[order], recv_sem=a2a_recv.at[order],
            device_id=beside({"gx": k}), device_id_type=MESH,
        )

    for k in range(1, group):
        for order in range(2):
            exchange(order, pl.ds(k * (1, 3)[order], (1, 3)[order]), k).start()
    arrivals = [
        exchange(order, pl.ds(step, step * (group - 1)), 1)
        for order, step in enumerate((1, 3)) if group > 1
    ]
    greet(relay_sem.at[0])
    loads[1].wait()
    loads[2].wait()

    for x in range(cx):
        for place, y in enumerate((0, 1, cy - 2, cy - 1)):
            rows_v[place, x:x + 1] = load_v[x, y:y + 1]
        for place, y in enumerate((0, cy - 1)):
            drows_v[place, x:x + 1] = diag_v[x, y:y + 1]
    upper, lower = jnp.zeros((cy, cz), F32), jnp.zeros((cy, cz), F32)
    for x in range(cx):
        plane, weights = load_v[x], diag_v[x]
        for side in range(2):
            spot = cx * side + x
            upper = jnp.where(lane == spot, turn(plane, spot + side), upper)
            lower = jnp.where(lane == spot, turn(plane, spot + 3 * side - 1), lower)
            spot = spot + 2 * cx
            upper = jnp.where(lane == spot, turn(weights, spot + side), upper)
    cols_v[...] = jnp.concatenate([upper, lower], axis=0).T[:4 * cx]

    for relay in range(relays):
        pl.semaphore_wait(relay_sem.at[relay], greeted(min(relay + 1, 2)))
        if relay < relays - 1:
            greet(relay_sem.at[relay + 1], 2)
    for copy in arrivals:
        copy.wait_recv()

    for k in range(group):
        turned_v[k] = pltpu.roll(recv_v[k], cz // 2, axis=1)
    sources = []
    for k in range(group):
        tags = rtag_v[3 * k]
        swapped = pltpu.roll(jnp.broadcast_to(tags, (8, cz)), cz // 2, axis=1)[:1]
        sources += [(recv_v.at[k], tags), (turned_v.at[k], swapped)]
    half1 = jnp.where(lane1 >= cz // 2, 1, 0)

    def scatter(x):
        want = (2 * x + half1).astype(F32)
        plane = load_v[x]
        for values, tags in sources:
            plane = plane + jnp.where(tags == want, values[...], 0.0)
        load_v[x] = plane

    def inside(src, x):
        plane = src[x]
        around = jnp.where(lane == 0, 0.0, pltpu.roll(plane, 1, axis=1))
        around = around + jnp.where(lane == cz - 1, 0.0, pltpu.roll(plane, cz - 1, axis=1))
        around = around + jnp.where(row == 0, 0.0, pltpu.roll(plane, 1, axis=0))
        around = around + jnp.where(row == cy - 1, 0.0, pltpu.roll(plane, cy - 1, axis=0))
        if x > 0:
            around = around + src[x - 1]
        if x < cx - 1:
            around = around + src[x + 1]
        return diag_v[x] * plane - around

    want = (2 * layer + jnp.where(lane_x >= cz // 2, 1, 0)).astype(F32)
    faces = [rows_v[place] for place in range(4)]
    for values, tags in sources:
        hit = jnp.broadcast_to(tags, (cx, cz)) == want
        for place, y in enumerate((0, 1, cy - 2, cy - 1)):
            spread = jnp.broadcast_to(values[y:y + 1], (cx, cz))
            faces[place] = faces[place] + jnp.where(hit, spread, 0.0)
    for side in range(2):
        face, second = faces[3 * side], faces[1 + side]
        around = jnp.where(lane_x == 0, 0.0, pltpu.roll(face, 1, axis=1)) + second
        around = around + jnp.where(lane_x == cz - 1, 0.0, pltpu.roll(face, cz - 1, axis=1))
        around = around + jnp.where(layer == 0, 0.0, pltpu.roll(face, 1, axis=0))
        around = around + jnp.where(layer == cx - 1, 0.0, pltpu.roll(face, cx - 1, axis=0))
        ysend_v[side, 0] = face
        ysend_v[side, 1] = drows_v[side] * face - around
        for s in range(2):
            xy_v[2 * s + side] = face[(cx - 1) * s:(cx - 1) * s + 1]
    send("xy")
    send("y")

    line = lax.broadcasted_iota(jnp.int32, (2 * cx, cz), 0)
    lane_z = lax.broadcasted_iota(jnp.int32, (2 * cx, cz), 1)
    own_tile = (2 * (line % cx) + line // cx).astype(F32)
    turned = cols_v[:2 * cx]
    for k in range(group):
        tags = rtag_v[3 * k]
        for place in range(CAP):
            tag = tags[:, :1] if place == 0 else tags[:, cz - 1:]
            hit = jnp.broadcast_to(tag, (2 * cx, cz)) == own_tile
            values = jnp.broadcast_to(rtag_v[3 * k + 1 + place], (2 * cx, cz))
            turned = turned + jnp.where(hit, values, 0.0)
    around = jnp.where(lane_z == 0, 0.0, turn(turned, 1)) + turn(turned, cz // 2)
    around = around + jnp.where(lane_z == cy - 1, 0.0, turn(turned, -1))
    around = around + jnp.where(line % cx == 0, 0.0, turn(turned, 1, 0))
    around = around + jnp.where(line % cx == cx - 1, 0.0, turn(turned, -1, 0))
    image = cols_v[2 * cx:] * turned - around
    turned = jnp.where(lane_z < cy, turned, turn(image, cz // 2))
    for side in range(2):
        zsend_v[side] = turned[cx * side:cx * side + cx]
    send("z")
    groups = cx // 8
    tile = jnp.zeros((8, cz), F32)
    for side in range(2):
        for part in range(groups):
            spot = 2 * (groups * side + part)
            piece = turn(ysend_v[side, 0, 8 * part:8 * part + 8], spot + 1)
            tile = jnp.where(lane8 // 2 == spot // 2, piece, tile)
        for s in range(2):
            spot = cx * side + (cx - 1) * s
            xz_v[2 * s + side] = turned[spot:spot + 1]
    yz_v[...] = tile
    for name in ("yz", "xz"):
        send(name)

    for x in (0, 1, cx - 2, cx - 1):
        scatter(x)
    for x in (0, cx - 1):
        p_v[x] = inside(load_v, x)
    send("x")

    def fold(acc, values):
        for part in range(cy // 8):
            acc = acc + values[8 * part:8 * part + 8]
        return acc

    for x in range(2, cx - 2):
        scatter(x)
    for x in range(1, cx - 1):
        p_v[x] = inside(load_v, x)
    acc = [jnp.zeros((8, cz), F32) for _ in range(4)]
    for x in range(cx):
        acc[0] = fold(acc[0], load_v[x] * load_v[x])

    def rim(plane, first, last):
        top = plane[:8] - jnp.where(row8 == 0, first, 0.0)
        bottom = plane[cy - 8:] - jnp.where(row8 == 7, last, 0.0)
        return jnp.concatenate([top, plane[8:cy - 8], bottom], axis=0)

    for name in ("x", "y", "z"):
        receive(name)
    finish("x")
    def columned(halves):
        for side in range(2):
            mix_v[pl.ds(1 - side, cx, stride=2), :] = halves[side]
        columns = mix_v[...].T
        return jnp.concatenate([columns, jnp.zeros((cz, cz - 2 * cx), F32)], axis=1)

    l_halo = columned([hz_v[0], hz_v[1]])[:cy]
    for x in range(cx):
        plane = p_v[x] - jnp.where(ends, turn(l_halo, -2 * x - 1), 0.0)
        plane = rim(plane, hy_v[0, 0, x:x + 1], hy_v[1, 0, x:x + 1])
        if x == 0:
            plane = plane - hx_v[0, 0]
        if x == cx - 1:
            plane = plane - hx_v[1, 0]
        p_v[x] = plane
        acc[1] = fold(acc[1], plane * load_v[x])
        acc[2] = fold(acc[2], plane * plane)
    for x in range(cx):
        q_v[x] = inside(p_v, x)

    for name in ("xy", "xz", "yz"):
        receive(name)
    there = {
        (axis, side): jnp.where(near(axis, side), 1.0, 0.0) for axis in AXES for side in range(2)
    }
    y_halo = []
    for side in range(2):
        halo = hy_v[side, 1] - there["gy", side] * ysend_v[side, 0]
        halo = halo - jnp.where(layer == 0, 2.0 * hxy_v[side], 0.0)
        y_halo.append(halo - jnp.where(layer == cx - 1, 2.0 * hxy_v[2 + side], 0.0))
    halves = []
    for side in range(2):
        halo = hz_v[side] - there["gz", side] * turn(zsend_v[side], cz // 2)
        for s in range(2):
            corner = turn(jnp.broadcast_to(hxz_v[2 * s + side], (8, cz)), cz // 2)[:1]
            halo = halo - jnp.where(layer == (cx - 1) * s, 2.0 * corner, 0.0)
        parts = []
        for part in range(groups):
            piece = halo[8 * part:8 * part + 8]
            for s in range(2):
                spot = 2 * (groups * (1 - s) + part) + side
                goal = cy if s == 0 else 2 * cy - 1
                corner = turn(hyz_v[2 * s + side], goal - spot)
                piece = piece - jnp.where(lane8 == goal, 2.0 * corner, 0.0)
            parts.append(piece)
        halves.append(jnp.concatenate(parts, axis=0))
    z_halo = columned(halves)[cy:2 * cy]
    for x in range(cx):
        plane = q_v[x] - jnp.where(ends, turn(z_halo, -2 * x - 1), 0.0)
        plane = rim(plane, y_halo[0][x:x + 1], y_halo[1][x:x + 1])
        for side in range(2):
            if x == (cx - 1) * side:
                plane = plane - hx_v[side, 1] + there["gx", side] * load_v[x]
        q_v[x] = plane
        acc[3] = fold(acc[3], plane * p_v[x])

    mine = jnp.zeros((8, cz), F32)
    for order in range(4):
        mine = jnp.where(row8 == order, jnp.sum(acc[order], axis=0, keepdims=True), mine)
    mine = mine + pltpu.roll(mine, cz // 2, axis=1)
    mine = mine + pltpu.roll(mine, cz // 4, axis=1)
    own = row8 == lane8 // (cz // 4)
    mine = jnp.sum(jnp.where(own, mine, 0.0), axis=0, keepdims=True)
    slot = 0
    waiting = []
    for order, axes in enumerate(stages):
        part_v[order] = mine
        offsets = offsets_of(sizes, axes)

        def part(offset, src, dst):
            return pltpu.make_async_remote_copy(
                src_ref=src, dst_ref=dst,
                send_sem=red_send.at[order], recv_sem=red_recv.at[order],
                device_id=across(offset), device_id_type=MESH,
            )

        for place, offset in enumerate(offsets):
            part(offset, part_v.at[order], gath_v.at[slot + place]).start()
        if offsets:
            span = gath_v.at[pl.ds(slot, len(offsets))]
            waiting.append(part(offsets[0], span, span))
            waiting[-1].wait_recv()
        for place in range(len(offsets)):
            mine = mine + gath_v[slot + place]
        slot += len(offsets)

    sums = jnp.sum(jnp.where(own, mine, 0.0), axis=1, keepdims=True)
    s0, s1, s2, s3 = (sums[n:n + 1] for n in range(4))
    step = 6.0 * s0 + s1
    a = s0 / step
    c = s1 / step
    norm = c * c * s0 - 2.0 * a * c * s1 + a * a * s2
    e = c + norm / s0
    curve = 6.0 * (e * e * s0 - 2.0 * e * a * s1 + a * a * s2) + (
        e * e * s1 - 2.0 * e * a * s2 + a * a * s3
    )
    b = norm / curve
    x_load, x_p = a + b * e, b * a
    r_load, r_p, r_q = c - 6.0 * b * e, a + b * (e - 6.0 * a), b * a
    for order, value in enumerate((x_load, x_p, r_load, r_p, r_q)):
        coef_ref[order:order + 1] = jnp.broadcast_to(value, (1, cz))
    for copy in arrivals + waiting:
        copy.wait_send()
    for name in ("y", "z", "xy", "xz", "yz"):
        finish(name)


def combine(load_ref, p_ref, q_ref, coef_ref, x_hbm, r_hbm, x_v, r_v, sem):
    cx = load_ref.shape[0]
    x_load, x_p, r_load, r_p, r_q = (coef_ref[n:n + 1] for n in range(5))
    pieces = 4
    for piece in range(pieces):
        first, last = cx * piece // pieces, cx * (piece + 1) // pieces
        for x in range(first, last):
            load, p = load_ref[x], p_ref[x]
            x_v[x] = x_load * load - x_p * p
            r_v[x] = r_load * load - r_p * p + r_q * q_ref[x]
        span = pl.ds(first, last - first)
        for number, (src, dst) in enumerate(((x_v, x_hbm), (r_v, r_hbm))):
            pltpu.make_async_copy(src.at[span], dst.at[span], sem.at[number]).start()
    for number, (src, dst) in enumerate(((x_v, x_hbm), (r_v, r_hbm))):
        pltpu.make_async_copy(src, dst, sem.at[number]).wait()


def combined(load, p, q, coef):
    cx, cy, cz = load.shape
    box = jax.ShapeDtypeStruct((cx, cy, cz), F32)
    vmem, hbm = (pl.BlockSpec(memory_space=space) for space in (pltpu.VMEM, pltpu.HBM))
    return pl.pallas_call(
        combine,
        out_shape=(box, box),
        in_specs=[vmem] * 4,
        out_specs=(hbm, hbm),
        scratch_shapes=[pltpu.VMEM((cx, cy, cz), F32)] * 2 + [pltpu.SemaphoreType.DMA((2,))],
    )(*(pltpu.with_memory_space_constraint(a, pltpu.VMEM) for a in (load, p, q, coef)))


def per_device(sizes, face_blocks, owner_rank, owner_tile, live_count, right_side, diagonal):
    blocks = face_blocks.shape[3]
    cx, cy, cz = right_side.shape
    group = sizes["gx"]
    stages = stages_of(sizes)
    relays = relays_of(sizes, stages)
    slots = sum(len(offsets_of(sizes, axes)) for axes in stages)
    vmem, hbm = (pl.BlockSpec(memory_space=space) for space in (pltpu.VMEM, pltpu.HBM))
    box = pltpu.VMEM((cx, cy, cz), F32)
    load, p, q, coef = pl.pallas_call(
        functools.partial(kernel, sizes, stages, relays),
        out_shape=(box, box, box, pltpu.VMEM((8, cz), F32)),
        in_specs=[hbm] * 6,
        out_specs=(vmem, vmem, vmem, vmem),
        scratch_shapes=[
            pltpu.SMEM((blocks,), jnp.int32),
            pltpu.SMEM((blocks,), jnp.int32),
            pltpu.SMEM(live_count.shape, jnp.int32),
            pltpu.VMEM((blocks, 2 * cy, cz), F32),
            pltpu.VMEM((cx, cy, cz), F32),
            pltpu.VMEM((blocks * cy, cz), F32),
            pltpu.VMEM((group, cy, cz), F32),
            pltpu.VMEM((3 * group, 1, cz), F32),
            pltpu.VMEM((group, cy, cz), F32),
            pltpu.VMEM((3 * group, 1, cz), F32),
            pltpu.VMEM((group, cy, cz), F32),
            pltpu.VMEM((4, cx, cz), F32),
            pltpu.VMEM((2, cx, cz), F32),
            pltpu.VMEM((4 * cx, cz), F32),
            pltpu.VMEM((2, 2, cy, cz), F32),
            pltpu.VMEM((2, 2, cx, cz), F32),
            pltpu.VMEM((2, 2, cx, cz), F32),
            pltpu.VMEM((2, cx, cz), F32),
            pltpu.VMEM((2, cx, cz), F32),
            pltpu.VMEM((4, 1, cz), F32),
            pltpu.VMEM((4, 1, cz), F32),
            pltpu.VMEM((8, cz), F32),
            pltpu.VMEM((4, 8, cz), F32),
            pltpu.VMEM((4, 1, cz), F32),
            pltpu.VMEM((4, 1, cz), F32),
            pltpu.VMEM((2 * cx, cz), F32),
            pltpu.VMEM((len(stages), 1, cz), F32),
            pltpu.VMEM((slots, 1, cz), F32),
            pltpu.SemaphoreType.DMA((6,)),
            pltpu.SemaphoreType.DMA((2,)),
            pltpu.SemaphoreType.DMA((2,)),
            pltpu.SemaphoreType.REGULAR((relays,)),
            pltpu.SemaphoreType.DMA((6,)),
            pltpu.SemaphoreType.DMA((6,)),
            pltpu.SemaphoreType.DMA((len(stages),)),
            pltpu.SemaphoreType.DMA((len(stages),)),
        ],
        compiler_params=pltpu.CompilerParams(collective_id=0, has_side_effects=True),
    )(
        owner_rank.reshape(blocks), owner_tile.reshape(blocks),
        live_count,
        face_blocks.reshape(blocks, 2 * cy, cz), right_side, diagonal,
    )
    return combined(load, p, q, coef)


def solution(mesh):
    sizes = dict(mesh.shape)
    return jax.shard_map(
        functools.partial(per_device, sizes),
        mesh=mesh,
        in_specs=(
            P("gx", "gy", "gz", None, None),
            P("gx", "gy", "gz", None, None),
            P("gx", "gy", "gz", None),
            P("gx", "gy", "gz"),
            P("gx", "gy", "gz"),
            P("gx", "gy", "gz"),
        ),
        out_specs=(P("gx", "gy", "gz"), P("gx", "gy", "gz")),
        check_vma=False,
    )
```

```python
import functools
import math

import jax
import jax.numpy as jnp
from jax import lax
from jax.experimental import pallas as pl
from jax.experimental.pallas import tpu as pltpu
from jax.sharding import PartitionSpec as P

CAP = 2
AXES = ("gx", "gy", "gz")
MESH = pl.DeviceIdType.MESH
F32 = jnp.float32


def offsets_of(sizes, axes):
    found = [()]
    for axis in axes:
        found = [done + (step,) for done in found for step in range(sizes[axis])]
    offsets = [dict(zip(axes, steps)) for steps in found if any(steps)]
    return sorted(
        offsets, key=lambda o: -sum(s if a != "gx" else s / sizes[a] for a, s in o.items())
    )


def stages_of(sizes):
    stages = []
    for axis in ("gx", "gz", "gy"):
        if stages and math.prod(sizes[a] for a in stages[-1] + [axis]) <= 32:
            stages[-1].append(axis)
        else:
            stages.append([axis])
    return stages


def relays_of(sizes, stages):
    rounds = 1
    for axes in stages:
        steps = [sizes[axis] - 1 for axis in axes if axis != "gx"]
        single = sum(n % 2 for n in steps) + (1 if "gx" in axes and sizes["gx"] > 1 else 0)
        rounds = max(rounds, 1 + sum(n // 2 for n in steps) + max(0, single - 3))
    return rounds


def kernel(
    sizes, stages, relays,
    rank_hbm, tile_hbm, live_hbm, face_hbm, right_hbm, diag_hbm,
    load_v, p_v, q_v, coef_ref,
    rank_ref, tile_ref, live_ref, face_v, diag_v, sums_v,
    send_v, stag_v, recv_v, rtag_v, turned_v, rows_v, drows_v, cols_v,
    hx_v, xr_v, hxr_v, qrows_v, qcols_v, ysend_v, hy_v, zsend_v, hz_v, xy_v, hxy_v, yz_v, hyz_v, xz_v, hxz_v, mix_v, part_v, gath_v,
    in_sem, a2a_send, a2a_recv, relay_sem, halo_send, halo_recv, red_send, red_recv,
):
    cx, cy, cz = load_v.shape
    blocks = face_v.shape[0]
    group = sizes["gx"]
    at = {axis: lax.axis_index(axis) for axis in AXES}

    def near(axis, side):
        return at[axis] > 0 if side == 0 else at[axis] < sizes[axis] - 1

    def beside(offset):
        return {a: lax.rem(at[a] + s, sizes[a]) for a, s in offset.items() if s}

    def across(offset):
        where = {}
        for axis, step in offset.items():
            if sizes[axis] & (sizes[axis] - 1):
                where[axis] = lax.rem(at[axis] + step, sizes[axis])
            else:
                where[axis] = at[axis]
                for bit in (1 << n for n in range(sizes[axis].bit_length())):
                    if step & bit:
                        where[axis] = where[axis] + bit - 2 * bit * lax.rem(at[axis] // bit, 2)
        return {axis: index for axis, index in where.items() if offset[axis]}

    def near_all(sides):
        found = near(*sides[0])
        for axis, side in sides[1:]:
            found = found & near(axis, side)
        return found

    loads = [
        pltpu.make_async_copy(face_hbm, face_v, in_sem.at[0]),
        pltpu.make_async_copy(right_hbm, load_v, in_sem.at[1]),
        pltpu.make_async_copy(diag_hbm, diag_v, in_sem.at[2]),
        pltpu.make_async_copy(live_hbm, live_ref, in_sem.at[3]),
        pltpu.make_async_copy(rank_hbm, rank_ref, in_sem.at[4]),
        pltpu.make_async_copy(tile_hbm, tile_ref, in_sem.at[5]),
    ]
    for copy in loads:
        copy.start()

    def within(axis, step):
        return at[axis] + step >= 0 if step < 0 else at[axis] + step < sizes[axis]

    def greet(semaphore, reach=1):
        for k in range(1, group):
            pl.semaphore_signal(
                semaphore, inc=1, device_id=beside({"gx": k}), device_id_type=MESH
            )
        for axis in ("gy", "gz"):
            for step in range(-reach, reach + 1):
                if 0 < abs(step) < sizes[axis]:
                    @pl.when(within(axis, step))
                    def _():
                        pl.semaphore_signal(
                            semaphore, inc=1, device_id={axis: at[axis] + step},
                            device_id_type=MESH,
                        )

    def greeted(reach=1):
        count = jnp.int32(group - 1)
        for axis in ("gy", "gz"):
            for step in range(-reach, reach + 1):
                if 0 < abs(step) < sizes[axis]:
                    count = count + jnp.where(within(axis, step), 1, 0)
        return count

    barrier = pltpu.get_barrier_semaphore()
    greet(barrier)

    messages = {"x": [], "z": [], "y": [], "xr": [], "xy": [], "xz": [], "yz": []}
    places = {
        "x": hx_v, "y": hy_v, "z": hz_v, "xr": hxr_v, "xy": hxy_v, "xz": hxz_v, "yz": hyz_v,
    }
    kinds = list(messages)
    for s in range(2):
        end = (cx - 1) * s
        messages["x"].append(((("gx", s),), load_v.at[end], lambda s: hx_v.at[s, 0]))
        messages["x"].append(((("gx", s),), p_v.at[end], lambda s: hx_v.at[s, 1]))
        messages["xr"].append(((("gx", s),), xr_v.at[s], lambda s: hxr_v.at[s]))
        messages["y"].append(((("gy", s),), ysend_v.at[s], lambda s: hy_v.at[s]))
        messages["z"].append(((("gz", s),), zsend_v.at[s], lambda s: hz_v.at[s]))
        for t in range(2):
            messages["xy"].append(
                ((("gx", s), ("gy", t)), xy_v.at[2 * s + t], lambda s, t: hxy_v.at[2 * s + t])
            )
            messages["xz"].append(
                ((("gx", s), ("gz", t)), xz_v.at[2 * s + t], lambda s, t: hxz_v.at[2 * s + t])
            )
            messages["yz"].append(
                ((("gy", s), ("gz", t)), yz_v, lambda s, t: hyz_v.at[2 * s + t])
            )

    def send(name):
        for sides, src, place in messages[name]:
            @pl.when(near_all(sides))
            def _():
                pltpu.make_async_remote_copy(
                    src_ref=src, dst_ref=place(*[1 - side for _, side in sides]),
                    send_sem=halo_send.at[kinds.index(name)],
                    recv_sem=halo_recv.at[kinds.index(name)],
                    device_id={
                        axis: lax.rem(at[axis] + (1 if side else sizes[axis] - 1), sizes[axis])
                        for axis, side in sides
                    },
                    device_id_type=MESH,
                ).start()

    def settle(name, act):
        count = jnp.int32(1)
        for axis, _ in messages[name][0][0]:
            count = count * sum(jnp.where(near(axis, side), 1, 0) for side in range(2))
        for found in (1, 2, 4)[:places[name].shape[0] // 2 + 1]:
            @pl.when(count == found)
            def _():
                slots = places[name].at[pl.ds(0, found)]
                act(pltpu.make_async_remote_copy(
                    src_ref=slots, dst_ref=slots,
                    send_sem=halo_send.at[kinds.index(name)],
                    recv_sem=halo_recv.at[kinds.index(name)],
                    device_id=beside({"gx": 1}), device_id_type=MESH,
                ))

    def receive(name):
        settle(name, lambda copy: copy.wait_recv())

    def finish(name):
        settle(name, lambda copy: copy.wait_send())

    for name in messages:
        for sides, _, place in messages[name]:
            slot = place(*[side for _, side in sides])

            @pl.when(jnp.logical_not(near_all(sides)))
            def _():
                slot[...] = jnp.zeros(slot.shape, F32)

    lane = lax.broadcasted_iota(jnp.int32, (cy, cz), 1)
    lane1 = lax.broadcasted_iota(jnp.int32, (1, cz), 1)
    lane8 = lax.broadcasted_iota(jnp.int32, (8, cz), 1)
    row = lax.broadcasted_iota(jnp.int32, (cy, cz), 0)
    row8 = lax.broadcasted_iota(jnp.int32, (8, cz), 0)
    layer = lax.broadcasted_iota(jnp.int32, (cx, cz), 0)
    lane_x = lax.broadcasted_iota(jnp.int32, (cx, cz), 1)
    right_half = lane >= cz // 2
    ends = (lane == 0) | (lane == cz - 1)

    def turn(values, by, axis=1):
        by = by % values.shape[axis]
        return values if by == 0 else pltpu.roll(values, by, axis=axis)

    loads[0].wait()
    for copy in loads[3:]:
        copy.wait()
    pair = (
        lax.broadcasted_iota(jnp.int32, (cz, cz), 0) // 2
        == lax.broadcasted_iota(jnp.int32, (cz, cz), 1) % (cz // 2)
    )
    pair = jnp.where(pair, 0.25, 0.0).astype(jnp.bfloat16)
    for b in range(blocks):
        sums_v[b * cy:(b + 1) * cy] = (
            face_v[b, pl.ds(0, cy, stride=2), :] + face_v[b, pl.ds(1, cy, stride=2), :]
        )
    whole = sums_v[...]
    high = whole.astype(jnp.bfloat16)
    rest = whole - high.astype(F32)
    middle = rest.astype(jnp.bfloat16)
    low = (rest - middle.astype(F32)).astype(jnp.bfloat16)
    column = lax.broadcasted_iota(jnp.int32, (8, cz), 0)
    column = jnp.where(column < 2, column, cz // 2 - 4 + column)
    choice = (lax.broadcasted_iota(jnp.int32, (8, cz), 1) // 2 == column) & (column < cz // 2)
    choice = jnp.where(choice, 0.25, 0.0).astype(jnp.bfloat16)

    def columns_of(values):
        return lax.dot_general(
            choice, values, (((1,), (1,)), ((), ())), preferred_element_type=F32
        )

    columns = columns_of(low) + columns_of(middle) + columns_of(high)
    sums_v[...] = (
        jnp.dot(low, pair, preferred_element_type=F32)
        + jnp.dot(middle, pair, preferred_element_type=F32)
    ) + jnp.dot(high, pair, preferred_element_type=F32)

    target = [rank_ref[b] for b in range(blocks)]
    alive = [live_ref[0, 0, 0] > b for b in range(blocks)]
    position = []
    for b in range(blocks):
        count = jnp.int32(0)
        for before in range(b):
            count = count + jnp.where((target[before] == target[b]) & alive[before], 1, 0)
        position.append(count)
    edges = []
    for b in range(blocks):
        here = columns[:, b // 2 * cz:b // 2 * cz + cz]
        there = pltpu.roll(here, cz // 2, axis=1)
        first, last = (here, there) if b % 2 == 0 else (there, here)
        even = jnp.where(lane1 < cz // 2, first[0:1], last[1:2])
        other = jnp.where(lane1 < cz // 2, first[3:4], last[2:3])
        edges.append(jnp.where(lax.rem(tile_ref[b], 2) == 0, even, other))
    for k in range(group):
        dest = lax.rem(at["gx"] + k, group)
        outer = [jnp.zeros((1, cz), F32) for _ in range(CAP)]
        total = jnp.zeros((cy, cz), F32)
        tags = jnp.full((1, cz), -1.0, F32)
        for b in range(blocks):
            code = jnp.where(alive[b] & (target[b] == dest), position[b], CAP)
            left, right = jnp.where(code == 0, 1.0, 0.0), jnp.where(code == 1, 1.0, 0.0)
            weight = jnp.where(lane1 < cz // 2, left, right)
            tag = tile_ref[b].astype(F32)
            tags = jnp.where(weight > 0.5, tag, tags)
            values = sums_v[b * cy:(b + 1) * cy]
            total = total + values * jnp.where(right_half, right, left)
            outer = [outer[0] + left * edges[b], outer[1] + right * edges[b]]
        (recv_v if k == 0 else send_v)[k] = total
        for place, values in enumerate([tags] + outer):
            (rtag_v if k == 0 else stag_v)[3 * k + place] = values

    pl.semaphore_wait(barrier, greeted())
    boxes = ((send_v, recv_v), (stag_v, rtag_v))

    def exchange(order, slots, k):
        src, dst = boxes[order]
        return pltpu.make_async_remote_copy(
            src_ref=src.at[slots], dst_ref=dst.at[slots],
            send_sem=a2a_send.at[order], recv_sem=a2a_recv.at[order],
            device_id=beside({"gx": k}), device_id_type=MESH,
        )

    for k in range(1, group):
        for order in range(2):
            exchange(order, pl.ds(k * (1, 3)[order], (1, 3)[order]), k).start()
    arrivals = [
        exchange(order, pl.ds(step, step * (group - 1)), 1)
        for order, step in enumerate((1, 3)) if group > 1
    ]
    greet(relay_sem.at[0])
    loads[1].wait()
    loads[2].wait()

    for x in range(cx):
        for place, y in enumerate((0, 1, cy - 2, cy - 1)):
            rows_v[place, x:x + 1] = load_v[x, y:y + 1]
        for place, y in enumerate((0, cy - 1)):
            drows_v[place, x:x + 1] = diag_v[x, y:y + 1]
    upper, lower = jnp.zeros((cy, cz), F32), jnp.zeros((cy, cz), F32)
    for x in range(cx):
        plane, weights = load_v[x], diag_v[x]
        for side in range(2):
            spot = cx * side + x
            upper = jnp.where(lane == spot, turn(plane, spot + side), upper)
            lower = jnp.where(lane == spot, turn(plane, spot + 3 * side - 1), lower)
            spot = spot + 2 * cx
            upper = jnp.where(lane == spot, turn(weights, spot + side), upper)
    cols_v[...] = jnp.concatenate([upper, lower], axis=0).T[:4 * cx]

    for relay in range(relays):
        pl.semaphore_wait(relay_sem.at[relay], greeted(min(relay + 1, 2)))
        if relay < relays - 1:
            greet(relay_sem.at[relay + 1], 2)
    for copy in arrivals:
        copy.wait_recv()

    for k in range(group):
        turned_v[k] = pltpu.roll(recv_v[k], cz // 2, axis=1)
    sources = []
    for k in range(group):
        tags = rtag_v[3 * k]
        swapped = pltpu.roll(jnp.broadcast_to(tags, (8, cz)), cz // 2, axis=1)[:1]
        sources += [(recv_v.at[k], tags), (turned_v.at[k], swapped)]
    half1 = jnp.where(lane1 >= cz // 2, 1, 0)

    def scatter(x):
        want = (2 * x + half1).astype(F32)
        plane = load_v[x]
        for values, tags in sources:
            plane = plane + jnp.where(tags == want, values[...], 0.0)
        load_v[x] = plane

    def inside(src, x):
        plane = src[x]
        around = jnp.where(lane == 0, 0.0, pltpu.roll(plane, 1, axis=1))
        around = around + jnp.where(lane == cz - 1, 0.0, pltpu.roll(plane, cz - 1, axis=1))
        around = around + jnp.where(row == 0, 0.0, pltpu.roll(plane, 1, axis=0))
        around = around + jnp.where(row == cy - 1, 0.0, pltpu.roll(plane, cy - 1, axis=0))
        if x > 0:
            around = around + src[x - 1]
        if x < cx - 1:
            around = around + src[x + 1]
        return diag_v[x] * plane - around

    want = (2 * layer + jnp.where(lane_x >= cz // 2, 1, 0)).astype(F32)
    faces = [rows_v[place] for place in range(4)]
    for values, tags in sources:
        hit = jnp.broadcast_to(tags, (cx, cz)) == want
        for place, y in enumerate((0, 1, cy - 2, cy - 1)):
            spread = jnp.broadcast_to(values[y:y + 1], (cx, cz))
            faces[place] = faces[place] + jnp.where(hit, spread, 0.0)
    for side in range(2):
        face, second = faces[3 * side], faces[1 + side]
        around = jnp.where(lane_x == 0, 0.0, pltpu.roll(face, 1, axis=1)) + second
        around = around + jnp.where(lane_x == cz - 1, 0.0, pltpu.roll(face, cz - 1, axis=1))
        around = around + jnp.where(layer == 0, 0.0, pltpu.roll(face, 1, axis=0))
        around = around + jnp.where(layer == cx - 1, 0.0, pltpu.roll(face, cx - 1, axis=0))
        ysend_v[side, 0] = face
        ysend_v[side, 1] = drows_v[side] * face - around
        for s in range(2):
            xy_v[2 * s + side] = face[(cx - 1) * s:(cx - 1) * s + 1]
    send("xy")
    send("y")

    line = lax.broadcasted_iota(jnp.int32, (2 * cx, cz), 0)
    lane_z = lax.broadcasted_iota(jnp.int32, (2 * cx, cz), 1)
    own_tile = (2 * (line % cx) + line // cx).astype(F32)
    turned = cols_v[:2 * cx]
    for k in range(group):
        tags = rtag_v[3 * k]
        for place in range(CAP):
            tag = tags[:, :1] if place == 0 else tags[:, cz - 1:]
            hit = jnp.broadcast_to(tag, (2 * cx, cz)) == own_tile
            values = jnp.broadcast_to(rtag_v[3 * k + 1 + place], (2 * cx, cz))
            turned = turned + jnp.where(hit, values, 0.0)
    around = jnp.where(lane_z == 0, 0.0, turn(turned, 1)) + turn(turned, cz // 2)
    around = around + jnp.where(lane_z == cy - 1, 0.0, turn(turned, -1))
    around = around + jnp.where(line % cx == 0, 0.0, turn(turned, 1, 0))
    around = around + jnp.where(line % cx == cx - 1, 0.0, turn(turned, -1, 0))
    image = cols_v[2 * cx:] * turned - around
    deeper = turn(turned, cz // 2)
    turned = jnp.where(lane_z < cy, turned, turn(image, cz // 2))
    for side in range(2):
        zsend_v[side] = turned[cx * side:cx * side + cx]
    send("z")
    groups = cx // 8
    tile = jnp.zeros((8, cz), F32)
    for side in range(2):
        for part in range(groups):
            spot = 2 * (groups * side + part)
            piece = turn(ysend_v[side, 0, 8 * part:8 * part + 8], spot + 1)
            tile = jnp.where(lane8 // 2 == spot // 2, piece, tile)
        for s in range(2):
            spot = cx * side + (cx - 1) * s
            xz_v[2 * s + side] = turned[spot:spot + 1]
            xr_v[s, 2 * side] = turned[spot:spot + 1]
            xr_v[s, 2 * side + 1] = deeper[spot:spot + 1]
    yz_v[...] = tile
    for name in ("yz", "xz", "xr"):
        send(name)

    for x in (0, 1, cx - 2, cx - 1):
        scatter(x)
    for x in (0, cx - 1):
        p_v[x] = inside(load_v, x)
    send("x")

    def fold(acc, values):
        for part in range(cy // 8):
            acc = acc + values[8 * part:8 * part + 8]
        return acc

    for x in range(2, cx - 2):
        scatter(x)
    for x in range(1, cx - 1):
        p_v[x] = inside(load_v, x)
    acc = [jnp.zeros((8, cz), F32) for _ in range(4)]
    image = jnp.zeros((cy, cz), F32)
    for x in range(cx):
        load, p, q = load_v[x], p_v[x], inside(p_v, x)
        q_v[x] = q
        pairs = ((load, load), (load, p), (p, p), (p, q))
        acc = [fold(total, one * other) for total, (one, other) in zip(acc, pairs)]
        for side in range(2):
            y = (cy - 1) * side
            qrows_v[side, x:x + 1] = q[y:y + 1]
            spot = cx * side + x
            image = jnp.where(lane == spot, turn(q, spot + side), image)
    qcols_v[...] = jnp.concatenate([image, jnp.zeros((cz - cy, cz), F32)], axis=0).T[:2 * cx]

    def rim(plane, first, last):
        top = plane[:8] - jnp.where(row8 == 0, first, 0.0)
        bottom = plane[cy - 8:] - jnp.where(row8 == 7, last, 0.0)
        return jnp.concatenate([top, plane[8:cy - 8], bottom], axis=0)

    for name in ("x", "xr", "y", "z", "xy", "xz", "yz"):
        receive(name)
    there = {
        (axis, side): jnp.where(near(axis, side), 1.0, 0.0) for axis in AXES for side in range(2)
    }
    y_halo = []
    for side in range(2):
        halo = hy_v[side, 1] - there["gy", side] * ysend_v[side, 0]
        halo = halo - jnp.where(layer == 0, 2.0 * hxy_v[side], 0.0)
        y_halo.append(halo - jnp.where(layer == cx - 1, 2.0 * hxy_v[2 + side], 0.0))
    halves = []
    for side in range(2):
        halo = hz_v[side] - there["gz", side] * turn(zsend_v[side], cz // 2)
        for s in range(2):
            corner = turn(jnp.broadcast_to(hxz_v[2 * s + side], (8, cz)), cz // 2)[:1]
            halo = halo - jnp.where(layer == (cx - 1) * s, 2.0 * corner, 0.0)
        parts = []
        for part in range(groups):
            piece = halo[8 * part:8 * part + 8]
            for s in range(2):
                spot = 2 * (groups * (1 - s) + part) + side
                goal = cy if s == 0 else 2 * cy - 1
                corner = turn(hyz_v[2 * s + side], goal - spot)
                piece = piece - jnp.where(lane8 == goal, 2.0 * corner, 0.0)
            parts.append(piece)
        halves.append(jnp.concatenate(parts, axis=0))

    def add(at_sum, values):
        for part in range(values.shape[0] // 8):
            acc[at_sum] = acc[at_sum] + values[8 * part:8 * part + 8]

    def face_sums(h, halo, load, p, q, stencil):
        add(1, -(load * h))
        add(2, h * (h - 2.0 * p))
        add(3, h * (stencil + halo - 2.0 * q) - p * halo)

    rows = [jnp.zeros((1, cz), F32) for _ in range(4)]
    for side in range(2):
        x = (cx - 1) * side
        h, load = hx_v[side, 0], load_v[x]
        around = jnp.where(lane == 0, 0.0, turn(h, 1))
        around = around + jnp.where(lane == cz - 1, 0.0, turn(h, -1))
        around = around + jnp.where(row == 0, 0.0, turn(h, 1, 0))
        around = around + jnp.where(row == cy - 1, 0.0, turn(h, -1, 0))
        halo = hx_v[side, 1] - there["gx", side] * load
        face_sums(h, halo, load, p_v[x], q_v[x], diag_v[x] * h - around)
    y_stencil = []
    for side in range(2):
        h = hy_v[side, 0]
        around = jnp.where(lane_x == 0, 0.0, turn(h, 1))
        around = around + jnp.where(lane_x == cz - 1, 0.0, turn(h, -1))
        around = around + jnp.where(layer == 0, 0.0, turn(h, 1, 0))
        around = around + jnp.where(layer == cx - 1, 0.0, turn(h, -1, 0))
        y_stencil.append(drows_v[side] * h - around)
        face_sums(
            h, y_halo[side], ysend_v[side, 0], ysend_v[side, 1], qrows_v[side], y_stencil[side]
        )
    z_stencil, z_h, z_halves = [], [], []
    used = lane_x < cy
    for side in range(2):
        h = jnp.where(used, hz_v[side], 0.0)
        halo = jnp.where(used, turn(halves[side], cz // 2), 0.0)
        around = turn(h, 1) + jnp.where(lane_x == cz - 1, 0.0, turn(h, -1))
        around = around + jnp.where(layer == 0, 0.0, turn(h, 1, 0))
        around = around + jnp.where(layer == cx - 1, 0.0, turn(h, -1, 0))
        span = pl.ds(cx * side, cx)
        z_stencil.append(cols_v[pl.ds(2 * cx + cx * side, cx)] * h - around)
        z_h.append(h)
        z_halves.append(halo)
        own_p = turn(zsend_v[side], cz // 2)
        face_sums(h, halo, zsend_v[side], own_p, qcols_v[span], z_stencil[side])

    def edge_sums(one, one_in, one_halo, other, other_halo, other_stencil):
        second = 2.0 * one * other
        third = 2.0 * (one * other_stencil - one_in * other)
        return second, third + one * other_halo + other * one_halo

    for s in range(2):
        x = (cx - 1) * s
        for t in range(2):
            y, y_in = ((0, 1), (cy - 1, cy - 2))[t]
            second, third = edge_sums(
                hx_v[s, 0, y:y + 1], hx_v[s, 0, y_in:y_in + 1],
                hx_v[s, 1, y:y + 1] - there["gx", s] * load_v[x, y:y + 1],
                hy_v[t, 0, x:x + 1], y_halo[t][x:x + 1], y_stencil[t][x:x + 1],
            )
            rows[2], rows[3] = rows[2] + second, rows[3] + third
            second, third = edge_sums(
                hxr_v[s, 2 * t], hxr_v[s, 2 * t + 1],
                turn(jnp.broadcast_to(hxr_v[s, 2 * t], (8, cz)), cz // 2)[:1]
                - there["gx", s] * zsend_v[t, x:x + 1],
                z_h[t][x:x + 1], z_halves[t][x:x + 1], z_stencil[t][x:x + 1],
            )
            used1 = lane1 < cy
            rows[2] = rows[2] + jnp.where(used1, second, 0.0)
            rows[3] = rows[3] + jnp.where(used1, third, 0.0)
            goal = (cy - 1) * s
            spot, spot_in = ((0, 1), (cz - 1, cz - 2))[t]
            second, third = edge_sums(
                turn(hy_v[s, 0], goal - spot), turn(hy_v[s, 0], goal - spot_in),
                turn(y_halo[s], goal - spot), z_h[t], z_halves[t], z_stencil[t],
            )
            add(2, jnp.where(lane_x == goal, second, 0.0))
            add(3, jnp.where(lane_x == goal, third, 0.0))

    def columned(halves):
        for side in range(2):
            mix_v[pl.ds(1 - side, cx, stride=2), :] = halves[side]
        columns = mix_v[...].T
        return jnp.concatenate([columns, jnp.zeros((cz, cz - 2 * cx), F32)], axis=1)

    def complete():
        finish("x")
        l_halo = columned([hz_v[0], hz_v[1]])[:cy]
        for x in range(cx):
            plane = p_v[x] - jnp.where(ends, turn(l_halo, -2 * x - 1), 0.0)
            plane = rim(plane, hy_v[0, 0, x:x + 1], hy_v[1, 0, x:x + 1])
            for side in range(2):
                if x == (cx - 1) * side:
                    plane = plane - hx_v[side, 0]
            p_v[x] = plane
        z_halo = columned(halves)[cy:2 * cy]
        for x in range(cx):
            plane = inside(p_v, x) - jnp.where(ends, turn(z_halo, -2 * x - 1), 0.0)
            plane = rim(plane, y_halo[0][x:x + 1], y_halo[1][x:x + 1])
            for side in range(2):
                if x == (cx - 1) * side:
                    plane = plane - hx_v[side, 1] + there["gx", side] * load_v[x]
            q_v[x] = plane

    mine = jnp.zeros((8, cz), F32)
    for order in range(4):
        mine = jnp.where(row8 == order, jnp.sum(acc[order], axis=0, keepdims=True) + rows[order], mine)
    mine = mine + pltpu.roll(mine, cz // 2, axis=1)
    mine = mine + pltpu.roll(mine, cz // 4, axis=1)
    own = row8 == lane8 // (cz // 4)
    mine = jnp.sum(jnp.where(own, mine, 0.0), axis=0, keepdims=True)
    slot = 0
    waiting = []
    for order, axes in enumerate(stages):
        part_v[order] = mine
        offsets = offsets_of(sizes, axes)

        def part(offset, src, dst):
            return pltpu.make_async_remote_copy(
                src_ref=src, dst_ref=dst,
                send_sem=red_send.at[order], recv_sem=red_recv.at[order],
                device_id=across(offset), device_id_type=MESH,
            )

        for place, offset in enumerate(offsets):
            part(offset, part_v.at[order], gath_v.at[slot + place]).start()
        if order == 0:
            complete()
        if offsets:
            span = gath_v.at[pl.ds(slot, len(offsets))]
            waiting.append(part(offsets[0], span, span))
            waiting[-1].wait_recv()
        for place in range(len(offsets)):
            mine = mine + gath_v[slot + place]
        slot += len(offsets)

    sums = jnp.sum(jnp.where(own, mine, 0.0), axis=1, keepdims=True)
    s0, s1, s2, s3 = (sums[n:n + 1] for n in range(4))
    step = 6.0 * s0 + s1
    a = s0 / step
    c = s1 / step
    norm = c * c * s0 - 2.0 * a * c * s1 + a * a * s2
    e = c + norm / s0
    curve = 6.0 * (e * e * s0 - 2.0 * e * a * s1 + a * a * s2) + (
        e * e * s1 - 2.0 * e * a * s2 + a * a * s3
    )
    b = norm / curve
    x_load, x_p = a + b * e, b * a
    r_load, r_p, r_q = c - 6.0 * b * e, a + b * (e - 6.0 * a), b * a
    for order, value in enumerate((x_load, x_p, r_load, r_p, r_q)):
        coef_ref[order:order + 1] = jnp.broadcast_to(value, (1, cz))
    for copy in arrivals + waiting:
        copy.wait_send()
    for name in ("y", "z", "xr", "xy", "xz", "yz"):
        finish(name)


def combine(load_ref, p_ref, q_ref, coef_ref, x_hbm, r_hbm, x_v, r_v, sem):
    cx = load_ref.shape[0]
    x_load, x_p, r_load, r_p, r_q = (coef_ref[n:n + 1] for n in range(5))
    pieces = 4
    for piece in range(pieces):
        first, last = cx * piece // pieces, cx * (piece + 1) // pieces
        for x in range(first, last):
            load, p = load_ref[x], p_ref[x]
            x_v[x] = x_load * load - x_p * p
            r_v[x] = r_load * load - r_p * p + r_q * q_ref[x]
        span = pl.ds(first, last - first)
        for number, (src, dst) in enumerate(((x_v, x_hbm), (r_v, r_hbm))):
            pltpu.make_async_copy(src.at[span], dst.at[span], sem.at[number]).start()
    for number, (src, dst) in enumerate(((x_v, x_hbm), (r_v, r_hbm))):
        pltpu.make_async_copy(src, dst, sem.at[number]).wait()


def combined(load, p, q, coef):
    cx, cy, cz = load.shape
    box = jax.ShapeDtypeStruct((cx, cy, cz), F32)
    vmem, hbm = (pl.BlockSpec(memory_space=space) for space in (pltpu.VMEM, pltpu.HBM))
    return pl.pallas_call(
        combine,
        out_shape=(box, box),
        in_specs=[vmem] * 4,
        out_specs=(hbm, hbm),
        scratch_shapes=[pltpu.VMEM((cx, cy, cz), F32)] * 2 + [pltpu.SemaphoreType.DMA((2,))],
    )(*(pltpu.with_memory_space_constraint(a, pltpu.VMEM) for a in (load, p, q, coef)))


def per_device(sizes, face_blocks, owner_rank, owner_tile, live_count, right_side, diagonal):
    blocks = face_blocks.shape[3]
    cx, cy, cz = right_side.shape
    group = sizes["gx"]
    stages = stages_of(sizes)
    relays = relays_of(sizes, stages)
    slots = sum(len(offsets_of(sizes, axes)) for axes in stages)
    vmem, hbm = (pl.BlockSpec(memory_space=space) for space in (pltpu.VMEM, pltpu.HBM))
    box = pltpu.VMEM((cx, cy, cz), F32)
    load, p, q, coef = pl.pallas_call(
        functools.partial(kernel, sizes, stages, relays),
        out_shape=(box, box, box, pltpu.VMEM((8, cz), F32)),
        in_specs=[hbm] * 6,
        out_specs=(vmem, vmem, vmem, vmem),
        scratch_shapes=[
            pltpu.SMEM((blocks,), jnp.int32),
            pltpu.SMEM((blocks,), jnp.int32),
            pltpu.SMEM(live_count.shape, jnp.int32),
            pltpu.VMEM((blocks, 2 * cy, cz), F32),
            pltpu.VMEM((cx, cy, cz), F32),
            pltpu.VMEM((blocks * cy, cz), F32),
            pltpu.VMEM((group, cy, cz), F32),
            pltpu.VMEM((3 * group, 1, cz), F32),
            pltpu.VMEM((group, cy, cz), F32),
            pltpu.VMEM((3 * group, 1, cz), F32),
            pltpu.VMEM((group, cy, cz), F32),
            pltpu.VMEM((4, cx, cz), F32),
            pltpu.VMEM((2, cx, cz), F32),
            pltpu.VMEM((4 * cx, cz), F32),
            pltpu.VMEM((2, 2, cy, cz), F32),
            pltpu.VMEM((2, 4, 1, cz), F32),
            pltpu.VMEM((2, 4, 1, cz), F32),
            pltpu.VMEM((2, cx, cz), F32),
            pltpu.VMEM((2 * cx, cz), F32),
            pltpu.VMEM((2, 2, cx, cz), F32),
            pltpu.VMEM((2, 2, cx, cz), F32),
            pltpu.VMEM((2, cx, cz), F32),
            pltpu.VMEM((2, cx, cz), F32),
            pltpu.VMEM((4, 1, cz), F32),
            pltpu.VMEM((4, 1, cz), F32),
            pltpu.VMEM((8, cz), F32),
            pltpu.VMEM((4, 8, cz), F32),
            pltpu.VMEM((4, 1, cz), F32),
            pltpu.VMEM((4, 1, cz), F32),
            pltpu.VMEM((2 * cx, cz), F32),
            pltpu.VMEM((len(stages), 1, cz), F32),
            pltpu.VMEM((slots, 1, cz), F32),
            pltpu.SemaphoreType.DMA((6,)),
            pltpu.SemaphoreType.DMA((2,)),
            pltpu.SemaphoreType.DMA((2,)),
            pltpu.SemaphoreType.REGULAR((relays,)),
            pltpu.SemaphoreType.DMA((7,)),
            pltpu.SemaphoreType.DMA((7,)),
            pltpu.SemaphoreType.DMA((len(stages),)),
            pltpu.SemaphoreType.DMA((len(stages),)),
        ],
        compiler_params=pltpu.CompilerParams(collective_id=0, has_side_effects=True),
    )(
        owner_rank.reshape(blocks), owner_tile.reshape(blocks),
        live_count,
        face_blocks.reshape(blocks, 2 * cy, cz), right_side, diagonal,
    )
    return combined(load, p, q, coef)


def solution(mesh):
    sizes = dict(mesh.shape)
    return jax.shard_map(
        functools.partial(per_device, sizes),
        mesh=mesh,
        in_specs=(
            P("gx", "gy", "gz", None, None),
            P("gx", "gy", "gz", None, None),
            P("gx", "gy", "gz", None),
            P("gx", "gy", "gz"),
            P("gx", "gy", "gz"),
            P("gx", "gy", "gz"),
        ),
        out_specs=(P("gx", "gy", "gz"), P("gx", "gy", "gz")),
        check_vma=False,
    )
```

```python
import functools
import math

import jax
import jax.numpy as jnp
from jax import lax
from jax.experimental import pallas as pl
from jax.experimental.pallas import tpu as pltpu
from jax.sharding import PartitionSpec as P

CAP = 2
AXES = ("gx", "gy", "gz")
MESH = pl.DeviceIdType.MESH
F32 = jnp.float32


def offsets_of(sizes, axes):
    found = [()]
    for axis in axes:
        found = [done + (step,) for done in found for step in range(sizes[axis])]
    offsets = [dict(zip(axes, steps)) for steps in found if any(steps)]
    return sorted(
        offsets, key=lambda o: -sum(s if a != "gx" else s / sizes[a] for a, s in o.items())
    )


def stages_of(sizes):
    stages = []
    for axis in ("gx", "gz", "gy"):
        if stages and math.prod(sizes[a] for a in stages[-1] + [axis]) <= 32:
            stages[-1].append(axis)
        else:
            stages.append([axis])
    return stages


def relays_of(sizes, stages):
    rounds = 1
    for axes in stages:
        steps = [sizes[axis] - 1 for axis in axes if axis != "gx"]
        single = sum(n % 2 for n in steps) + (1 if "gx" in axes and sizes["gx"] > 1 else 0)
        rounds = max(rounds, 1 + sum(n // 2 for n in steps) + max(0, single - 3))
    return rounds


def message_rows(cx, cy, nx, ny, nz):
    return (2 * cy + 4) * nx + 2 * cx * ny + cx * nz + nx * ny + nx * nz + 8 * ny * nz


def kernel(
    sizes, stages, relays,
    rank_hbm, tile_hbm, live_hbm, face_hbm, right_hbm, diag_hbm,
    load_v, p_v, q_v, coef_ref,
    rank_ref, tile_ref, live_ref, face_v, diag_v, sums_v,
    send_v, scard_v, recv_v, rcard_v, turned_v, rows_v, drows_v, cols_v,
    hx_v, xr_v, hxr_v, qrows_v, qcols_v, ysend_v, hy_v, zsend_v, hz_v, xy_v, hxy_v, yz_v, hyz_v, xz_v, hxz_v, mix_v, tally_v, part_v, gath_v,
    in_sem, a2a_send, a2a_recv, relay_sem, halo_send, halo_recv, red_send, red_recv,
):
    cx, cy, cz = load_v.shape
    blocks = face_v.shape[0]
    group = sizes["gx"]
    at = {axis: lax.axis_index(axis) for axis in AXES}

    def near(axis, side):
        return at[axis] > 0 if side == 0 else at[axis] < sizes[axis] - 1

    def beside(offset):
        return {a: lax.rem(at[a] + s, sizes[a]) for a, s in offset.items() if s}

    def across(offset):
        where = {}
        for axis, step in offset.items():
            if sizes[axis] & (sizes[axis] - 1):
                where[axis] = lax.rem(at[axis] + step, sizes[axis])
            else:
                where[axis] = at[axis]
                for bit in (1 << n for n in range(sizes[axis].bit_length())):
                    if step & bit:
                        where[axis] = where[axis] + bit - 2 * bit * lax.rem(at[axis] // bit, 2)
        return {axis: index for axis, index in where.items() if offset[axis]}

    def near_all(sides):
        found = near(*sides[0])
        for axis, side in sides[1:]:
            found = found & near(axis, side)
        return found

    loads = [
        pltpu.make_async_copy(face_hbm, face_v, in_sem.at[0]),
        pltpu.make_async_copy(right_hbm, load_v, in_sem.at[1]),
        pltpu.make_async_copy(diag_hbm, diag_v, in_sem.at[2]),
        pltpu.make_async_copy(live_hbm, live_ref, in_sem.at[3]),
        pltpu.make_async_copy(rank_hbm, rank_ref, in_sem.at[4]),
        pltpu.make_async_copy(tile_hbm, tile_ref, in_sem.at[5]),
    ]
    for copy in loads:
        copy.start()

    def within(axis, step):
        return at[axis] + step >= 0 if step < 0 else at[axis] + step < sizes[axis]

    def greet(semaphore, reach=1):
        for k in range(1, group):
            pl.semaphore_signal(
                semaphore, inc=1, device_id=beside({"gx": k}), device_id_type=MESH
            )
        for axis in ("gy", "gz"):
            for step in range(-reach, reach + 1):
                if 0 < abs(step) < sizes[axis]:
                    @pl.when(within(axis, step))
                    def _():
                        pl.semaphore_signal(
                            semaphore, inc=1, device_id={axis: at[axis] + step},
                            device_id_type=MESH,
                        )

    def greeted(reach=1):
        count = jnp.int32(group - 1)
        for axis in ("gy", "gz"):
            for step in range(-reach, reach + 1):
                if 0 < abs(step) < sizes[axis]:
                    count = count + jnp.where(within(axis, step), 1, 0)
        return count

    barrier = pltpu.get_barrier_semaphore()
    greet(barrier)

    messages = {"x": [], "z": [], "y": [], "xr": [], "xy": [], "xz": [], "yz": []}
    for s in range(2):
        end = (cx - 1) * s
        messages["x"].append(((("gx", s),), load_v.at[end], lambda s: hx_v.at[s, 0]))
        messages["x"].append(((("gx", s),), p_v.at[end], lambda s: hx_v.at[s, 1]))
        messages["xr"].append(((("gx", s),), xr_v.at[s], lambda s: hxr_v.at[s]))
        messages["y"].append(((("gy", s),), ysend_v.at[s], lambda s: hy_v.at[s]))
        messages["z"].append(((("gz", s),), zsend_v.at[s], lambda s: hz_v.at[s]))
        for t in range(2):
            messages["xy"].append(
                ((("gx", s), ("gy", t)), xy_v.at[2 * s + t], lambda s, t: hxy_v.at[2 * s + t])
            )
            messages["xz"].append(
                ((("gx", s), ("gz", t)), xz_v.at[2 * s + t], lambda s, t: hxz_v.at[2 * s + t])
            )
            messages["yz"].append(
                ((("gy", s), ("gz", t)), yz_v, lambda s, t: hyz_v.at[2 * s + t])
            )

    def send(name, part=None):
        for order, (sides, src, place) in enumerate(messages[name]):
            if part in (None, order % 2):
                @pl.when(near_all(sides))
                def _():
                    pltpu.make_async_remote_copy(
                        src_ref=src, dst_ref=place(*[1 - side for _, side in sides]),
                        send_sem=halo_send.at[0], recv_sem=halo_recv.at[0],
                        device_id={
                            axis: lax.rem(
                                at[axis] + (1 if side else sizes[axis] - 1), sizes[axis]
                            )
                            for axis, side in sides
                        },
                        device_id_type=MESH,
                    ).start()

    def settle(act):
        beside_on = {
            axis: sum(jnp.where(near(axis, side), 1, 0) for side in range(2)) for axis in AXES
        }
        counts = [range(min(1, sizes[axis] - 1), min(2, sizes[axis] - 1) + 1) for axis in AXES]
        for nx in counts[0]:
            for ny in counts[1]:
                for nz in counts[2]:
                    lines = message_rows(cx, cy, nx, ny, nz)
                    if lines:
                        @pl.when(
                            (beside_on["gx"] == nx) & (beside_on["gy"] == ny)
                            & (beside_on["gz"] == nz)
                        )
                        def _():
                            span = tally_v.at[pl.ds(0, lines)]
                            act(pltpu.make_async_remote_copy(
                                src_ref=span, dst_ref=span,
                                send_sem=halo_send.at[0], recv_sem=halo_recv.at[0],
                                device_id=beside({"gx": 1}), device_id_type=MESH,
                            ))

    for name in messages:
        for sides, _, place in messages[name]:
            slot = place(*[side for _, side in sides])

            @pl.when(jnp.logical_not(near_all(sides)))
            def _():
                slot[...] = jnp.zeros(slot.shape, F32)

    lane = lax.broadcasted_iota(jnp.int32, (cy, cz), 1)
    lane1 = lax.broadcasted_iota(jnp.int32, (1, cz), 1)
    lane8 = lax.broadcasted_iota(jnp.int32, (8, cz), 1)
    row = lax.broadcasted_iota(jnp.int32, (cy, cz), 0)
    row8 = lax.broadcasted_iota(jnp.int32, (8, cz), 0)
    layer = lax.broadcasted_iota(jnp.int32, (cx, cz), 0)
    lane_x = lax.broadcasted_iota(jnp.int32, (cx, cz), 1)
    ends = (lane == 0) | (lane == cz - 1)

    def turn(values, by, axis=1):
        by = by % values.shape[axis]
        return values if by == 0 else pltpu.roll(values, by, axis=axis)

    loads[0].wait()
    for copy in loads[3:]:
        copy.wait()
    pair = (
        lax.broadcasted_iota(jnp.int32, (cz, cz), 0) // 2
        == lax.broadcasted_iota(jnp.int32, (cz, cz), 1) % (cz // 2)
    )
    pair = jnp.where(pair, 0.25, 0.0).astype(jnp.bfloat16)
    for b in range(blocks):
        sums_v[b * cy:(b + 1) * cy] = (
            face_v[b, pl.ds(0, cy, stride=2), :] + face_v[b, pl.ds(1, cy, stride=2), :]
        )
    whole = sums_v[...]
    high = whole.astype(jnp.bfloat16)
    rest = whole - high.astype(F32)
    middle = rest.astype(jnp.bfloat16)
    column = lax.broadcasted_iota(jnp.int32, (8, cz), 0)
    column = jnp.where(column < 2, column, cz // 2 - 4 + column)
    choice = (lax.broadcasted_iota(jnp.int32, (8, cz), 1) // 2 == column) & (column < cz // 2)
    choice = jnp.where(choice, 0.25, 0.0).astype(jnp.bfloat16)

    def columns_of(values):
        return lax.dot_general(
            choice, values, (((1,), (1,)), ((), ())), preferred_element_type=F32
        )

    columns = columns_of(middle) + columns_of(high)
    sums_v[...] = (
        jnp.dot(middle, pair, preferred_element_type=F32)
        + jnp.dot(high, pair, preferred_element_type=F32)
    )

    target = [rank_ref[b] for b in range(blocks)]
    alive = [live_ref[0, 0, 0] > b for b in range(blocks)]
    position = []
    for b in range(blocks):
        count = jnp.int32(0)
        for before in range(b):
            count = count + jnp.where((target[before] == target[b]) & alive[before], 1, 0)
        position.append(count)
    edges = []
    for b in range(blocks):
        here = columns[:, b // 2 * cz:b // 2 * cz + cz]
        there = pltpu.roll(here, cz // 2, axis=1)
        first, last = (here, there) if b % 2 == 0 else (there, here)
        even = jnp.where(lane1 < cz // 2, first[0:1], last[1:2])
        other = jnp.where(lane1 < cz // 2, first[3:4], last[2:3])
        edges.append(jnp.where(lax.rem(tile_ref[b], 2) == 0, even, other))
    cards = []
    for b in range(blocks):
        card = jnp.where(row8 < 6, edges[b], (tile_ref[b] + 1).astype(F32))
        for place, y in enumerate((0, 1, cy - 2, cy - 1)):
            card = jnp.where(row8 == place, sums_v[b * cy + y:b * cy + y + 1], card)
        cards.append(card)
    slot0 = jnp.where(row8 == 4, 1, jnp.where(row8 == 5, 0, jnp.where(lane8 < cz // 2, 1, 0)))
    slot0 = slot0.astype(F32)
    slot1 = 1.0 - slot0
    boxes = ((send_v, recv_v), (scard_v, rcard_v))

    def exchange(order, slots, offset):
        src, dst = boxes[order]
        return pltpu.make_async_remote_copy(
            src_ref=src.at[slots], dst_ref=dst.at[slots],
            send_sem=a2a_send.at[order], recv_sem=a2a_recv.at[order],
            device_id=across(offset), device_id_type=MESH,
        )

    pl.semaphore_wait(barrier, greeted())
    shares = {}
    for k in reversed(range(group)):
        dest = across({"gx": k})["gx"] if k else at["gx"]
        total = jnp.zeros((8, cz), F32)
        for b in range(blocks):
            code = jnp.where(alive[b] & (target[b] == dest), position[b], CAP)
            left, right = jnp.where(code == 0, 1.0, 0.0), jnp.where(code == 1, 1.0, 0.0)
            shares[k, b] = left, right
            total = total + cards[b] * (slot0 * left + slot1 * right)
        (rcard_v if k == 0 else scard_v)[k] = total
        if k:
            exchange(1, pl.ds(k, 1), {"gx": k}).start()
    for k in reversed(range(group)):
        total = jnp.zeros((cy, cz), F32)
        for b in range(blocks):
            left, right = shares[k, b]
            values = sums_v[b * cy:(b + 1) * cy]
            total = total + values * jnp.where(lane1 < cz // 2, left, right)
        (recv_v if k == 0 else send_v)[k] = total
        if k:
            exchange(0, pl.ds(k, 1), {"gx": k}).start()
    arrivals = [
        exchange(order, pl.ds(1, group - 1), {"gx": 1}) for order in (1, 0) if group > 1
    ]
    greet(relay_sem.at[0])
    loads[1].wait()
    loads[2].wait()

    for x in range(cx):
        for place, y in enumerate((0, 1, cy - 2, cy - 1)):
            rows_v[place, x:x + 1] = load_v[x, y:y + 1]
        for place, y in enumerate((0, cy - 1)):
            drows_v[place, x:x + 1] = diag_v[x, y:y + 1]
    upper, lower = jnp.zeros((cy, cz), F32), jnp.zeros((cy, cz), F32)
    for x in range(cx):
        plane, weights = load_v[x], diag_v[x]
        for side in range(2):
            spot = cx * side + x
            upper = jnp.where(lane == spot, turn(plane, spot + side), upper)
            lower = jnp.where(lane == spot, turn(plane, spot + 3 * side - 1), lower)
            spot = spot + 2 * cx
            upper = jnp.where(lane == spot, turn(weights, spot + side), upper)
    cols_v[...] = jnp.concatenate([upper, lower], axis=0).T[:4 * cx]

    for relay in range(relays):
        pl.semaphore_wait(relay_sem.at[relay], greeted(min(relay + 1, 2)))
        if relay < relays - 1:
            greet(relay_sem.at[relay + 1], 2)
    for copy in arrivals[:1]:
        copy.wait_recv()

    received, sources = [], []
    for k in range(group):
        card = rcard_v[k]
        swapped = pltpu.roll(card, cz // 2, axis=1)
        received += [(card, card[6:7] - 1.0), (swapped, swapped[6:7] - 1.0)]
        sources += [(recv_v.at[k], received[-2][1]), (turned_v.at[k], received[-1][1])]
    half1 = jnp.where(lane1 >= cz // 2, 1, 0)

    def scatter(x):
        want = (2 * x + half1).astype(F32)
        plane = load_v[x]
        for values, tags in sources:
            plane = plane + jnp.where(tags == want, values[...], 0.0)
        load_v[x] = plane

    def inside(src, x):
        plane = src[x]
        around = jnp.where(lane == 0, 0.0, pltpu.roll(plane, 1, axis=1))
        around = around + jnp.where(lane == cz - 1, 0.0, pltpu.roll(plane, cz - 1, axis=1))
        around = around + jnp.where(row == 0, 0.0, pltpu.roll(plane, 1, axis=0))
        around = around + jnp.where(row == cy - 1, 0.0, pltpu.roll(plane, cy - 1, axis=0))
        if x > 0:
            around = around + src[x - 1]
        if x < cx - 1:
            around = around + src[x + 1]
        return diag_v[x] * plane - around

    want = (2 * layer + jnp.where(lane_x >= cz // 2, 1, 0)).astype(F32)
    faces = [rows_v[place] for place in range(4)]
    for card, tags in received:
        hit = jnp.broadcast_to(tags, (cx, cz)) == want
        for place in range(4):
            spread = jnp.broadcast_to(card[place:place + 1], (cx, cz))
            faces[place] = faces[place] + jnp.where(hit, spread, 0.0)
    for side in range(2):
        face, second = faces[3 * side], faces[1 + side]
        around = jnp.where(lane_x == 0, 0.0, pltpu.roll(face, 1, axis=1)) + second
        around = around + jnp.where(lane_x == cz - 1, 0.0, pltpu.roll(face, cz - 1, axis=1))
        around = around + jnp.where(layer == 0, 0.0, pltpu.roll(face, 1, axis=0))
        around = around + jnp.where(layer == cx - 1, 0.0, pltpu.roll(face, cx - 1, axis=0))
        ysend_v[side, 0] = face
        ysend_v[side, 1] = drows_v[side] * face - around
        for s in range(2):
            xy_v[2 * s + side] = face[(cx - 1) * s:(cx - 1) * s + 1]
    send("xy")
    send("y")

    line = lax.broadcasted_iota(jnp.int32, (2 * cx, cz), 0)
    lane_z = lax.broadcasted_iota(jnp.int32, (2 * cx, cz), 1)
    own_tile = (2 * (line % cx) + line // cx).astype(F32)
    turned = cols_v[:2 * cx]
    for k in range(group):
        card, tags = received[2 * k]
        for place in range(CAP):
            tag = tags[:, :1] if place == 0 else tags[:, cz - 1:]
            hit = jnp.broadcast_to(tag, (2 * cx, cz)) == own_tile
            values = jnp.broadcast_to(card[4 + place:5 + place], (2 * cx, cz))
            turned = turned + jnp.where(hit, values, 0.0)
    around = jnp.where(lane_z == 0, 0.0, turn(turned, 1)) + turn(turned, cz // 2)
    around = around + jnp.where(lane_z == cy - 1, 0.0, turn(turned, -1))
    around = around + jnp.where(line % cx == 0, 0.0, turn(turned, 1, 0))
    around = around + jnp.where(line % cx == cx - 1, 0.0, turn(turned, -1, 0))
    image = cols_v[2 * cx:] * turned - around
    deeper = turn(turned, cz // 2)
    turned = jnp.where(lane_z < cy, turned, turn(image, cz // 2))
    for side in range(2):
        zsend_v[side] = turned[cx * side:cx * side + cx]
    send("z")
    groups = cx // 8
    tile = jnp.zeros((8, cz), F32)
    for side in range(2):
        for part in range(groups):
            spot = 2 * (groups * side + part)
            piece = turn(ysend_v[side, 0, 8 * part:8 * part + 8], spot + 1)
            tile = jnp.where(lane8 // 2 == spot // 2, piece, tile)
        for s in range(2):
            spot = cx * side + (cx - 1) * s
            xz_v[2 * s + side] = turned[spot:spot + 1]
            xr_v[s, 2 * side] = turned[spot:spot + 1]
            xr_v[s, 2 * side + 1] = deeper[spot:spot + 1]
    yz_v[...] = tile
    for name in ("yz", "xz", "xr"):
        send(name)

    for copy in arrivals[1:]:
        copy.wait_recv()
    for k in range(group):
        turned_v[k] = pltpu.roll(recv_v[k], cz // 2, axis=1)

    for x in (0, cx - 1):
        scatter(x)
    send("x", 0)
    for x in (1, cx - 2):
        scatter(x)
    for x in (0, cx - 1):
        p_v[x] = inside(load_v, x)
    send("x", 1)

    def fold(acc, values):
        for part in range(cy // 8):
            acc = acc + values[8 * part:8 * part + 8]
        return acc

    for x in range(2, cx - 2):
        scatter(x)
    for x in range(1, cx - 1):
        p_v[x] = inside(load_v, x)
    acc = [jnp.zeros((8, cz), F32) for _ in range(4)]
    for x in range(cx):
        q_v[x] = inside(p_v, x)
    for x in range(cx):
        load, p, q = load_v[x], p_v[x], q_v[x]
        pairs = ((load, load), (load, p), (p, p), (p, q))
        acc = [fold(total, one * other) for total, (one, other) in zip(acc, pairs)]
    image = jnp.zeros((cy, cz), F32)
    for x in range(cx):
        q = q_v[x]
        for side in range(2):
            y = (cy - 1) * side
            qrows_v[side, x:x + 1] = q_v[x, y:y + 1]
            spot = cx * side + x
            image = jnp.where(lane == spot, turn(q, spot + side), image)
    qcols_v[...] = jnp.concatenate([image, jnp.zeros((cz - cy, cz), F32)], axis=0).T[:2 * cx]

    def rim(plane, first, last):
        top = plane[:8] - jnp.where(row8 == 0, first, 0.0)
        bottom = plane[cy - 8:] - jnp.where(row8 == 7, last, 0.0)
        return jnp.concatenate([top, plane[8:cy - 8], bottom], axis=0)

    settle(lambda copy: copy.wait_recv())
    there = {
        (axis, side): jnp.where(near(axis, side), 1.0, 0.0) for axis in AXES for side in range(2)
    }
    def add(at_sum, values):
        for part in range(values.shape[0] // 8):
            acc[at_sum] = acc[at_sum] + values[8 * part:8 * part + 8]

    def face_sums(h, halo, load, p, q, stencil):
        add(1, -(load * h))
        add(2, h * (h - 2.0 * p))
        add(3, h * (stencil + halo - 2.0 * q) - p * halo)

    rows = [jnp.zeros((1, cz), F32) for _ in range(4)]
    for side in range(2):
        x = (cx - 1) * side
        h, load = hx_v[side, 0], load_v[x]
        around = jnp.where(lane == 0, 0.0, turn(h, 1))
        around = around + jnp.where(lane == cz - 1, 0.0, turn(h, -1))
        around = around + jnp.where(row == 0, 0.0, turn(h, 1, 0))
        around = around + jnp.where(row == cy - 1, 0.0, turn(h, -1, 0))
        halo = hx_v[side, 1] - there["gx", side] * load
        face_sums(h, halo, load, p_v[x], q_v[x], diag_v[x] * h - around)
    y_halo = []
    for side in range(2):
        halo = hy_v[side, 1] - there["gy", side] * ysend_v[side, 0]
        halo = halo - jnp.where(layer == 0, 2.0 * hxy_v[side], 0.0)
        y_halo.append(halo - jnp.where(layer == cx - 1, 2.0 * hxy_v[2 + side], 0.0))
    halves = []
    for side in range(2):
        halo = hz_v[side] - there["gz", side] * turn(zsend_v[side], cz // 2)
        for s in range(2):
            corner = turn(jnp.broadcast_to(hxz_v[2 * s + side], (8, cz)), cz // 2)[:1]
            halo = halo - jnp.where(layer == (cx - 1) * s, 2.0 * corner, 0.0)
        parts = []
        for part in range(groups):
            piece = halo[8 * part:8 * part + 8]
            for s in range(2):
                spot = 2 * (groups * (1 - s) + part) + side
                goal = cy if s == 0 else 2 * cy - 1
                corner = turn(hyz_v[2 * s + side], goal - spot)
                piece = piece - jnp.where(lane8 == goal, 2.0 * corner, 0.0)
            parts.append(piece)
        halves.append(jnp.concatenate(parts, axis=0))

    y_stencil = []
    for side in range(2):
        h = hy_v[side, 0]
        around = jnp.where(lane_x == 0, 0.0, turn(h, 1))
        around = around + jnp.where(lane_x == cz - 1, 0.0, turn(h, -1))
        around = around + jnp.where(layer == 0, 0.0, turn(h, 1, 0))
        around = around + jnp.where(layer == cx - 1, 0.0, turn(h, -1, 0))
        y_stencil.append(drows_v[side] * h - around)
        face_sums(
            h, y_halo[side], ysend_v[side, 0], ysend_v[side, 1], qrows_v[side], y_stencil[side]
        )
    z_stencil, z_h, z_halves = [], [], []
    used = lane_x < cy
    for side in range(2):
        h = jnp.where(used, hz_v[side], 0.0)
        halo = jnp.where(used, turn(halves[side], cz // 2), 0.0)
        around = turn(h, 1) + jnp.where(lane_x == cz - 1, 0.0, turn(h, -1))
        around = around + jnp.where(layer == 0, 0.0, turn(h, 1, 0))
        around = around + jnp.where(layer == cx - 1, 0.0, turn(h, -1, 0))
        span = pl.ds(cx * side, cx)
        z_stencil.append(cols_v[pl.ds(2 * cx + cx * side, cx)] * h - around)
        z_h.append(h)
        z_halves.append(halo)
        own_p = turn(zsend_v[side], cz // 2)
        face_sums(h, halo, zsend_v[side], own_p, qcols_v[span], z_stencil[side])

    def edge_sums(one, one_in, one_halo, other, other_halo, other_stencil):
        second = 2.0 * one * other
        third = 2.0 * (one * other_stencil - one_in * other)
        return second, third + one * other_halo + other * one_halo

    for s in range(2):
        x = (cx - 1) * s
        for t in range(2):
            y, y_in = ((0, 1), (cy - 1, cy - 2))[t]
            second, third = edge_sums(
                hx_v[s, 0, y:y + 1], hx_v[s, 0, y_in:y_in + 1],
                hx_v[s, 1, y:y + 1] - there["gx", s] * load_v[x, y:y + 1],
                hy_v[t, 0, x:x + 1], y_halo[t][x:x + 1], y_stencil[t][x:x + 1],
            )
            rows[2], rows[3] = rows[2] + second, rows[3] + third
            second, third = edge_sums(
                hxr_v[s, 2 * t], hxr_v[s, 2 * t + 1],
                turn(jnp.broadcast_to(hxr_v[s, 2 * t], (8, cz)), cz // 2)[:1]
                - there["gx", s] * zsend_v[t, x:x + 1],
                z_h[t][x:x + 1], z_halves[t][x:x + 1], z_stencil[t][x:x + 1],
            )
            used1 = lane1 < cy
            rows[2] = rows[2] + jnp.where(used1, second, 0.0)
            rows[3] = rows[3] + jnp.where(used1, third, 0.0)
            goal = (cy - 1) * s
            spot, spot_in = ((0, 1), (cz - 1, cz - 2))[t]
            second, third = edge_sums(
                turn(hy_v[s, 0], goal - spot), turn(hy_v[s, 0], goal - spot_in),
                turn(y_halo[s], goal - spot), z_h[t], z_halves[t], z_stencil[t],
            )
            add(2, jnp.where(lane_x == goal, second, 0.0))
            add(3, jnp.where(lane_x == goal, third, 0.0))

    def columned(halves):
        for side in range(2):
            mix_v[pl.ds(1 - side, cx, stride=2), :] = halves[side]
        columns = mix_v[...].T
        return jnp.concatenate([columns, jnp.zeros((cz, cz - 2 * cx), F32)], axis=1)

    def complete():
        settle(lambda copy: copy.wait_send())
        l_halo = columned([hz_v[0], hz_v[1]])[:cy]
        for x in range(cx):
            plane = p_v[x] - jnp.where(ends, turn(l_halo, -2 * x - 1), 0.0)
            plane = rim(plane, hy_v[0, 0, x:x + 1], hy_v[1, 0, x:x + 1])
            for side in range(2):
                if x == (cx - 1) * side:
                    plane = plane - hx_v[side, 0]
            p_v[x] = plane
        z_halo = columned(halves)[cy:2 * cy]
        for x in range(cx):
            plane = inside(p_v, x) - jnp.where(ends, turn(z_halo, -2 * x - 1), 0.0)
            plane = rim(plane, y_halo[0][x:x + 1], y_halo[1][x:x + 1])
            for side in range(2):
                if x == (cx - 1) * side:
                    plane = plane - hx_v[side, 1] + there["gx", side] * load_v[x]
            q_v[x] = plane

    mine = jnp.zeros((8, cz), F32)
    for order in range(4):
        mine = jnp.where(row8 == order, jnp.sum(acc[order], axis=0, keepdims=True) + rows[order], mine)
    mine = mine + pltpu.roll(mine, cz // 2, axis=1)
    mine = mine + pltpu.roll(mine, cz // 4, axis=1)
    own = row8 == lane8 // (cz // 4)
    mine = jnp.sum(jnp.where(own, mine, 0.0), axis=0, keepdims=True)
    slot = 0
    waiting = []
    for order, axes in enumerate(stages):
        part_v[order] = mine
        offsets = offsets_of(sizes, axes)

        def part(offset, src, dst):
            return pltpu.make_async_remote_copy(
                src_ref=src, dst_ref=dst,
                send_sem=red_send.at[order], recv_sem=red_recv.at[order],
                device_id=across(offset), device_id_type=MESH,
            )

        for place, offset in enumerate(offsets):
            part(offset, part_v.at[order], gath_v.at[slot + place]).start()
        if order == 0:
            complete()
        if offsets:
            span = gath_v.at[pl.ds(slot, len(offsets))]
            waiting.append(part(offsets[0], span, span))
            waiting[-1].wait_recv()
        parts = [mine] + [gath_v[slot + place] for place in range(len(offsets))]
        while len(parts) > 1:
            parts = [sum(parts[n:n + 2]) for n in range(0, len(parts), 2)]
        mine = parts[0]
        slot += len(offsets)

    sums = jnp.sum(jnp.where(own, mine, 0.0), axis=1, keepdims=True)
    s0, s1, s2, s3 = (sums[n:n + 1] for n in range(4))
    inverse = 1.0 / (6.0 * s0 + s1)
    a, c, m, third = s0 * inverse, s1 * inverse, s2 * inverse, s3 * inverse
    growth = a * m - c * c
    e = c + growth
    curve = 6.0 * (e * e * a - 2.0 * e * a * c + a * a * m) + (
        e * e * c - 2.0 * e * a * m + a * a * third
    )
    b = a * growth / curve
    x_load, x_p = a + b * e, b * a
    r_load, r_p, r_q = c - 6.0 * b * e, a + b * (e - 6.0 * a), b * a
    for order, value in enumerate((x_load, x_p, r_load, r_p, r_q)):
        coef_ref[order:order + 1] = jnp.broadcast_to(value, (1, cz))
    for copy in arrivals + waiting:
        copy.wait_send()


def combine(load_ref, p_ref, q_ref, coef_ref, x_hbm, r_hbm, x_v, r_v, sem):
    cx = load_ref.shape[0]
    x_load, x_p, r_load, r_p, r_q = (coef_ref[n:n + 1] for n in range(5))
    pieces = 8
    for piece in range(pieces):
        first, last = cx * piece // pieces, cx * (piece + 1) // pieces
        for x in range(first, last):
            load, p = load_ref[x], p_ref[x]
            x_v[x] = x_load * load - x_p * p
            r_v[x] = r_load * load - r_p * p + r_q * q_ref[x]
        span = pl.ds(first, last - first)
        for number, (src, dst) in enumerate(((x_v, x_hbm), (r_v, r_hbm))):
            pltpu.make_async_copy(src.at[span], dst.at[span], sem.at[number]).start()
    for number, (src, dst) in enumerate(((x_v, x_hbm), (r_v, r_hbm))):
        pltpu.make_async_copy(src, dst, sem.at[number]).wait()


def combined(load, p, q, coef):
    cx, cy, cz = load.shape
    box = jax.ShapeDtypeStruct((cx, cy, cz), F32)
    vmem, hbm = (pl.BlockSpec(memory_space=space) for space in (pltpu.VMEM, pltpu.HBM))
    return pl.pallas_call(
        combine,
        out_shape=(box, box),
        in_specs=[vmem] * 4,
        out_specs=(hbm, hbm),
        scratch_shapes=[pltpu.VMEM((cx, cy, cz), F32)] * 2 + [pltpu.SemaphoreType.DMA((2,))],
    )(*(pltpu.with_memory_space_constraint(a, pltpu.VMEM) for a in (load, p, q, coef)))


def per_device(sizes, face_blocks, owner_rank, owner_tile, live_count, right_side, diagonal):
    blocks = face_blocks.shape[3]
    cx, cy, cz = right_side.shape
    group = sizes["gx"]
    stages = stages_of(sizes)
    relays = relays_of(sizes, stages)
    slots = sum(len(offsets_of(sizes, axes)) for axes in stages)
    vmem, hbm = (pl.BlockSpec(memory_space=space) for space in (pltpu.VMEM, pltpu.HBM))
    box = pltpu.VMEM((cx, cy, cz), F32)
    load, p, q, coef = pl.pallas_call(
        functools.partial(kernel, sizes, stages, relays),
        out_shape=(box, box, box, pltpu.VMEM((8, cz), F32)),
        in_specs=[hbm] * 6,
        out_specs=(vmem, vmem, vmem, vmem),
        scratch_shapes=[
            pltpu.SMEM((blocks,), jnp.int32),
            pltpu.SMEM((blocks,), jnp.int32),
            pltpu.SMEM(live_count.shape, jnp.int32),
            pltpu.VMEM((blocks, 2 * cy, cz), F32),
            pltpu.VMEM((cx, cy, cz), F32),
            pltpu.VMEM((blocks * cy, cz), F32),
            pltpu.VMEM((group, cy, cz), F32),
            pltpu.VMEM((group, 8, cz), F32),
            pltpu.VMEM((group, cy, cz), F32),
            pltpu.VMEM((group, 8, cz), F32),
            pltpu.VMEM((group, cy, cz), F32),
            pltpu.VMEM((4, cx, cz), F32),
            pltpu.VMEM((2, cx, cz), F32),
            pltpu.VMEM((4 * cx, cz), F32),
            pltpu.VMEM((2, 2, cy, cz), F32),
            pltpu.VMEM((2, 4, 1, cz), F32),
            pltpu.VMEM((2, 4, 1, cz), F32),
            pltpu.VMEM((2, cx, cz), F32),
            pltpu.VMEM((2 * cx, cz), F32),
            pltpu.VMEM((2, 2, cx, cz), F32),
            pltpu.VMEM((2, 2, cx, cz), F32),
            pltpu.VMEM((2, cx, cz), F32),
            pltpu.VMEM((2, cx, cz), F32),
            pltpu.VMEM((4, 1, cz), F32),
            pltpu.VMEM((4, 1, cz), F32),
            pltpu.VMEM((8, cz), F32),
            pltpu.VMEM((4, 8, cz), F32),
            pltpu.VMEM((4, 1, cz), F32),
            pltpu.VMEM((4, 1, cz), F32),
            pltpu.VMEM((2 * cx, cz), F32),
            pltpu.VMEM((message_rows(cx, cy, 2, 2, 2), 1, cz), F32),
            pltpu.VMEM((len(stages), 1, cz), F32),
            pltpu.VMEM((slots, 1, cz), F32),
            pltpu.SemaphoreType.DMA((6,)),
            pltpu.SemaphoreType.DMA((2,)),
            pltpu.SemaphoreType.DMA((2,)),
            pltpu.SemaphoreType.REGULAR((relays,)),
            pltpu.SemaphoreType.DMA((1,)),
            pltpu.SemaphoreType.DMA((1,)),
            pltpu.SemaphoreType.DMA((len(stages),)),
            pltpu.SemaphoreType.DMA((len(stages),)),
        ],
        compiler_params=pltpu.CompilerParams(collective_id=0, has_side_effects=True),
    )(
        owner_rank.reshape(blocks), owner_tile.reshape(blocks),
        live_count,
        face_blocks.reshape(blocks, 2 * cy, cz), right_side, diagonal,
    )
    return combined(load, p, q, coef)


def solution(mesh):
    sizes = dict(mesh.shape)
    return jax.shard_map(
        functools.partial(per_device, sizes),
        mesh=mesh,
        in_specs=(
            P("gx", "gy", "gz", None, None),
            P("gx", "gy", "gz", None, None),
            P("gx", "gy", "gz", None),
            P("gx", "gy", "gz"),
            P("gx", "gy", "gz"),
            P("gx", "gy", "gz"),
        ),
        out_specs=(P("gx", "gy", "gz"), P("gx", "gy", "gz")),
        check_vma=False,
    )
```

```python
import functools
import math

import jax
import jax.numpy as jnp
from jax import lax
from jax.experimental import pallas as pl
from jax.experimental.pallas import tpu as pltpu
from jax.sharding import PartitionSpec as P

CAP = 2
AXES = ("gx", "gy", "gz")
MESH = pl.DeviceIdType.MESH
F32 = jnp.float32


def offsets_of(sizes, axes):
    found = [()]
    for axis in axes:
        found = [done + (step,) for done in found for step in range(sizes[axis])]
    offsets = [dict(zip(axes, steps)) for steps in found if any(steps)]
    return sorted(
        offsets, key=lambda o: -sum(s if a != "gx" else s / sizes[a] for a, s in o.items())
    )


def stages_of(sizes):
    stages = []
    for axis in ("gx", "gz", "gy"):
        if stages and math.prod(sizes[a] for a in stages[-1] + [axis]) <= 32:
            stages[-1].append(axis)
        else:
            stages.append([axis])
    return stages


def relays_of(sizes, stages):
    rounds = 2
    for axes in stages:
        steps = [sizes[axis] - 1 for axis in axes if axis != "gx"]
        single = sum(n % 2 for n in steps) + (1 if "gx" in axes and sizes["gx"] > 1 else 0)
        rounds = max(rounds, 1 + sum(n // 2 for n in steps) + max(0, single - 2))
    return rounds


def message_rows(cx, cy, nx, ny, nz):
    rest = 4 * nx + 2 * cx * ny + cx * nz + nx * ny + nx * nz + 8 * ny * nz
    return 2 * cy * nx, rest


def kernel(
    sizes, stages, relays,
    rank_hbm, tile_hbm, live_hbm, face_hbm, right_hbm, diag_hbm,
    load_v, p_v, q_v, coef_ref,
    rank_ref, tile_ref, live_ref, face_v, diag_v, sums_v,
    send_v, scard_v, recv_v, rcard_v, turned_v, rows_v, drows_v, cols_v,
    hx_v, xr_v, hxr_v, qrows_v, qcols_v, ysend_v, hy_v, zsend_v, hz_v, xy_v, hxy_v, yz_v, hyz_v, xz_v, hxz_v, mix_v, tally_v, part_v, gath_v,
    in_sem, a2a_send, a2a_recv, relay_sem, halo_send, halo_recv, red_send, red_recv,
):
    cx, cy, cz = load_v.shape
    blocks = face_v.shape[0]
    group = sizes["gx"]
    at = {axis: lax.axis_index(axis) for axis in AXES}

    def near(axis, side):
        return at[axis] > 0 if side == 0 else at[axis] < sizes[axis] - 1

    def beside(offset):
        return {a: lax.rem(at[a] + s, sizes[a]) for a, s in offset.items() if s}

    def across(offset):
        where = {}
        for axis, step in offset.items():
            if sizes[axis] & (sizes[axis] - 1):
                where[axis] = lax.rem(at[axis] + step, sizes[axis])
            else:
                where[axis] = at[axis]
                for bit in (1 << n for n in range(sizes[axis].bit_length())):
                    if step & bit:
                        where[axis] = where[axis] + bit - 2 * bit * lax.rem(at[axis] // bit, 2)
        return {axis: index for axis, index in where.items() if offset[axis]}

    def near_all(sides):
        found = near(*sides[0])
        for axis, side in sides[1:]:
            found = found & near(axis, side)
        return found

    loads = [
        pltpu.make_async_copy(face_hbm, face_v, in_sem.at[0]),
        pltpu.make_async_copy(right_hbm, load_v, in_sem.at[1]),
        pltpu.make_async_copy(diag_hbm, diag_v, in_sem.at[2]),
        pltpu.make_async_copy(live_hbm, live_ref, in_sem.at[3]),
        pltpu.make_async_copy(rank_hbm, rank_ref, in_sem.at[4]),
        pltpu.make_async_copy(tile_hbm, tile_ref, in_sem.at[5]),
    ]
    for copy in loads:
        copy.start()

    def within(axis, step):
        return at[axis] + step >= 0 if step < 0 else at[axis] + step < sizes[axis]

    def greet(semaphore, reach=1):
        for k in range(1, group):
            pl.semaphore_signal(
                semaphore, inc=1, device_id=beside({"gx": k}), device_id_type=MESH
            )
        for axis in ("gy", "gz"):
            for step in range(-reach, reach + 1):
                if 0 < abs(step) < sizes[axis]:
                    @pl.when(within(axis, step))
                    def _():
                        pl.semaphore_signal(
                            semaphore, inc=1, device_id={axis: at[axis] + step},
                            device_id_type=MESH,
                        )

    def greeted(reach=1):
        count = jnp.int32(group - 1)
        for axis in ("gy", "gz"):
            for step in range(-reach, reach + 1):
                if 0 < abs(step) < sizes[axis]:
                    count = count + jnp.where(within(axis, step), 1, 0)
        return count

    barrier = pltpu.get_barrier_semaphore()
    greet(barrier)

    messages = {"x": [], "z": [], "y": [], "xr": [], "xy": [], "xz": [], "yz": []}
    for s in range(2):
        end = (cx - 1) * s
        messages["x"].append(((("gx", s),), load_v.at[end], lambda s: hx_v.at[s, 0]))
        messages["x"].append(((("gx", s),), p_v.at[end], lambda s: hx_v.at[s, 1]))
        messages["xr"].append(((("gx", s),), xr_v.at[s], lambda s: hxr_v.at[s]))
        messages["y"].append(((("gy", s),), ysend_v.at[s], lambda s: hy_v.at[s]))
        messages["z"].append(((("gz", s),), zsend_v.at[s], lambda s: hz_v.at[s]))
        for t in range(2):
            messages["xy"].append(
                ((("gx", s), ("gy", t)), xy_v.at[2 * s + t], lambda s, t: hxy_v.at[2 * s + t])
            )
            messages["xz"].append(
                ((("gx", s), ("gz", t)), xz_v.at[2 * s + t], lambda s, t: hxz_v.at[2 * s + t])
            )
            messages["yz"].append(
                ((("gy", s), ("gz", t)), yz_v, lambda s, t: hyz_v.at[2 * s + t])
            )

    def kind_of(name):
        return 0 if name == "x" else 1

    def send(name, part=None):
        for order, (sides, src, place) in enumerate(messages[name]):
            if part in (None, order % 2):
                @pl.when(near_all(sides))
                def _():
                    pltpu.make_async_remote_copy(
                        src_ref=src, dst_ref=place(*[1 - side for _, side in sides]),
                        send_sem=halo_send.at[kind_of(name)],
                        recv_sem=halo_recv.at[kind_of(name)],
                        device_id={
                            axis: lax.rem(
                                at[axis] + (1 if side else sizes[axis] - 1), sizes[axis]
                            )
                            for axis, side in sides
                        },
                        device_id_type=MESH,
                    ).start()

    def settle(kind, act):
        beside_on = {
            axis: sum(jnp.where(near(axis, side), 1, 0) for side in range(2)) for axis in AXES
        }
        counts = [range(min(1, sizes[axis] - 1), min(2, sizes[axis] - 1) + 1) for axis in AXES]
        for nx in counts[0]:
            for ny in counts[1] if kind else (0,):
                for nz in counts[2] if kind else (0,):
                    lines = message_rows(cx, cy, nx, ny, nz)[kind]
                    found = beside_on["gx"] == nx
                    if kind:
                        found = found & (beside_on["gy"] == ny) & (beside_on["gz"] == nz)
                    if lines:
                        @pl.when(found)
                        def _():
                            span = tally_v.at[pl.ds(0, lines)]
                            act(pltpu.make_async_remote_copy(
                                src_ref=span, dst_ref=span,
                                send_sem=halo_send.at[kind], recv_sem=halo_recv.at[kind],
                                device_id=beside({"gx": 1}), device_id_type=MESH,
                            ))

    for name in messages:
        for sides, _, place in messages[name]:
            slot = place(*[side for _, side in sides])

            @pl.when(jnp.logical_not(near_all(sides)))
            def _():
                slot[...] = jnp.zeros(slot.shape, F32)

    lane = lax.broadcasted_iota(jnp.int32, (cy, cz), 1)
    lane1 = lax.broadcasted_iota(jnp.int32, (1, cz), 1)
    lane8 = lax.broadcasted_iota(jnp.int32, (8, cz), 1)
    row = lax.broadcasted_iota(jnp.int32, (cy, cz), 0)
    row8 = lax.broadcasted_iota(jnp.int32, (8, cz), 0)
    layer = lax.broadcasted_iota(jnp.int32, (cx, cz), 0)
    lane_x = lax.broadcasted_iota(jnp.int32, (cx, cz), 1)
    ends = (lane == 0) | (lane == cz - 1)

    def turn(values, by, axis=1):
        by = by % values.shape[axis]
        return values if by == 0 else pltpu.roll(values, by, axis=axis)

    loads[0].wait()
    for copy in loads[3:]:
        copy.wait()
    pair = (
        lax.broadcasted_iota(jnp.int32, (cz, cz), 0) // 2
        == lax.broadcasted_iota(jnp.int32, (cz, cz), 1) % (cz // 2)
    )
    pair = jnp.where(pair, 0.25, 0.0).astype(jnp.bfloat16)
    for b in range(blocks):
        sums_v[b * cy:(b + 1) * cy] = (
            face_v[b, pl.ds(0, cy, stride=2), :] + face_v[b, pl.ds(1, cy, stride=2), :]
        )
    whole = sums_v[...]
    high = whole.astype(jnp.bfloat16)
    rest = whole - high.astype(F32)
    middle = rest.astype(jnp.bfloat16)
    column = lax.broadcasted_iota(jnp.int32, (8, cz), 0)
    column = jnp.where(column < 2, column, cz // 2 - 4 + column)
    choice = (lax.broadcasted_iota(jnp.int32, (8, cz), 1) // 2 == column) & (column < cz // 2)
    choice = jnp.where(choice, 0.25, 0.0).astype(jnp.bfloat16)

    def columns_of(values):
        return lax.dot_general(
            choice, values, (((1,), (1,)), ((), ())), preferred_element_type=F32
        )

    columns = columns_of(middle) + columns_of(high)
    sums_v[...] = (
        jnp.dot(middle, pair, preferred_element_type=F32)
        + jnp.dot(high, pair, preferred_element_type=F32)
    )

    target = [rank_ref[b] for b in range(blocks)]
    alive = [live_ref[0, 0, 0] > b for b in range(blocks)]
    position = []
    for b in range(blocks):
        count = jnp.int32(0)
        for before in range(b):
            count = count + jnp.where((target[before] == target[b]) & alive[before], 1, 0)
        position.append(count)
    edges = []
    for b in range(blocks):
        here = columns[:, b // 2 * cz:b // 2 * cz + cz]
        there = pltpu.roll(here, cz // 2, axis=1)
        first, last = (here, there) if b % 2 == 0 else (there, here)
        even = jnp.where(lane1 < cz // 2, first[0:1], last[1:2])
        other = jnp.where(lane1 < cz // 2, first[3:4], last[2:3])
        edges.append(jnp.where(lax.rem(tile_ref[b], 2) == 0, even, other))
    cards = []
    for b in range(blocks):
        card = jnp.where(row8 < 6, edges[b], (tile_ref[b] + 1).astype(F32))
        for place, y in enumerate((0, 1, cy - 2, cy - 1)):
            card = jnp.where(row8 == place, sums_v[b * cy + y:b * cy + y + 1], card)
        cards.append(card)
    slot0 = jnp.where(row8 == 4, 1, jnp.where(row8 == 5, 0, jnp.where(lane8 < cz // 2, 1, 0)))
    slot0 = slot0.astype(F32)
    slot1 = 1.0 - slot0
    boxes = ((send_v, recv_v), (scard_v, rcard_v))

    def exchange(order, slots, offset):
        src, dst = boxes[order]
        return pltpu.make_async_remote_copy(
            src_ref=src.at[slots], dst_ref=dst.at[slots],
            send_sem=a2a_send.at[order], recv_sem=a2a_recv.at[order],
            device_id=across(offset), device_id_type=MESH,
        )

    pl.semaphore_wait(barrier, greeted())
    shares = {}
    for k in reversed(range(group)):
        dest = across({"gx": k})["gx"] if k else at["gx"]
        total = jnp.zeros((8, cz), F32)
        for b in range(blocks):
            code = jnp.where(alive[b] & (target[b] == dest), position[b], CAP)
            left, right = jnp.where(code == 0, 1.0, 0.0), jnp.where(code == 1, 1.0, 0.0)
            shares[k, b] = left, right
            total = total + cards[b] * (slot0 * left + slot1 * right)
        (rcard_v if k == 0 else scard_v)[k] = total
        if k:
            exchange(1, pl.ds(k, 1), {"gx": k}).start()
    for k in reversed(range(group)):
        total = jnp.zeros((cy, cz), F32)
        for b in range(blocks):
            left, right = shares[k, b]
            values = sums_v[b * cy:(b + 1) * cy]
            total = total + values * jnp.where(lane1 < cz // 2, left, right)
        (recv_v if k == 0 else send_v)[k] = total
        if k:
            exchange(0, pl.ds(k, 1), {"gx": k}).start()
    arrivals = [
        exchange(order, pl.ds(1, group - 1), {"gx": 1}) for order in (1, 0) if group > 1
    ]
    greet(relay_sem.at[0])
    loads[1].wait()
    loads[2].wait()

    for x in range(cx):
        for place, y in enumerate((0, 1, cy - 2, cy - 1)):
            rows_v[place, x:x + 1] = load_v[x, y:y + 1]
        for place, y in enumerate((0, cy - 1)):
            drows_v[place, x:x + 1] = diag_v[x, y:y + 1]
    upper, lower = jnp.zeros((cy, cz), F32), jnp.zeros((cy, cz), F32)
    for x in range(cx):
        plane, weights = load_v[x], diag_v[x]
        for side in range(2):
            spot = cx * side + x
            upper = jnp.where(lane == spot, turn(plane, spot + side), upper)
            lower = jnp.where(lane == spot, turn(plane, spot + 3 * side - 1), lower)
            spot = spot + 2 * cx
            upper = jnp.where(lane == spot, turn(weights, spot + side), upper)
    cols_v[...] = jnp.concatenate([upper, lower], axis=0).T[:4 * cx]

    def hear(relay):
        pl.semaphore_wait(relay_sem.at[relay], greeted(min(relay + 1, 2)))
        if relay < relays - 1:
            greet(relay_sem.at[relay + 1], 2)

    hear(0)
    for copy in arrivals[:1]:
        copy.wait_recv()

    received, sources = [], []
    for k in range(group):
        card = rcard_v[k]
        swapped = pltpu.roll(card, cz // 2, axis=1)
        received += [(card, card[6:7] - 1.0), (swapped, swapped[6:7] - 1.0)]
        sources += [(recv_v.at[k], received[-2][1]), (turned_v.at[k], received[-1][1])]
    half1 = jnp.where(lane1 >= cz // 2, 1, 0)

    def scatter(x):
        want = (2 * x + half1).astype(F32)
        plane = load_v[x]
        for values, tags in sources:
            plane = plane + jnp.where(tags == want, values[...], 0.0)
        load_v[x] = plane

    def inside(src, x):
        plane = src[x]
        around = jnp.where(lane == 0, 0.0, pltpu.roll(plane, 1, axis=1))
        around = around + jnp.where(lane == cz - 1, 0.0, pltpu.roll(plane, cz - 1, axis=1))
        around = around + jnp.where(row == 0, 0.0, pltpu.roll(plane, 1, axis=0))
        around = around + jnp.where(row == cy - 1, 0.0, pltpu.roll(plane, cy - 1, axis=0))
        if x > 0:
            around = around + src[x - 1]
        if x < cx - 1:
            around = around + src[x + 1]
        return diag_v[x] * plane - around

    want = (2 * layer + jnp.where(lane_x >= cz // 2, 1, 0)).astype(F32)
    faces = [rows_v[place] for place in range(4)]
    for card, tags in received:
        hit = jnp.broadcast_to(tags, (cx, cz)) == want
        for place in range(4):
            spread = jnp.broadcast_to(card[place:place + 1], (cx, cz))
            faces[place] = faces[place] + jnp.where(hit, spread, 0.0)
    for side in range(2):
        face, second = faces[3 * side], faces[1 + side]
        around = jnp.where(lane_x == 0, 0.0, pltpu.roll(face, 1, axis=1)) + second
        around = around + jnp.where(lane_x == cz - 1, 0.0, pltpu.roll(face, cz - 1, axis=1))
        around = around + jnp.where(layer == 0, 0.0, pltpu.roll(face, 1, axis=0))
        around = around + jnp.where(layer == cx - 1, 0.0, pltpu.roll(face, cx - 1, axis=0))
        ysend_v[side, 0] = face
        ysend_v[side, 1] = drows_v[side] * face - around
        for s in range(2):
            xy_v[2 * s + side] = face[(cx - 1) * s:(cx - 1) * s + 1]
    send("xy")
    send("y")

    line = lax.broadcasted_iota(jnp.int32, (2 * cx, cz), 0)
    lane_z = lax.broadcasted_iota(jnp.int32, (2 * cx, cz), 1)
    own_tile = (2 * (line % cx) + line // cx).astype(F32)
    turned = cols_v[:2 * cx]
    for k in range(group):
        card, tags = received[2 * k]
        for place in range(CAP):
            tag = tags[:, :1] if place == 0 else tags[:, cz - 1:]
            hit = jnp.broadcast_to(tag, (2 * cx, cz)) == own_tile
            values = jnp.broadcast_to(card[4 + place:5 + place], (2 * cx, cz))
            turned = turned + jnp.where(hit, values, 0.0)
    around = jnp.where(lane_z == 0, 0.0, turn(turned, 1)) + turn(turned, cz // 2)
    around = around + jnp.where(lane_z == cy - 1, 0.0, turn(turned, -1))
    around = around + jnp.where(line % cx == 0, 0.0, turn(turned, 1, 0))
    around = around + jnp.where(line % cx == cx - 1, 0.0, turn(turned, -1, 0))
    image = cols_v[2 * cx:] * turned - around
    deeper = turn(turned, cz // 2)
    turned = jnp.where(lane_z < cy, turned, turn(image, cz // 2))
    for side in range(2):
        zsend_v[side] = turned[cx * side:cx * side + cx]
    send("z")
    groups = cx // 8
    tile = jnp.zeros((8, cz), F32)
    for side in range(2):
        for part in range(groups):
            spot = 2 * (groups * side + part)
            piece = turn(ysend_v[side, 0, 8 * part:8 * part + 8], spot + 1)
            tile = jnp.where(lane8 // 2 == spot // 2, piece, tile)
        for s in range(2):
            spot = cx * side + (cx - 1) * s
            xz_v[2 * s + side] = turned[spot:spot + 1]
            xr_v[s, 2 * side] = turned[spot:spot + 1]
            xr_v[s, 2 * side + 1] = deeper[spot:spot + 1]
    yz_v[...] = tile
    for name in ("yz", "xz", "xr"):
        send(name)

    for copy in arrivals[1:]:
        copy.wait_recv()
    for k in range(group):
        turned_v[k] = pltpu.roll(recv_v[k], cz // 2, axis=1)

    for x in (0, cx - 1):
        scatter(x)
    send("x", 0)
    for x in (1, cx - 2):
        scatter(x)
    for x in (0, cx - 1):
        p_v[x] = inside(load_v, x)
    send("x", 1)
    for relay in range(1, relays - 1):
        hear(relay)

    def fold(acc, values):
        for part in range(cy // 8):
            acc = acc + values[8 * part:8 * part + 8]
        return acc

    for x in range(2, cx - 2):
        scatter(x)
    for x in range(1, cx - 1):
        p_v[x] = inside(load_v, x)
    acc = [jnp.zeros((8, cz), F32) for _ in range(4)]
    for x in range(cx):
        q_v[x] = inside(p_v, x)
    for x in range(cx):
        load, p, q = load_v[x], p_v[x], q_v[x]
        pairs = ((load, load), (load, p), (p, p), (p, q))
        acc = [fold(total, one * other) for total, (one, other) in zip(acc, pairs)]
    image = jnp.zeros((cy, cz), F32)
    for x in range(cx):
        q = q_v[x]
        for side in range(2):
            y = (cy - 1) * side
            qrows_v[side, x:x + 1] = q_v[x, y:y + 1]
            spot = cx * side + x
            image = jnp.where(lane == spot, turn(q, spot + side), image)
    qcols_v[...] = jnp.concatenate([image, jnp.zeros((cz - cy, cz), F32)], axis=0).T[:2 * cx]

    def rim(plane, first, last):
        top = plane[:8] - jnp.where(row8 == 0, first, 0.0)
        bottom = plane[cy - 8:] - jnp.where(row8 == 7, last, 0.0)
        return jnp.concatenate([top, plane[8:cy - 8], bottom], axis=0)

    settle(1, lambda copy: copy.wait_recv())
    there = {
        (axis, side): jnp.where(near(axis, side), 1.0, 0.0) for axis in AXES for side in range(2)
    }
    def add(at_sum, values):
        for part in range(values.shape[0] // 8):
            acc[at_sum] = acc[at_sum] + values[8 * part:8 * part + 8]

    def face_sums(h, halo, load, p, q, stencil):
        add(1, -(load * h))
        add(2, h * (h - 2.0 * p))
        add(3, h * (stencil + halo - 2.0 * q) - p * halo)

    rows = [jnp.zeros((1, cz), F32) for _ in range(4)]
    y_halo = []
    for side in range(2):
        halo = hy_v[side, 1] - there["gy", side] * ysend_v[side, 0]
        halo = halo - jnp.where(layer == 0, 2.0 * hxy_v[side], 0.0)
        y_halo.append(halo - jnp.where(layer == cx - 1, 2.0 * hxy_v[2 + side], 0.0))
    halves = []
    for side in range(2):
        halo = hz_v[side] - there["gz", side] * turn(zsend_v[side], cz // 2)
        for s in range(2):
            corner = turn(jnp.broadcast_to(hxz_v[2 * s + side], (8, cz)), cz // 2)[:1]
            halo = halo - jnp.where(layer == (cx - 1) * s, 2.0 * corner, 0.0)
        parts = []
        for part in range(groups):
            piece = halo[8 * part:8 * part + 8]
            for s in range(2):
                spot = 2 * (groups * (1 - s) + part) + side
                goal = cy if s == 0 else 2 * cy - 1
                corner = turn(hyz_v[2 * s + side], goal - spot)
                piece = piece - jnp.where(lane8 == goal, 2.0 * corner, 0.0)
            parts.append(piece)
        halves.append(jnp.concatenate(parts, axis=0))

    y_stencil = []
    for side in range(2):
        h = hy_v[side, 0]
        around = jnp.where(lane_x == 0, 0.0, turn(h, 1))
        around = around + jnp.where(lane_x == cz - 1, 0.0, turn(h, -1))
        around = around + jnp.where(layer == 0, 0.0, turn(h, 1, 0))
        around = around + jnp.where(layer == cx - 1, 0.0, turn(h, -1, 0))
        y_stencil.append(drows_v[side] * h - around)
        face_sums(
            h, y_halo[side], ysend_v[side, 0], ysend_v[side, 1], qrows_v[side], y_stencil[side]
        )
    z_stencil, z_h, z_halves = [], [], []
    used = lane_x < cy
    for side in range(2):
        h = jnp.where(used, hz_v[side], 0.0)
        halo = jnp.where(used, turn(halves[side], cz // 2), 0.0)
        around = turn(h, 1) + jnp.where(lane_x == cz - 1, 0.0, turn(h, -1))
        around = around + jnp.where(layer == 0, 0.0, turn(h, 1, 0))
        around = around + jnp.where(layer == cx - 1, 0.0, turn(h, -1, 0))
        span = pl.ds(cx * side, cx)
        z_stencil.append(cols_v[pl.ds(2 * cx + cx * side, cx)] * h - around)
        z_h.append(h)
        z_halves.append(halo)
        own_p = turn(zsend_v[side], cz // 2)
        face_sums(h, halo, zsend_v[side], own_p, qcols_v[span], z_stencil[side])

    def edge_sums(one, one_in, one_halo, other, other_halo, other_stencil):
        second = 2.0 * one * other
        third = 2.0 * (one * other_stencil - one_in * other)
        return second, third + one * other_halo + other * one_halo

    for s in range(2):
        for t in range(2):
            goal = (cy - 1) * s
            spot, spot_in = ((0, 1), (cz - 1, cz - 2))[t]
            second, third = edge_sums(
                turn(hy_v[s, 0], goal - spot), turn(hy_v[s, 0], goal - spot_in),
                turn(y_halo[s], goal - spot), z_h[t], z_halves[t], z_stencil[t],
            )
            add(2, jnp.where(lane_x == goal, second, 0.0))
            add(3, jnp.where(lane_x == goal, third, 0.0))

    settle(0, lambda copy: copy.wait_recv())
    for side in range(2):
        x = (cx - 1) * side
        h, load = hx_v[side, 0], load_v[x]
        around = jnp.where(lane == 0, 0.0, turn(h, 1))
        around = around + jnp.where(lane == cz - 1, 0.0, turn(h, -1))
        around = around + jnp.where(row == 0, 0.0, turn(h, 1, 0))
        around = around + jnp.where(row == cy - 1, 0.0, turn(h, -1, 0))
        halo = hx_v[side, 1] - there["gx", side] * load
        face_sums(h, halo, load, p_v[x], q_v[x], diag_v[x] * h - around)
    for s in range(2):
        x = (cx - 1) * s
        for t in range(2):
            y, y_in = ((0, 1), (cy - 1, cy - 2))[t]
            second, third = edge_sums(
                hx_v[s, 0, y:y + 1], hx_v[s, 0, y_in:y_in + 1],
                hx_v[s, 1, y:y + 1] - there["gx", s] * load_v[x, y:y + 1],
                hy_v[t, 0, x:x + 1], y_halo[t][x:x + 1], y_stencil[t][x:x + 1],
            )
            rows[2], rows[3] = rows[2] + second, rows[3] + third
            second, third = edge_sums(
                hxr_v[s, 2 * t], hxr_v[s, 2 * t + 1],
                turn(jnp.broadcast_to(hxr_v[s, 2 * t], (8, cz)), cz // 2)[:1]
                - there["gx", s] * zsend_v[t, x:x + 1],
                z_h[t][x:x + 1], z_halves[t][x:x + 1], z_stencil[t][x:x + 1],
            )
            used1 = lane1 < cy
            rows[2] = rows[2] + jnp.where(used1, second, 0.0)
            rows[3] = rows[3] + jnp.where(used1, third, 0.0)
    def columned(halves):
        for side in range(2):
            mix_v[pl.ds(1 - side, cx, stride=2), :] = halves[side]
        columns = mix_v[...].T
        return jnp.concatenate([columns, jnp.zeros((cz, cz - 2 * cx), F32)], axis=1)

    def complete():
        for kind in range(2):
            settle(kind, lambda copy: copy.wait_send())
        l_halo = columned([hz_v[0], hz_v[1]])[:cy]
        for x in range(cx):
            plane = p_v[x] - jnp.where(ends, turn(l_halo, -2 * x - 1), 0.0)
            plane = rim(plane, hy_v[0, 0, x:x + 1], hy_v[1, 0, x:x + 1])
            for side in range(2):
                if x == (cx - 1) * side:
                    plane = plane - hx_v[side, 0]
            p_v[x] = plane
        z_halo = columned(halves)[cy:2 * cy]
        for x in range(cx):
            plane = inside(p_v, x) - jnp.where(ends, turn(z_halo, -2 * x - 1), 0.0)
            plane = rim(plane, y_halo[0][x:x + 1], y_halo[1][x:x + 1])
            for side in range(2):
                if x == (cx - 1) * side:
                    plane = plane - hx_v[side, 1] + there["gx", side] * load_v[x]
            q_v[x] = plane

    own = row8 == lane8 // (cz // 4)
    mine = jnp.zeros((8, cz), F32)
    for order in range(4):
        total = acc[order] + jnp.where(row8 == 0, rows[order], 0.0)
        total = total + pltpu.roll(total, cz // 2, axis=1)
        total = total + pltpu.roll(total, cz // 4, axis=1)
        mine = jnp.where(lane8 // (cz // 4) == order, total, mine)
    mine = jnp.sum(mine, axis=0, keepdims=True)
    hear(relays - 1)
    slot = 0
    waiting = []
    for order, axes in enumerate(stages):
        part_v[order] = mine
        offsets = offsets_of(sizes, axes)

        def part(offset, src, dst):
            return pltpu.make_async_remote_copy(
                src_ref=src, dst_ref=dst,
                send_sem=red_send.at[order], recv_sem=red_recv.at[order],
                device_id=across(offset), device_id_type=MESH,
            )

        for place, offset in enumerate(offsets):
            part(offset, part_v.at[order], gath_v.at[slot + place]).start()
        if order == 0:
            complete()
        if offsets:
            span = gath_v.at[pl.ds(slot, len(offsets))]
            waiting.append(part(offsets[0], span, span))
            waiting[-1].wait_recv()
        parts = [mine] + [gath_v[slot + place] for place in range(len(offsets))]
        while len(parts) > 1:
            parts = [sum(parts[n:n + 2]) for n in range(0, len(parts), 2)]
        mine = parts[0]
        slot += len(offsets)

    sums = jnp.sum(jnp.where(own, mine, 0.0), axis=1, keepdims=True)
    s0, s1, s2, s3 = (sums[n:n + 1] for n in range(4))
    inverse = 1.0 / (6.0 * s0 + s1)
    a, c, m, third = s0 * inverse, s1 * inverse, s2 * inverse, s3 * inverse
    growth = a * m - c * c
    e = c + growth
    curve = 6.0 * (e * e * a - 2.0 * e * a * c + a * a * m) + (
        e * e * c - 2.0 * e * a * m + a * a * third
    )
    b = a * growth / curve
    x_load, x_p = a + b * e, b * a
    r_load, r_p, r_q = c - 6.0 * b * e, a + b * (e - 6.0 * a), b * a
    for order, value in enumerate((x_load, x_p, r_load, r_p, r_q)):
        coef_ref[order:order + 1] = jnp.broadcast_to(value, (1, cz))
    for copy in arrivals + waiting:
        copy.wait_send()


def combine(load_ref, p_ref, q_ref, coef_ref, x_hbm, r_hbm, x_v, r_v, sem):
    cx = load_ref.shape[0]
    x_load, x_p, r_load, r_p, r_q = (coef_ref[n:n + 1] for n in range(5))
    pieces = 16
    for piece in range(pieces):
        first, last = cx * piece // pieces, cx * (piece + 1) // pieces
        for x in range(first, last):
            load, p = load_ref[x], p_ref[x]
            x_v[x] = x_load * load - x_p * p
            r_v[x] = r_load * load - r_p * p + r_q * q_ref[x]
        span = pl.ds(first, last - first)
        for number, (src, dst) in enumerate(((x_v, x_hbm), (r_v, r_hbm))):
            pltpu.make_async_copy(src.at[span], dst.at[span], sem.at[number]).start()
    for number, (src, dst) in enumerate(((x_v, x_hbm), (r_v, r_hbm))):
        pltpu.make_async_copy(src, dst, sem.at[number]).wait()


def combined(load, p, q, coef):
    cx, cy, cz = load.shape
    box = jax.ShapeDtypeStruct((cx, cy, cz), F32)
    vmem, hbm = (pl.BlockSpec(memory_space=space) for space in (pltpu.VMEM, pltpu.HBM))
    return pl.pallas_call(
        combine,
        out_shape=(box, box),
        in_specs=[vmem] * 4,
        out_specs=(hbm, hbm),
        scratch_shapes=[pltpu.VMEM((cx, cy, cz), F32)] * 2 + [pltpu.SemaphoreType.DMA((2,))],
    )(*(pltpu.with_memory_space_constraint(a, pltpu.VMEM) for a in (load, p, q, coef)))


def per_device(sizes, face_blocks, owner_rank, owner_tile, live_count, right_side, diagonal):
    blocks = face_blocks.shape[3]
    cx, cy, cz = right_side.shape
    group = sizes["gx"]
    stages = stages_of(sizes)
    relays = relays_of(sizes, stages)
    slots = sum(len(offsets_of(sizes, axes)) for axes in stages)
    vmem, hbm = (pl.BlockSpec(memory_space=space) for space in (pltpu.VMEM, pltpu.HBM))
    box = pltpu.VMEM((cx, cy, cz), F32)
    load, p, q, coef = pl.pallas_call(
        functools.partial(kernel, sizes, stages, relays),
        out_shape=(box, box, box, pltpu.VMEM((8, cz), F32)),
        in_specs=[hbm] * 6,
        out_specs=(vmem, vmem, vmem, vmem),
        scratch_shapes=[
            pltpu.SMEM((blocks,), jnp.int32),
            pltpu.SMEM((blocks,), jnp.int32),
            pltpu.SMEM(live_count.shape, jnp.int32),
            pltpu.VMEM((blocks, 2 * cy, cz), F32),
            pltpu.VMEM((cx, cy, cz), F32),
            pltpu.VMEM((blocks * cy, cz), F32),
            pltpu.VMEM((group, cy, cz), F32),
            pltpu.VMEM((group, 8, cz), F32),
            pltpu.VMEM((group, cy, cz), F32),
            pltpu.VMEM((group, 8, cz), F32),
            pltpu.VMEM((group, cy, cz), F32),
            pltpu.VMEM((4, cx, cz), F32),
            pltpu.VMEM((2, cx, cz), F32),
            pltpu.VMEM((4 * cx, cz), F32),
            pltpu.VMEM((2, 2, cy, cz), F32),
            pltpu.VMEM((2, 4, 1, cz), F32),
            pltpu.VMEM((2, 4, 1, cz), F32),
            pltpu.VMEM((2, cx, cz), F32),
            pltpu.VMEM((2 * cx, cz), F32),
            pltpu.VMEM((2, 2, cx, cz), F32),
            pltpu.VMEM((2, 2, cx, cz), F32),
            pltpu.VMEM((2, cx, cz), F32),
            pltpu.VMEM((2, cx, cz), F32),
            pltpu.VMEM((4, 1, cz), F32),
            pltpu.VMEM((4, 1, cz), F32),
            pltpu.VMEM((8, cz), F32),
            pltpu.VMEM((4, 8, cz), F32),
            pltpu.VMEM((4, 1, cz), F32),
            pltpu.VMEM((4, 1, cz), F32),
            pltpu.VMEM((2 * cx, cz), F32),
            pltpu.VMEM((max(message_rows(cx, cy, 2, 2, 2)), 1, cz), F32),
            pltpu.VMEM((len(stages), 1, cz), F32),
            pltpu.VMEM((slots, 1, cz), F32),
            pltpu.SemaphoreType.DMA((6,)),
            pltpu.SemaphoreType.DMA((2,)),
            pltpu.SemaphoreType.DMA((2,)),
            pltpu.SemaphoreType.REGULAR((relays,)),
            pltpu.SemaphoreType.DMA((2,)),
            pltpu.SemaphoreType.DMA((2,)),
            pltpu.SemaphoreType.DMA((len(stages),)),
            pltpu.SemaphoreType.DMA((len(stages),)),
        ],
        compiler_params=pltpu.CompilerParams(collective_id=0, has_side_effects=True),
    )(
        owner_rank.reshape(blocks), owner_tile.reshape(blocks),
        live_count,
        face_blocks.reshape(blocks, 2 * cy, cz), right_side, diagonal,
    )
    return combined(load, p, q, coef)


def solution(mesh):
    sizes = dict(mesh.shape)
    return jax.shard_map(
        functools.partial(per_device, sizes),
        mesh=mesh,
        in_specs=(
            P("gx", "gy", "gz", None, None),
            P("gx", "gy", "gz", None, None),
            P("gx", "gy", "gz", None),
            P("gx", "gy", "gz"),
            P("gx", "gy", "gz"),
            P("gx", "gy", "gz"),
        ),
        out_specs=(P("gx", "gy", "gz"), P("gx", "gy", "gz")),
        check_vma=False,
    )
```

```python
import functools
import math

import jax
import jax.numpy as jnp
from jax import lax
from jax.experimental import pallas as pl
from jax.experimental.pallas import tpu as pltpu
from jax.sharding import PartitionSpec as P

CAP = 2
AXES = ("gx", "gy", "gz")
MESH = pl.DeviceIdType.MESH
F32 = jnp.float32


def offsets_of(sizes, axes):
    found = [()]
    for axis in axes:
        found = [done + (step,) for done in found for step in range(sizes[axis])]
    offsets = [dict(zip(axes, steps)) for steps in found if any(steps)]
    return sorted(
        offsets, key=lambda o: -sum(s if a != "gx" else s / sizes[a] for a, s in o.items())
    )


def stages_of(sizes):
    stages = []
    for axis in ("gx", "gz", "gy"):
        if stages and math.prod(sizes[a] for a in stages[-1] + [axis]) <= 32:
            stages[-1].append(axis)
        else:
            stages.append([axis])
    return stages


def relays_of(sizes, stages):
    rounds = 2
    for axes in stages:
        steps = [sizes[axis] - 1 for axis in axes if axis != "gx"]
        single = sum(n % 2 for n in steps) + (1 if "gx" in axes and sizes["gx"] > 1 else 0)
        rounds = max(rounds, 1 + sum(n // 2 for n in steps) + max(0, single - 2))
    return rounds


def message_rows(cx, cy, nx, ny, nz):
    half = cy // 2
    faces = 4 * nx + 2 * cx * ny + cx * nz
    return (cy + half) * nx, faces, nx * ny + nx * nz + 8 * ny * nz, half * nx


def kernel(
    sizes, stages, relays,
    rank_hbm, tile_hbm, live_hbm, face_hbm, right_hbm, diag_hbm,
    load_v, p_v, q_v, coef_ref,
    rank_ref, tile_ref, live_ref, face_v, diag_v, sums_v,
    send_v, scard_v, recv_v, rcard_v, turned_v, rows_v, drows_v, cols_v,
    hx_v, xr_v, hxr_v, qrows_v, qcols_v, ysend_v, hy_v, zsend_v, hz_v, xy_v, hxy_v, yz_v, hyz_v, xz_v, hxz_v, mix_v, tally_v, part_v, gath_v,
    in_sem, a2a_send, a2a_recv, relay_sem, halo_send, halo_recv, red_send, red_recv,
):
    cx, cy, cz = load_v.shape
    blocks = face_v.shape[0]
    group = sizes["gx"]
    at = {axis: lax.axis_index(axis) for axis in AXES}

    def near(axis, side):
        return at[axis] > 0 if side == 0 else at[axis] < sizes[axis] - 1

    def beside(offset):
        return {a: lax.rem(at[a] + s, sizes[a]) for a, s in offset.items() if s}

    def across(offset):
        where = {}
        for axis, step in offset.items():
            if sizes[axis] & (sizes[axis] - 1):
                where[axis] = lax.rem(at[axis] + step, sizes[axis])
            else:
                where[axis] = at[axis]
                for bit in (1 << n for n in range(sizes[axis].bit_length())):
                    if step & bit:
                        where[axis] = where[axis] + bit - 2 * bit * lax.rem(at[axis] // bit, 2)
        return {axis: index for axis, index in where.items() if offset[axis]}

    def near_all(sides):
        found = near(*sides[0])
        for axis, side in sides[1:]:
            found = found & near(axis, side)
        return found

    loads = [
        pltpu.make_async_copy(face_hbm, face_v, in_sem.at[0]),
        pltpu.make_async_copy(right_hbm, load_v, in_sem.at[1]),
        pltpu.make_async_copy(diag_hbm, diag_v, in_sem.at[2]),
        pltpu.make_async_copy(live_hbm, live_ref, in_sem.at[3]),
        pltpu.make_async_copy(rank_hbm, rank_ref, in_sem.at[4]),
        pltpu.make_async_copy(tile_hbm, tile_ref, in_sem.at[5]),
    ]
    for copy in loads[:1] + loads[3:]:
        copy.start()

    def within(axis, step):
        return at[axis] + step >= 0 if step < 0 else at[axis] + step < sizes[axis]

    def greet(semaphore, reach=1):
        for k in range(1, group):
            pl.semaphore_signal(
                semaphore, inc=1, device_id=beside({"gx": k}), device_id_type=MESH
            )
        for axis in ("gy", "gz"):
            for step in range(-reach, reach + 1):
                if 0 < abs(step) < sizes[axis]:
                    @pl.when(within(axis, step))
                    def _():
                        pl.semaphore_signal(
                            semaphore, inc=1, device_id={axis: at[axis] + step},
                            device_id_type=MESH,
                        )

    def greeted(reach=1):
        count = jnp.int32(group - 1)
        for axis in ("gy", "gz"):
            for step in range(-reach, reach + 1):
                if 0 < abs(step) < sizes[axis]:
                    count = count + jnp.where(within(axis, step), 1, 0)
        return count

    barrier = pltpu.get_barrier_semaphore()
    greet(barrier)

    half = cy // 2
    messages = {"x": [], "late": [], "z": [], "y": [], "xr": [], "xy": [], "xz": [], "yz": []}
    for s in range(2):
        end = (cx - 1) * s
        messages["x"].append(((("gx", s),), load_v.at[end], lambda s: hx_v.at[s, 0]))
        messages["x"].append((
            (("gx", s),), p_v.at[end, pl.ds(half * s, half)],
            lambda s: hx_v.at[s, 1, pl.ds(half * (1 - s), half)],
        ))
        messages["late"].append((
            (("gx", s),), p_v.at[end, pl.ds(half * (1 - s), half)],
            lambda s: hx_v.at[s, 1, pl.ds(half * s, half)],
        ))
        messages["xr"].append(((("gx", s),), xr_v.at[s], lambda s: hxr_v.at[s]))
        messages["y"].append(((("gy", s),), ysend_v.at[s], lambda s: hy_v.at[s]))
        messages["z"].append(((("gz", s),), zsend_v.at[s], lambda s: hz_v.at[s]))
        for t in range(2):
            messages["xy"].append(
                ((("gx", s), ("gy", t)), xy_v.at[2 * s + t], lambda s, t: hxy_v.at[2 * s + t])
            )
            messages["xz"].append(
                ((("gx", s), ("gz", t)), xz_v.at[2 * s + t], lambda s, t: hxz_v.at[2 * s + t])
            )
            messages["yz"].append(
                ((("gy", s), ("gz", t)), yz_v, lambda s, t: hyz_v.at[2 * s + t])
            )

    def kind_of(name):
        return {"x": 0, "y": 1, "z": 1, "xr": 1, "late": 3}.get(name, 2)

    def send(name, part=None):
        for order, (sides, src, place) in enumerate(messages[name]):
            if part in (None, order % 2):
                @pl.when(near_all(sides))
                def _():
                    pltpu.make_async_remote_copy(
                        src_ref=src, dst_ref=place(*[1 - side for _, side in sides]),
                        send_sem=halo_send.at[kind_of(name)],
                        recv_sem=halo_recv.at[kind_of(name)],
                        device_id={
                            axis: lax.rem(
                                at[axis] + (1 if side else sizes[axis] - 1), sizes[axis]
                            )
                            for axis, side in sides
                        },
                        device_id_type=MESH,
                    ).start()

    def settle(kind, act):
        beside_on = {
            axis: sum(jnp.where(near(axis, side), 1, 0) for side in range(2)) for axis in AXES
        }
        counts = [range(min(1, sizes[axis] - 1), min(2, sizes[axis] - 1) + 1) for axis in AXES]
        for nx in counts[0]:
            for ny in counts[1] if kind in (1, 2) else (0,):
                for nz in counts[2] if kind in (1, 2) else (0,):
                    lines = message_rows(cx, cy, nx, ny, nz)[kind]
                    found = beside_on["gx"] == nx
                    if kind in (1, 2):
                        found = found & (beside_on["gy"] == ny) & (beside_on["gz"] == nz)
                    if lines:
                        @pl.when(found)
                        def _():
                            span = tally_v.at[pl.ds(0, lines)]
                            act(pltpu.make_async_remote_copy(
                                src_ref=span, dst_ref=span,
                                send_sem=halo_send.at[kind], recv_sem=halo_recv.at[kind],
                                device_id=beside({"gx": 1}), device_id_type=MESH,
                            ))

    for name in messages:
        for sides, _, place in messages[name]:
            slot = place(*[side for _, side in sides])

            @pl.when(jnp.logical_not(near_all(sides)))
            def _():
                slot[...] = jnp.zeros(slot.shape, F32)

    lane = lax.broadcasted_iota(jnp.int32, (cy, cz), 1)
    lane1 = lax.broadcasted_iota(jnp.int32, (1, cz), 1)
    lane8 = lax.broadcasted_iota(jnp.int32, (8, cz), 1)
    row = lax.broadcasted_iota(jnp.int32, (cy, cz), 0)
    row8 = lax.broadcasted_iota(jnp.int32, (8, cz), 0)
    layer = lax.broadcasted_iota(jnp.int32, (cx, cz), 0)
    lane_x = lax.broadcasted_iota(jnp.int32, (cx, cz), 1)
    ends = (lane == 0) | (lane == cz - 1)

    def turn(values, by, axis=1):
        by = by % values.shape[axis]
        return values if by == 0 else pltpu.roll(values, by, axis=axis)

    loads[0].wait()
    for copy in loads[1:3]:
        copy.start()
    for copy in loads[3:]:
        copy.wait()
    pair = (
        lax.broadcasted_iota(jnp.int32, (cz, cz), 0) // 2
        == lax.broadcasted_iota(jnp.int32, (cz, cz), 1) % (cz // 2)
    )
    pair = jnp.where(pair, 0.25, 0.0).astype(jnp.bfloat16)
    for b in range(blocks):
        sums_v[b * cy:(b + 1) * cy] = (
            face_v[b, pl.ds(0, cy, stride=2), :] + face_v[b, pl.ds(1, cy, stride=2), :]
        )
    whole = sums_v[...]
    high = whole.astype(jnp.bfloat16)
    rest = whole - high.astype(F32)
    middle = rest.astype(jnp.bfloat16)
    column = lax.broadcasted_iota(jnp.int32, (8, cz), 0)
    column = jnp.where(column < 2, column, cz // 2 - 4 + column)
    choice = (lax.broadcasted_iota(jnp.int32, (8, cz), 1) // 2 == column) & (column < cz // 2)
    choice = jnp.where(choice, 0.25, 0.0).astype(jnp.bfloat16)

    def columns_of(values):
        return lax.dot_general(
            choice, values, (((1,), (1,)), ((), ())), preferred_element_type=F32
        )

    columns = columns_of(middle) + columns_of(high)
    sums_v[...] = (
        jnp.dot(middle, pair, preferred_element_type=F32)
        + jnp.dot(high, pair, preferred_element_type=F32)
    )

    target = [rank_ref[b] for b in range(blocks)]
    alive = [live_ref[0, 0, 0] > b for b in range(blocks)]
    position = []
    for b in range(blocks):
        count = jnp.int32(0)
        for before in range(b):
            count = count + jnp.where((target[before] == target[b]) & alive[before], 1, 0)
        position.append(count)
    edges = []
    for b in range(blocks):
        here = columns[:, b // 2 * cz:b // 2 * cz + cz]
        there = pltpu.roll(here, cz // 2, axis=1)
        first, last = (here, there) if b % 2 == 0 else (there, here)
        even = jnp.where(lane1 < cz // 2, first[0:1], last[1:2])
        other = jnp.where(lane1 < cz // 2, first[3:4], last[2:3])
        edges.append(jnp.where(lax.rem(tile_ref[b], 2) == 0, even, other))
    cards = []
    for b in range(blocks):
        card = jnp.where(row8 < 6, edges[b], (tile_ref[b] + 1).astype(F32))
        for place, y in enumerate((0, 1, cy - 2, cy - 1)):
            card = jnp.where(row8 == place, sums_v[b * cy + y:b * cy + y + 1], card)
        cards.append(card)
    slot0 = jnp.where(row8 == 4, 1, jnp.where(row8 == 5, 0, jnp.where(lane8 < cz // 2, 1, 0)))
    slot0 = slot0.astype(F32)
    slot1 = 1.0 - slot0
    boxes = ((send_v, recv_v), (scard_v, rcard_v))

    def exchange(order, slots, offset):
        src, dst = boxes[order]
        return pltpu.make_async_remote_copy(
            src_ref=src.at[slots], dst_ref=dst.at[slots],
            send_sem=a2a_send.at[order], recv_sem=a2a_recv.at[order],
            device_id=across(offset), device_id_type=MESH,
        )

    pl.semaphore_wait(barrier, greeted())
    shares = {}
    for k in reversed(range(group)):
        dest = across({"gx": k})["gx"] if k else at["gx"]
        total = jnp.zeros((8, cz), F32)
        for b in range(blocks):
            code = jnp.where(alive[b] & (target[b] == dest), position[b], CAP)
            left, right = jnp.where(code == 0, 1.0, 0.0), jnp.where(code == 1, 1.0, 0.0)
            shares[k, b] = left, right
            total = total + cards[b] * (slot0 * left + slot1 * right)
        (rcard_v if k == 0 else scard_v)[k] = total
        if k:
            exchange(1, pl.ds(k, 1), {"gx": k}).start()
    for k in reversed(range(group)):
        total = jnp.zeros((cy, cz), F32)
        for b in range(blocks):
            left, right = shares[k, b]
            values = sums_v[b * cy:(b + 1) * cy]
            total = total + values * jnp.where(lane1 < cz // 2, left, right)
        (recv_v if k == 0 else send_v)[k] = total
        if k:
            exchange(0, pl.ds(k, 1), {"gx": k}).start()
    arrivals = [
        exchange(order, pl.ds(1, group - 1), {"gx": 1}) for order in (1, 0) if group > 1
    ]
    greet(relay_sem.at[0])
    loads[1].wait()
    loads[2].wait()

    for x in range(cx):
        for place, y in enumerate((0, 1, cy - 2, cy - 1)):
            rows_v[place, x:x + 1] = load_v[x, y:y + 1]
        for place, y in enumerate((0, cy - 1)):
            drows_v[place, x:x + 1] = diag_v[x, y:y + 1]
    upper, lower = jnp.zeros((cy, cz), F32), jnp.zeros((cy, cz), F32)
    for x in range(cx):
        plane, weights = load_v[x], diag_v[x]
        for side in range(2):
            spot = cx * side + x
            upper = jnp.where(lane == spot, turn(plane, spot + side), upper)
            lower = jnp.where(lane == spot, turn(plane, spot + 3 * side - 1), lower)
            spot = spot + 2 * cx
            upper = jnp.where(lane == spot, turn(weights, spot + side), upper)
    cols_v[...] = jnp.concatenate([upper, lower], axis=0).T[:4 * cx]

    def hear(relay):
        pl.semaphore_wait(relay_sem.at[relay], greeted(min(relay + 1, 2)))
        if relay < relays - 1:
            greet(relay_sem.at[relay + 1], 2)

    hear(0)
    for copy in arrivals[:1]:
        copy.wait_recv()

    received, sources = [], []
    for k in range(group):
        card = rcard_v[k]
        swapped = pltpu.roll(card, cz // 2, axis=1)
        received += [(card, card[6:7] - 1.0), (swapped, swapped[6:7] - 1.0)]
        sources += [(recv_v.at[k], received[-2][1]), (turned_v.at[k], received[-1][1])]
    half1 = jnp.where(lane1 >= cz // 2, 1, 0)

    def scatter(x):
        want = (2 * x + half1).astype(F32)
        plane = load_v[x]
        for values, tags in sources:
            plane = plane + jnp.where(tags == want, values[...], 0.0)
        load_v[x] = plane

    def inside(src, x):
        plane = src[x]
        around = jnp.where(lane == 0, 0.0, pltpu.roll(plane, 1, axis=1))
        around = around + jnp.where(lane == cz - 1, 0.0, pltpu.roll(plane, cz - 1, axis=1))
        around = around + jnp.where(row == 0, 0.0, pltpu.roll(plane, 1, axis=0))
        around = around + jnp.where(row == cy - 1, 0.0, pltpu.roll(plane, cy - 1, axis=0))
        if x > 0:
            around = around + src[x - 1]
        if x < cx - 1:
            around = around + src[x + 1]
        return diag_v[x] * plane - around

    want = (2 * layer + jnp.where(lane_x >= cz // 2, 1, 0)).astype(F32)
    faces = [rows_v[place] for place in range(4)]
    for card, tags in received:
        hit = jnp.broadcast_to(tags, (cx, cz)) == want
        for place in range(4):
            spread = jnp.broadcast_to(card[place:place + 1], (cx, cz))
            faces[place] = faces[place] + jnp.where(hit, spread, 0.0)
    for side in range(2):
        face, second = faces[3 * side], faces[1 + side]
        around = jnp.where(lane_x == 0, 0.0, pltpu.roll(face, 1, axis=1)) + second
        around = around + jnp.where(lane_x == cz - 1, 0.0, pltpu.roll(face, cz - 1, axis=1))
        around = around + jnp.where(layer == 0, 0.0, pltpu.roll(face, 1, axis=0))
        around = around + jnp.where(layer == cx - 1, 0.0, pltpu.roll(face, cx - 1, axis=0))
        ysend_v[side, 0] = face
        ysend_v[side, 1] = drows_v[side] * face - around
        for s in range(2):
            xy_v[2 * s + side] = face[(cx - 1) * s:(cx - 1) * s + 1]

    line = lax.broadcasted_iota(jnp.int32, (2 * cx, cz), 0)
    lane_z = lax.broadcasted_iota(jnp.int32, (2 * cx, cz), 1)
    own_tile = (2 * (line % cx) + line // cx).astype(F32)
    turned = cols_v[:2 * cx]
    for k in range(group):
        card, tags = received[2 * k]
        for place in range(CAP):
            tag = tags[:, :1] if place == 0 else tags[:, cz - 1:]
            hit = jnp.broadcast_to(tag, (2 * cx, cz)) == own_tile
            values = jnp.broadcast_to(card[4 + place:5 + place], (2 * cx, cz))
            turned = turned + jnp.where(hit, values, 0.0)
    around = jnp.where(lane_z == 0, 0.0, turn(turned, 1)) + turn(turned, cz // 2)
    around = around + jnp.where(lane_z == cy - 1, 0.0, turn(turned, -1))
    around = around + jnp.where(line % cx == 0, 0.0, turn(turned, 1, 0))
    around = around + jnp.where(line % cx == cx - 1, 0.0, turn(turned, -1, 0))
    image = cols_v[2 * cx:] * turned - around
    deeper = turn(turned, cz // 2)
    turned = jnp.where(lane_z < cy, turned, turn(image, cz // 2))
    for side in range(2):
        zsend_v[side] = turned[cx * side:cx * side + cx]
    groups = cx // 8
    tile = jnp.zeros((8, cz), F32)
    for side in range(2):
        for part in range(groups):
            spot = 2 * (groups * side + part)
            piece = turn(ysend_v[side, 0, 8 * part:8 * part + 8], spot + 1)
            tile = jnp.where(lane8 // 2 == spot // 2, piece, tile)
        for s in range(2):
            spot = cx * side + (cx - 1) * s
            xz_v[2 * s + side] = turned[spot:spot + 1]
            xr_v[s, 2 * side] = turned[spot:spot + 1]
            xr_v[s, 2 * side + 1] = deeper[spot:spot + 1]
    yz_v[...] = tile
    for name in ("yz", "xz", "xy", "z", "y", "xr"):
        send(name)

    for copy in arrivals[1:]:
        copy.wait_recv()
    for k in range(group):
        turned_v[k] = pltpu.roll(recv_v[k], cz // 2, axis=1)

    for x in (0, cx - 1):
        scatter(x)
    send("x", 0)
    for x in (1, cx - 2):
        scatter(x)
    for x in (0, cx - 1):
        p_v[x] = inside(load_v, x)
    send("x", 1)
    send("late")
    for relay in range(1, relays - 1):
        hear(relay)

    def fold(acc, values):
        for part in range(cy // 8):
            acc = acc + values[8 * part:8 * part + 8]
        return acc

    for x in range(2, cx - 2):
        scatter(x)
    for x in range(1, cx - 1):
        p_v[x] = inside(load_v, x)
    acc = [jnp.zeros((8, cz), F32) for _ in range(4)]
    for x in range(cx):
        q_v[x] = inside(p_v, x)
    for x in range(cx):
        load, p, q = load_v[x], p_v[x], q_v[x]
        pairs = ((load, load), (load, p), (p, p), (p, q))
        acc = [fold(total, one * other) for total, (one, other) in zip(acc, pairs)]
    image = jnp.zeros((cy, cz), F32)
    for x in range(cx):
        q = q_v[x]
        for side in range(2):
            y = (cy - 1) * side
            qrows_v[side, x:x + 1] = q_v[x, y:y + 1]
            spot = cx * side + x
            image = jnp.where(lane == spot, turn(q, spot + side), image)
    qcols_v[...] = jnp.concatenate([image, jnp.zeros((cz - cy, cz), F32)], axis=0).T[:2 * cx]

    def rim(plane, first, last):
        top = plane[:8] - jnp.where(row8 == 0, first, 0.0)
        bottom = plane[cy - 8:] - jnp.where(row8 == 7, last, 0.0)
        return jnp.concatenate([top, plane[8:cy - 8], bottom], axis=0)

    settle(1, lambda copy: copy.wait_recv())
    there = {
        (axis, side): jnp.where(near(axis, side), 1.0, 0.0) for axis in AXES for side in range(2)
    }
    def add(at_sum, values):
        for part in range(values.shape[0] // 8):
            acc[at_sum] = acc[at_sum] + values[8 * part:8 * part + 8]

    def face_sums(h, halo, load, p, q, stencil):
        add(1, -(load * h))
        add(2, h * (h - 2.0 * p))
        add(3, h * (stencil + halo - 2.0 * q) - p * halo)

    rows = [jnp.zeros((1, cz), F32) for _ in range(4)]
    y_base = [hy_v[side, 1] - there["gy", side] * ysend_v[side, 0] for side in range(2)]
    z_base = [
        hz_v[side] - there["gz", side] * turn(zsend_v[side], cz // 2) for side in range(2)
    ]
    y_stencil = []
    for side in range(2):
        h = hy_v[side, 0]
        around = jnp.where(lane_x == 0, 0.0, turn(h, 1))
        around = around + jnp.where(lane_x == cz - 1, 0.0, turn(h, -1))
        around = around + jnp.where(layer == 0, 0.0, turn(h, 1, 0))
        around = around + jnp.where(layer == cx - 1, 0.0, turn(h, -1, 0))
        y_stencil.append(drows_v[side] * h - around)
        face_sums(
            h, y_base[side], ysend_v[side, 0], ysend_v[side, 1], qrows_v[side], y_stencil[side]
        )
    z_stencil, z_h, z_halves = [], [], []
    used = lane_x < cy
    for side in range(2):
        h = jnp.where(used, hz_v[side], 0.0)
        halo = jnp.where(used, turn(z_base[side], cz // 2), 0.0)
        around = turn(h, 1) + jnp.where(lane_x == cz - 1, 0.0, turn(h, -1))
        around = around + jnp.where(layer == 0, 0.0, turn(h, 1, 0))
        around = around + jnp.where(layer == cx - 1, 0.0, turn(h, -1, 0))
        span = pl.ds(cx * side, cx)
        z_stencil.append(cols_v[pl.ds(2 * cx + cx * side, cx)] * h - around)
        z_h.append(h)
        z_halves.append(halo)
        own_p = turn(zsend_v[side], cz // 2)
        face_sums(h, halo, zsend_v[side], own_p, qcols_v[span], z_stencil[side])

    def edge_sums(one, one_in, one_halo, other, other_halo, other_stencil):
        second = 2.0 * one * other
        third = 2.0 * (one * other_stencil - one_in * other)
        return second, third + one * other_halo + other * one_halo

    for s in range(2):
        for t in range(2):
            goal = (cy - 1) * s
            spot, spot_in = ((0, 1), (cz - 1, cz - 2))[t]
            second, third = edge_sums(
                turn(hy_v[s, 0], goal - spot), turn(hy_v[s, 0], goal - spot_in),
                turn(y_base[s], goal - spot), z_h[t], z_halves[t], z_stencil[t],
            )
            add(2, jnp.where(lane_x == goal, second, 0.0))
            add(3, jnp.where(lane_x == goal, third, 0.0))

    share = [jnp.where((lane1 >= half) == (side == 0), 2.0, 0.0) for side in range(2)]
    settle(0, lambda copy: copy.wait_recv())
    for side in range(2):
        x = (cx - 1) * side
        h, load = hx_v[side, 0], load_v[x]
        around = jnp.where(lane == 0, 0.0, turn(h, 1))
        around = around + jnp.where(lane == cz - 1, 0.0, turn(h, -1))
        around = around + jnp.where(row == 0, 0.0, turn(h, 1, 0))
        around = around + jnp.where(row == cy - 1, 0.0, turn(h, -1, 0))
        face_sums(h, 0.0, load, p_v[x], q_v[x], diag_v[x] * h - around)
        first = half * (1 - side)
        halo = hx_v[side, 1, first:first + half] - there["gx", side] * load[first:first + half]
        add(3, 2.0 * (h[first:first + half] - p_v[x, first:first + half]) * halo)
    for s in range(2):
        x = (cx - 1) * s
        for t in range(2):
            y, y_in = ((0, 1), (cy - 1, cy - 2))[t]
            second, third = edge_sums(
                hx_v[s, 0, y:y + 1], hx_v[s, 0, y_in:y_in + 1],
                2.0 * (hx_v[s, 1, y:y + 1] - there["gx", s] * load_v[x, y:y + 1])
                if s != t else jnp.zeros((1, cz), F32),
                hy_v[t, 0, x:x + 1], y_base[t][x:x + 1], y_stencil[t][x:x + 1],
            )
            rows[2], rows[3] = rows[2] + second, rows[3] + third
            second, third = edge_sums(
                hxr_v[s, 2 * t], hxr_v[s, 2 * t + 1],
                share[s] * (
                    turn(jnp.broadcast_to(hxr_v[s, 2 * t], (8, cz)), cz // 2)[:1]
                    - there["gx", s] * zsend_v[t, x:x + 1]
                ),
                z_h[t][x:x + 1], z_halves[t][x:x + 1], z_stencil[t][x:x + 1],
            )
            used1 = lane1 < cy
            rows[2] = rows[2] + jnp.where(used1, second, 0.0)
            rows[3] = rows[3] + jnp.where(used1, third, 0.0)
    inner_p = [turn(zsend_v[side], cz // 2) - z_h[side] for side in range(2)]
    xy_p, xz_p, yz_p = {}, {}, {}
    for s in range(2):
        x = (cx - 1) * s
        for t in range(2):
            y, z, last = (cy - 1) * t, (cz - 1) * t, (cy - 1) * t
            ends_z = [
                jnp.broadcast_to(hz_v[side, x:x + 1, last:last + 1], (1, cz)) for side in range(2)
            ]
            tips = jnp.where(lane1 == 0, ends_z[0], jnp.where(lane1 == cz - 1, ends_z[1], 0.0))
            xy_p[s, t] = (
                ysend_v[t, 1, x:x + 1] - hy_v[t, 0, x:x + 1] - hx_v[s, 0, y:y + 1] - tips
            )
            ends_y = [
                jnp.broadcast_to(hy_v[side, 0, x:x + 1, z:z + 1], (1, cz)) for side in range(2)
            ]
            tips = jnp.where(lane1 == 0, ends_y[0], jnp.where(lane1 == cy - 1, ends_y[1], 0.0))
            xz_p[s, t] = inner_p[t][x:x + 1] - hxr_v[s, 2 * t] - tips
            goal, y = (cy - 1) * s, (cy - 1) * s
            values = inner_p[t] - turn(hy_v[s, 0], goal - z)
            for side in range(2):
                tip = jnp.broadcast_to(hx_v[side, 0, y:y + 1, z:z + 1], (cx, cz))
                values = values - jnp.where(layer == (cx - 1) * side, tip, 0.0)
            yz_p[s, t] = jnp.where(lane_x == goal, values, 0.0)
    settle(2, lambda copy: copy.wait_recv())
    groups = cx // 8
    for s in range(2):
        for t in range(2):
            rows[3] = rows[3] + (3.0 if s != t else 1.0) * xy_p[s, t] * hxy_v[2 * s + t]
            rows[3] = rows[3] + jnp.where(
                lane1 < cy, (1.0 + share[s]) * xz_p[s, t] * hxz_v[2 * s + t], 0.0
            )
            for part in range(groups):
                spot = 2 * (groups * (1 - s) + part) + t
                corner = turn(hyz_v[2 * s + t], (cy - 1) * s - spot)
                acc[3] = acc[3] + 2.0 * yz_p[s, t][8 * part:8 * part + 8] * corner

    def columned(halves):
        for side in range(2):
            mix_v[pl.ds(1 - side, cx, stride=2), :] = halves[side]
        columns = mix_v[...].T
        return jnp.concatenate([columns, jnp.zeros((cz, cz - 2 * cx), F32)], axis=1)

    def complete():
        settle(3, lambda copy: copy.wait_recv())
        for kind in range(4):
            settle(kind, lambda copy: copy.wait_send())
        y_halo = []
        for side in range(2):
            halo = hy_v[side, 1] - there["gy", side] * ysend_v[side, 0]
            halo = halo - jnp.where(layer == 0, 2.0 * hxy_v[side], 0.0)
            y_halo.append(halo - jnp.where(layer == cx - 1, 2.0 * hxy_v[2 + side], 0.0))
        halves = []
        for side in range(2):
            halo = hz_v[side] - there["gz", side] * turn(zsend_v[side], cz // 2)
            for s in range(2):
                corner = turn(jnp.broadcast_to(hxz_v[2 * s + side], (8, cz)), cz // 2)[:1]
                halo = halo - jnp.where(layer == (cx - 1) * s, 2.0 * corner, 0.0)
            parts = []
            for part in range(groups):
                piece = halo[8 * part:8 * part + 8]
                for s in range(2):
                    spot = 2 * (groups * (1 - s) + part) + side
                    goal = cy if s == 0 else 2 * cy - 1
                    corner = turn(hyz_v[2 * s + side], goal - spot)
                    piece = piece - jnp.where(lane8 == goal, 2.0 * corner, 0.0)
                parts.append(piece)
            halves.append(jnp.concatenate(parts, axis=0))
        l_halo = columned([hz_v[0], hz_v[1]])[:cy]
        for x in range(cx):
            plane = p_v[x] - jnp.where(ends, turn(l_halo, -2 * x - 1), 0.0)
            plane = rim(plane, hy_v[0, 0, x:x + 1], hy_v[1, 0, x:x + 1])
            for side in range(2):
                if x == (cx - 1) * side:
                    plane = plane - hx_v[side, 0]
            p_v[x] = plane
        z_halo = columned(halves)[cy:2 * cy]
        for x in range(cx):
            plane = inside(p_v, x) - jnp.where(ends, turn(z_halo, -2 * x - 1), 0.0)
            plane = rim(plane, y_halo[0][x:x + 1], y_halo[1][x:x + 1])
            for side in range(2):
                if x == (cx - 1) * side:
                    plane = plane - hx_v[side, 1] + there["gx", side] * load_v[x]
            q_v[x] = plane

    own = row8 == lane8 // (cz // 4)
    mine = jnp.zeros((8, cz), F32)
    for order in range(4):
        total = acc[order] + jnp.where(row8 == 0, rows[order], 0.0)
        total = total + pltpu.roll(total, cz // 2, axis=1)
        total = total + pltpu.roll(total, cz // 4, axis=1)
        mine = jnp.where(lane8 // (cz // 4) == order, total, mine)
    mine = jnp.sum(mine, axis=0, keepdims=True)
    hear(relays - 1)
    slot = 0
    waiting = []
    for order, axes in enumerate(stages):
        part_v[order] = mine
        offsets = offsets_of(sizes, axes)

        def part(offset, src, dst):
            return pltpu.make_async_remote_copy(
                src_ref=src, dst_ref=dst,
                send_sem=red_send.at[order], recv_sem=red_recv.at[order],
                device_id=across(offset), device_id_type=MESH,
            )

        for place, offset in enumerate(offsets):
            part(offset, part_v.at[order], gath_v.at[slot + place]).start()
        if order == 0:
            complete()
        if offsets:
            span = gath_v.at[pl.ds(slot, len(offsets))]
            waiting.append(part(offsets[0], span, span))
            waiting[-1].wait_recv()
        parts = [mine] + [gath_v[slot + place] for place in range(len(offsets))]
        while len(parts) > 1:
            parts = [sum(parts[n:n + 2]) for n in range(0, len(parts), 2)]
        mine = parts[0]
        slot += len(offsets)

    sums = jnp.sum(jnp.where(own, mine, 0.0), axis=1, keepdims=True)
    s0, s1, s2, s3 = (sums[n:n + 1] for n in range(4))
    inverse = 1.0 / (6.0 * s0 + s1)
    a, c, m, third = s0 * inverse, s1 * inverse, s2 * inverse, s3 * inverse
    growth = a * m - c * c
    e = c + growth
    curve = 6.0 * (e * e * a - 2.0 * e * a * c + a * a * m) + (
        e * e * c - 2.0 * e * a * m + a * a * third
    )
    b = a * growth / curve
    x_load, x_p = a + b * e, b * a
    r_load, r_p, r_q = c - 6.0 * b * e, a + b * (e - 6.0 * a), b * a
    for order, value in enumerate((x_load, x_p, r_load, r_p, r_q)):
        coef_ref[order:order + 1] = jnp.broadcast_to(value, (1, cz))
    for copy in arrivals + waiting:
        copy.wait_send()


def combine(load_ref, p_ref, q_ref, coef_ref, x_hbm, r_hbm, x_v, r_v, sem):
    cx = load_ref.shape[0]
    x_load, x_p, r_load, r_p, r_q = (coef_ref[n:n + 1] for n in range(5))
    pieces = 16
    for piece in range(pieces):
        first, last = cx * piece // pieces, cx * (piece + 1) // pieces
        for x in range(first, last):
            load, p = load_ref[x], p_ref[x]
            x_v[x] = x_load * load - x_p * p
            r_v[x] = r_load * load - r_p * p + r_q * q_ref[x]
        span = pl.ds(first, last - first)
        for number, (src, dst) in enumerate(((x_v, x_hbm), (r_v, r_hbm))):
            pltpu.make_async_copy(src.at[span], dst.at[span], sem.at[number]).start()
    for number, (src, dst) in enumerate(((x_v, x_hbm), (r_v, r_hbm))):
        pltpu.make_async_copy(src, dst, sem.at[number]).wait()


def combined(load, p, q, coef):
    cx, cy, cz = load.shape
    box = jax.ShapeDtypeStruct((cx, cy, cz), F32)
    vmem, hbm = (pl.BlockSpec(memory_space=space) for space in (pltpu.VMEM, pltpu.HBM))
    return pl.pallas_call(
        combine,
        out_shape=(box, box),
        in_specs=[vmem] * 4,
        out_specs=(hbm, hbm),
        scratch_shapes=[pltpu.VMEM((cx, cy, cz), F32)] * 2 + [pltpu.SemaphoreType.DMA((2,))],
    )(*(pltpu.with_memory_space_constraint(a, pltpu.VMEM) for a in (load, p, q, coef)))


def per_device(sizes, face_blocks, owner_rank, owner_tile, live_count, right_side, diagonal):
    blocks = face_blocks.shape[3]
    cx, cy, cz = right_side.shape
    group = sizes["gx"]
    stages = stages_of(sizes)
    relays = relays_of(sizes, stages)
    slots = sum(len(offsets_of(sizes, axes)) for axes in stages)
    vmem, hbm = (pl.BlockSpec(memory_space=space) for space in (pltpu.VMEM, pltpu.HBM))
    box = pltpu.VMEM((cx, cy, cz), F32)
    load, p, q, coef = pl.pallas_call(
        functools.partial(kernel, sizes, stages, relays),
        out_shape=(box, box, box, pltpu.VMEM((8, cz), F32)),
        in_specs=[hbm] * 6,
        out_specs=(vmem, vmem, vmem, vmem),
        scratch_shapes=[
            pltpu.SMEM((blocks,), jnp.int32),
            pltpu.SMEM((blocks,), jnp.int32),
            pltpu.SMEM(live_count.shape, jnp.int32),
            pltpu.VMEM((blocks, 2 * cy, cz), F32),
            pltpu.VMEM((cx, cy, cz), F32),
            pltpu.VMEM((blocks * cy, cz), F32),
            pltpu.VMEM((group, cy, cz), F32),
            pltpu.VMEM((group, 8, cz), F32),
            pltpu.VMEM((group, cy, cz), F32),
            pltpu.VMEM((group, 8, cz), F32),
            pltpu.VMEM((group, cy, cz), F32),
            pltpu.VMEM((4, cx, cz), F32),
            pltpu.VMEM((2, cx, cz), F32),
            pltpu.VMEM((4 * cx, cz), F32),
            pltpu.VMEM((2, 2, cy, cz), F32),
            pltpu.VMEM((2, 4, 1, cz), F32),
            pltpu.VMEM((2, 4, 1, cz), F32),
            pltpu.VMEM((2, cx, cz), F32),
            pltpu.VMEM((2 * cx, cz), F32),
            pltpu.VMEM((2, 2, cx, cz), F32),
            pltpu.VMEM((2, 2, cx, cz), F32),
            pltpu.VMEM((2, cx, cz), F32),
            pltpu.VMEM((2, cx, cz), F32),
            pltpu.VMEM((4, 1, cz), F32),
            pltpu.VMEM((4, 1, cz), F32),
            pltpu.VMEM((8, cz), F32),
            pltpu.VMEM((4, 8, cz), F32),
            pltpu.VMEM((4, 1, cz), F32),
            pltpu.VMEM((4, 1, cz), F32),
            pltpu.VMEM((2 * cx, cz), F32),
            pltpu.VMEM((max(message_rows(cx, cy, 2, 2, 2)), 1, cz), F32),
            pltpu.VMEM((len(stages), 1, cz), F32),
            pltpu.VMEM((slots, 1, cz), F32),
            pltpu.SemaphoreType.DMA((6,)),
            pltpu.SemaphoreType.DMA((2,)),
            pltpu.SemaphoreType.DMA((2,)),
            pltpu.SemaphoreType.REGULAR((relays,)),
            pltpu.SemaphoreType.DMA((4,)),
            pltpu.SemaphoreType.DMA((4,)),
            pltpu.SemaphoreType.DMA((len(stages),)),
            pltpu.SemaphoreType.DMA((len(stages),)),
        ],
        compiler_params=pltpu.CompilerParams(collective_id=0, has_side_effects=True),
    )(
        owner_rank.reshape(blocks), owner_tile.reshape(blocks),
        live_count,
        face_blocks.reshape(blocks, 2 * cy, cz), right_side, diagonal,
    )
    return combined(load, p, q, coef)


def solution(mesh):
    sizes = dict(mesh.shape)
    return jax.shard_map(
        functools.partial(per_device, sizes),
        mesh=mesh,
        in_specs=(
            P("gx", "gy", "gz", None, None),
            P("gx", "gy", "gz", None, None),
            P("gx", "gy", "gz", None),
            P("gx", "gy", "gz"),
            P("gx", "gy", "gz"),
            P("gx", "gy", "gz"),
        ),
        out_specs=(P("gx", "gy", "gz"), P("gx", "gy", "gz")),
        check_vma=False,
    )
```
